32 devices in a mesh: lat: 4 (over y, x), lon: 4 (over z), ens: 2 (over core).
Axes of the slice: x: 2, y: 2, z: 4, core: 2. Of those that a mesh axis runs over, the one named last changes fastest.
Arguments:
- parameters: float32 [2, 128, 32, 512], P(None, 'ens', 'lat', 'lon'), may hold values from -1.2 to 1.2, as said below
- initial_height: float32 [32, 512], P('lat', 'lon'), may hold values from -6 to 6
- initial_speed: float32 [2, 32, 512], P(None, 'lat', 'lon'), may hold values from -4 to 4
- obs_slots: int32 [2, 16, 16, 8], P(None, ('lat', 'lon')), may hold values from -1 to 1023, as said below
- obs_values: float32 [2, 16, 16, 8], P(None, ('lat', 'lon')), may hold values from -6 to 6
- obs_precision: float32 [2, 16, 16, 8], P(None, ('lat', 'lon')), may hold values from 0 to 2, as said below
Outputs:
- calibrated: float32 [2, 128, 32, 512], P(None, 'ens', 'lat', 'lon')
The draws below stay inside these ranges and needn't reach their ends.
Inputs may be any that keep to these rules, and one draw needn't show every extreme that they name: `obs_slots`: for each iteration and owner, the live slots towards one receiver come first and name distinct cells of the owner's block (local index row * 128 + column); no cell is named twice by one owner in one iteration; in each iteration some receiving block has all 8 slots live from every owner. `obs_precision`: zero exactly where the matching slot of obs_slots (with receiver and owner swapped) is empty, 0.5 or more elsewhere. `parameters`: friction rates lie in 0.02 to 0.2, forcing in -1.2 to 1.2.
All inputs are finite; a program needn't handle non-finite values.
Results may differ from the reference program's by a relative error of at most 0.0003.
Values sent between devices are 32-bit elements; how exact they have to be, the bound alone decides.
A program may use at most 64 MiB of HBM per device.

```python
import jax
import jax.numpy as jnp
from jax import lax

CLAT = 8
CLON = 128
MEMBERS = 128
STEPS = 6
ITERS = 2
CAP = 8
NLAT = 32
NLON = 512
OWNERS = 16
N_LAT = 4
N_LON = 4


def live_counts(key):
    owners = N_LAT * N_LON
    base = jax.random.fold_in(key, 7)
    counts = jax.random.randint(base, (ITERS, owners, owners), CAP // 4, CAP + 1)
    full_dest = jax.random.randint(jax.random.fold_in(base, 1), (ITERS,), 0, owners)
    receivers = jnp.arange(owners)
    counts = jnp.where(receivers[None, None, :] == full_dest[:, None, None], CAP, counts)
    slot_ids = jnp.arange(CAP)
    return slot_ids[None, None, None, :] < counts[..., None]


def draw_obs_slots(key, part):
    owners = N_LAT * N_LON
    live = live_counts(key)
    subkeys = jax.random.split(jax.random.fold_in(key, 11), ITERS * owners)
    orders = jax.vmap(lambda sub: jax.random.permutation(sub, CLAT * CLON))(subkeys)
    chosen = orders[:, :owners * CAP].reshape(ITERS, owners, owners, CAP).astype(jnp.int32)
    return jnp.where(live, chosen, -1).astype(jnp.int32)


def draw_obs_precision(key, part):
    owners = N_LAT * N_LON
    live = jnp.transpose(live_counts(key), (0, 2, 1, 3))
    sub = jax.random.fold_in(key, 23)
    values = jnp.exp(jax.random.uniform(sub, (ITERS, owners, owners, CAP), jnp.float32, jnp.log(0.5), jnp.log(2.0)))
    return jnp.where(live, values, 0.0).astype(jnp.float32)


def draw_parameters(key, part):
    first = jax.random.fold_in(key, 31)
    second = jax.random.fold_in(key, 37)
    friction = jnp.exp(jax.random.uniform(first, (MEMBERS, NLAT, NLON), jnp.float32, jnp.log(0.02), jnp.log(0.2)))
    forcing = jnp.clip(0.3 * jax.random.normal(second, (MEMBERS, NLAT, NLON), jnp.float32), -1.2, 1.2)
    return jnp.stack([friction, forcing]).astype(jnp.float32)


def levels(rng, shape, pieces, smallest, top_value):
    def one(position, shards_of):
        heights = jax.random.uniform(jax.random.fold_in(jax.random.fold_in(rng, 6), position), (shards_of,), jnp.float32, smallest / len(pieces), top_value / len(pieces))
        return jnp.repeat(jnp.exp(heights), shape[position] // shards_of).reshape((-1,) + (1,) * (len(shape) - position - 1))

    loudness = one(*pieces[0])
    for cut in pieces[1:]:
        loudness = loudness * one(*cut)
    return loudness


def bell_draw(stream_key, dims, deviation, most, pieces=(), held_as=jnp.bfloat16):
    gain = levels(stream_key, dims, pieces, -0.22, 0.18) if pieces else 1.0
    entries = jax.random.normal(stream_key, dims, jnp.float32) * deviation * gain
    return jnp.minimum(jnp.maximum(entries, -most), most).astype(held_as)


def setup_inputs(seed: int = 0) -> dict:
    arg_keys = jax.random.split(jax.random.key(seed), 7)
    parameters = draw_parameters(jax.random.fold_in(arg_keys[6], 71), 0)
    initial_height = bell_draw(arg_keys[1], (NLAT, NLON), 1.0, 6.0, ((0, 4), (1, 4)), jnp.float32)
    initial_speed = bell_draw(arg_keys[2], (2, NLAT, NLON), 0.5, 4.0, ((1, 4), (2, 4)), jnp.float32)
    obs_slots = draw_obs_slots(jax.random.fold_in(arg_keys[6], 71), 0)
    obs_values = bell_draw(arg_keys[4], (ITERS, OWNERS, OWNERS, CAP), 1.0, 6.0, ((1, 16),), jnp.float32)
    obs_precision = draw_obs_precision(jax.random.fold_in(arg_keys[6], 71), 0)
    return dict(parameters=parameters, initial_height=initial_height, initial_speed=initial_speed, obs_slots=obs_slots, obs_values=obs_values, obs_precision=obs_precision)


depth_step = 0.7
gravity_step = 0.7
coriolis = 0.1

def pad_grid(field):
    wrapped = jnp.concatenate([field[..., -1:], field, field[..., :1]], axis=-1)
    widths = [(0, 0)] * (field.ndim - 2) + [(1, 1), (0, 0)]
    return jnp.pad(wrapped, widths)

def forward(parameters, initial_height, initial_speed):
    members = parameters.shape[1]
    height = jnp.broadcast_to(initial_height, (members,) + initial_height.shape)
    speeds = jnp.broadcast_to(initial_speed[:, None], (2, members) + initial_height.shape)
    friction = parameters[0]
    forcing = parameters[1]
    for substep in range(STEPS):
        padded = pad_grid(speeds)
        east_diff = padded[0, :, 1:-1, 2:] - padded[0, :, 1:-1, :-2]
        north_diff = padded[1, :, 2:, 1:-1] - padded[1, :, :-2, 1:-1]
        height = height - depth_step * (east_diff + north_diff) + forcing
        padded_height = pad_grid(height)
        slope_east = padded_height[:, 1:-1, 2:] - padded_height[:, 1:-1, :-2]
        slope_north = padded_height[:, 2:, 1:-1] - padded_height[:, :-2, 1:-1]
        eastward = (1.0 - friction) * speeds[0] - gravity_step * slope_east + coriolis * speeds[1]
        northward = (1.0 - friction) * speeds[1] - gravity_step * slope_north - coriolis * speeds[0]
        speeds = jnp.stack([eastward, northward])
    return height

def gram_terms(predicted, observed, precision):
    members = predicted.shape[1]
    centre = lax.optimization_barrier(jnp.mean(predicted, axis=1, keepdims=True))
    spread = predicted - centre
    weighted = spread * precision[:, None]
    misfit = observed[:, None] - predicted
    gram_part = jnp.dot(spread.T, weighted, precision=lax.Precision.HIGHEST) / members
    cross_part = jnp.dot(weighted.T, misfit, precision=lax.Precision.HIGHEST) / jnp.sqrt(jnp.float32(members))
    return (gram_part, cross_part)

def solve_weights(gram_part, cross_part):
    members = gram_part.shape[0]
    system = jnp.eye(members, dtype=jnp.float32) + gram_part
    factor = jnp.linalg.cholesky(system)
    weights = jax.scipy.linalg.cho_solve((factor, True), cross_part) / jnp.sqrt(jnp.float32(members))
    return weights - lax.optimization_barrier(jnp.mean(weights, axis=0, keepdims=True))

def reference(parameters, initial_height, initial_speed, obs_slots, obs_values, obs_precision):
    owners = N_LAT * N_LON
    members = parameters.shape[1]
    owner_ids = jnp.arange(owners, dtype=jnp.int32)[:, None, None]
    for iteration in range(ITERS):
        height = forward(parameters, initial_height, initial_speed)
        cells = obs_slots[iteration]
        local = jnp.maximum(cells, 0)
        grid_row = owner_ids // N_LON * CLAT + local // CLON
        grid_col = owner_ids % N_LON * CLON + local % CLON
        global_ids = jnp.transpose(grid_row * NLON + grid_col, (1, 0, 2)).reshape(-1).astype(jnp.int32)
        live = jnp.transpose(cells >= 0, (1, 0, 2)).reshape(-1)
        flattened = height.reshape(members, -1)
        predicted = jnp.take(flattened, global_ids, axis=1).T
        predicted = jnp.where(live[:, None], predicted, jnp.float32(0.0))
        observed = obs_values[iteration].reshape(-1)
        precision = obs_precision[iteration].reshape(-1)
        gram_part, cross_part = gram_terms(predicted, observed, precision)
        centred = solve_weights(gram_part, cross_part)
        stacked = parameters.reshape(2, members, -1)
        increment = jnp.einsum('pjc,jm->pmc', stacked, centred, precision=lax.Precision.HIGHEST)
        parameters = parameters + increment.reshape(parameters.shape)
    return parameters
```

```python
import math

import functools

import jax
import jax.numpy as jnp
from jax import lax
from jax.experimental import pallas as pl
from jax.experimental.pallas import tpu as pltpu
from jax.sharding import PartitionSpec as P

STEPS = 6
ITERS = 2


depth_step = 0.7
gravity_step = 0.7
coriolis = 0.1


def padded_2(value, sides, width, wrap):
    for axis, dim in sides:
        peers, length = (lax.axis_size(axis), value.shape[dim])
        up = [(i, (i + 1) % peers) for i in range(peers if wrap else peers - 1)]
        down = [(j, i) for i, j in up]
        last = lax.slice_in_dim(value, length - width, length, axis=dim)
        leading = lax.slice_in_dim(value, 0, width, axis=dim)
        before = lax.ppermute(last, axis, up)
        after = lax.ppermute(leading, axis, down)
        value = jnp.concatenate([before, value, after], axis=dim)
    return value


def wall_rows(padded):
    row_count = padded.shape[-2]
    position = lax.axis_index("lat")
    last_block = lax.axis_size("lat") - 1
    row_ids = lax.broadcasted_iota(jnp.int32, (row_count, 1), 0)
    lower_wall = jnp.logical_and(row_ids == 0, position == 0)
    upper_wall = jnp.logical_and(row_ids == row_count - 1, position == last_block)
    keep_rows = jnp.logical_not(jnp.logical_or(lower_wall, upper_wall))
    return padded * keep_rows.astype(padded.dtype)


def advance(height, speeds, friction, forcing):
    east_padded = padded_2(speeds[0], (("lon", 2),), 1, True)
    north_padded = padded_2(speeds[1], (("lat", 1),), 1, False)
    east_diff = east_padded[:, :, 2:] - east_padded[:, :, :-2]
    north_diff = north_padded[:, 2:, :] - north_padded[:, :-2, :]
    height = height - depth_step * (east_diff + north_diff) + forcing
    padded_height = padded_2(height, (("lat", 1), ("lon", 2)), 1, True)
    padded_height = wall_rows(padded_height)
    slope_east = padded_height[:, 1:-1, 2:] - padded_height[:, 1:-1, :-2]
    slope_north = padded_height[:, 2:, 1:-1] - padded_height[:, :-2, 1:-1]
    eastward = (1.0 - friction) * speeds[0] - gravity_step * slope_east + coriolis * speeds[1]
    northward = (1.0 - friction) * speeds[1] - gravity_step * slope_north - coriolis * speeds[0]
    return (height, jnp.stack([eastward, northward]))


def forward(parameters, initial_height, initial_speed):
    members = parameters.shape[1]
    height = jnp.broadcast_to(initial_height, (members,) + initial_height.shape)
    speeds = jnp.broadcast_to(initial_speed[:, None], (2, members) + initial_height.shape)
    for substep in range(STEPS):
        height, speeds = advance(height, speeds, parameters[0], parameters[1])
    return height


def predict(height, cells):
    flattened = height.reshape(height.shape[0], -1)
    wanted = cells.reshape(-1)
    picked = jnp.take(flattened, jnp.clip(wanted, 0, flattened.shape[1] - 1), axis=1)
    picked = jnp.where(wanted[None, :] >= 0, picked, jnp.float32(0.0))
    return picked.T.reshape(cells.shape[0], -1)


def gram_terms(predicted, observed, precision):
    members = predicted.shape[1]
    centre = jnp.mean(predicted, axis=1, keepdims=True)
    spread = predicted - centre
    weighted = spread * precision[:, None]
    misfit = observed[:, None] - predicted
    gram_part = jnp.dot(spread.T, weighted, precision=lax.Precision.HIGHEST) / members
    cross_part = jnp.dot(weighted.T, misfit, precision=lax.Precision.HIGHEST) / math.sqrt(members)
    return (gram_part, cross_part)


def solve_weights(gram_part, cross_part):
    members = gram_part.shape[0]
    system = jnp.eye(members, dtype=jnp.float32) + gram_part
    factor = jnp.linalg.cholesky(system)
    weights = jax.scipy.linalg.cho_solve((factor, True), cross_part) / math.sqrt(members)
    return weights - jnp.mean(weights, axis=0, keepdims=True)


def per_device_halo(parameters, initial_height, initial_speed, obs_slots, obs_values, obs_precision):
    owners = obs_slots.shape[2]
    slot_count = obs_slots.shape[3]
    members_here = parameters.shape[1]
    member_block = lax.axis_index("ens")
    owner_values, owner_precision = (
        lax.all_to_all(obs_values[:, 0], ("lat", "lon"), split_axis=1, concat_axis=1, tiled=True),
        lax.all_to_all(
            obs_precision[:, 0], ("lat", "lon"), split_axis=1, concat_axis=1, tiled=True
        ),
    )
    for iteration in range(ITERS):
        height = forward(parameters, initial_height, initial_speed)
        outgoing = predict(height, obs_slots[iteration, 0])
        received = outgoing
        observed = owner_values[iteration]
        precision = owner_precision[iteration]
        received = received.reshape(owners, slot_count, members_here)
        gathered = lax.all_gather(received, "ens", axis=2, tiled=True)
        members = gathered.shape[2]
        gram_part, cross_part = gram_terms(
            gathered.reshape(-1, members), observed.reshape(-1), precision.reshape(-1)
        )
        gram_part, cross_part = lax.psum((gram_part, cross_part), ("lat", "lon"))
        centred = solve_weights(gram_part, cross_part)
        local_weights = lax.dynamic_slice_in_dim(
            centred, member_block * members_here, members_here, 1
        )
        starting = jnp.zeros(
            (2, members_here, parameters.shape[2] * parameters.shape[3]), jnp.float32
        )
        pieces = lax.all_gather(parameters, "ens", axis=1, tiled=True)
        stacked = pieces.reshape(pieces.shape[0], pieces.shape[1], -1)
        increment = starting + jnp.einsum(
            "pjc,jm->pmc", stacked, local_weights, precision=lax.Precision.HIGHEST
        )
        parameters = parameters + increment.reshape(parameters.shape)
    return parameters


MESH = pl.DeviceIdType.MESH
VMEM = pltpu.VMEM
EDGE = 16
SUB = 8
CHUNK = 4


def east(field):
    width, axis = (field.shape[-1], field.ndim - 1)
    return pltpu.roll(field, width - 1, axis) - pltpu.roll(field, 1, axis)


def north(field, first_row, last_row):
    height = field.shape[0]
    after = jnp.where(last_row, 0.0, pltpu.roll(field, height - 1, 0))
    before = jnp.where(first_row, 0.0, pltpu.roll(field, 1, 0))
    return after - before


def flat_line(block, width):
    depth, count = block.shape
    lanes = lax.broadcasted_iota(jnp.int32, (count, width), 1)
    slots = lax.broadcasted_iota(jnp.int32, (count, width), 0)
    spread_out = jnp.dot(
        block,
        (lax.rem(lanes, count) == slots).astype(jnp.float32),
        precision=lax.Precision.HIGHEST,
        preferred_element_type=jnp.float32,
    )
    owners = lax.broadcasted_iota(jnp.int32, (depth, width), 0)
    groups = lax.broadcasted_iota(jnp.int32, (depth, width), 1) // count
    return jnp.sum(jnp.where(owners == groups, spread_out, 0.0), axis=0, keepdims=True)


def each(start, count, body):
    def step(i, carry):
        body(i)
        return carry

    lax.fori_loop(start, count, step, 0)


def send(src, dst, send_sem, recv_sem, device):
    return pltpu.make_async_remote_copy(
        src_ref=src,
        dst_ref=dst,
        send_sem=send_sem,
        recv_sem=recv_sem,
        device_id=device,
        device_id_type=MESH,
    )


def run_group(k, got, start, height, speed_e, speed_n):
    rows = start.shape[1]
    chunks = [pl.ds(c, CHUNK) for c in range(0, rows, CHUNK)]
    upper = [pl.ds(c + 2, CHUNK) for c in range(0, rows, CHUNK)]
    inner = [pl.ds(c + 1, CHUNK) for c in range(0, rows, CHUNK)]

    def new_speeds(n, keep, old_e, old_n):
        slope_e = east(height[inner[n]])
        slope_n = height[upper[n]] - height[chunks[n]]
        speed_e[chunks[n]] = keep * old_e - gravity_step * slope_e + coriolis * old_n
        speed_n[inner[n]] = keep * old_n - gravity_step * slope_n - coriolis * old_e

    def new_height():
        for n in range(len(chunks)):
            flow = east(speed_e[chunks[n]]) + (speed_n[upper[n]] - speed_n[chunks[n]])
            height[inner[n]] = height[inner[n]] - depth_step * flow + got[k, 1, chunks[n]]

    for n in range(len(chunks)):
        height[inner[n]] = start[0, chunks[n]] + got[k, 1, chunks[n]]
    for n in range(len(chunks)):
        keep = 1.0 - got[k, 0, chunks[n]]
        got[k, 0, chunks[n]] = keep
        new_speeds(n, keep, start[1, chunks[n]], start[2, chunks[n]])

    def middle(step, carry):
        new_height()
        for n in range(len(chunks)):
            new_speeds(n, got[k, 0, chunks[n]], speed_e[chunks[n]], speed_n[inner[n]])
        return carry

    lax.fori_loop(1, STEPS - 1, middle, 0)
    new_height()


def ensemble_kernel(iteration, n_lat, n_lon, n_ens, *refs):
    first = iteration == 0
    if first:
        params, start_height, start_speed, slots_in, values_in, precision_in = refs[:6]
        gx, other, own, fields, cells, info = refs[6:12]
        aux, lin, fin, send_a, recv_a, send_l, recv_l = refs[12:19]
        refs = refs[19:]
    else:
        own, fields, cells, info, gx, other = refs[:6]
        refs = refs[6:]
    (got, edges, goth, start, height, speed_e, speed_n) = refs[:7]
    (outgoing, arrived, part, partner_part, half_sum, halves) = refs[7:13]
    (send_p, recv_p, send_h, recv_h, send_o, recv_o) = refs[13:19]
    (send_y, recv_y, send_x, recv_x, send_z, recv_z) = refs[19:]
    lat, lon, ens = (lax.axis_index("lat"), lax.axis_index("lon"), lax.axis_index("ens"))
    blocks = n_lat * n_lon
    me = lat * n_lon + lon
    column = n_lat * n_ens
    here = ens * n_lat + lat
    rows, cols = fields.shape[1] // n_lat, got.shape[-1] // 2
    groups_here = got.shape[0]
    groups = n_lat * groups_here
    share = n_lat // n_ens

    def at(lat_to, lon_to, ens_to):
        return {"lat": lat_to, "lon": lon_to, "ens": ens_to}

    def same_column(flat):
        return at(lax.rem(flat, n_lat), lon, flat // n_lat)

    def same_core(block):
        return at(block // n_lon, lax.rem(block, n_lon), ens)

    def east_of(d):
        return lax.rem(lon + d + n_lon, n_lon)

    barrier = pltpu.get_barrier_semaphore()

    def greet(device):
        pl.semaphore_signal(barrier, inc=1, device_id=device, device_id_type=MESH)

    each(1, blocks, lambda i: greet(same_core(lax.rem(me + i, blocks))))
    each(0, n_lat, lambda i: greet(at(i, lon, 1 - ens)))
    lane = lax.broadcasted_iota(jnp.int32, (SUB, cols), 1)

    if first:
        for g in range(groups):
            for p in range(2):
                for r in range(rows):
                    own[g, p, r] = params[p, g * SUB : (g + 1) * SUB, r, :]
        lines = []
        for ref in (slots_in, values_in, precision_in):
            for t in range(ITERS):
                lines.append(flat_line(ref[t, 0].astype(jnp.float32), cols))
        lines.append(jnp.zeros((rows - len(lines), cols), jnp.float32))
        aux[0] = start_height[...]
        aux[1] = start_speed[0]
        aux[2] = start_speed[1]
        aux[3] = jnp.concatenate(lines, axis=0)

    def pack_edges(g):
        for p in range(2):
            left = jnp.zeros((SUB, cols), jnp.float32)
            right = left
            for r in range(rows):
                tile = own[g, p, r]
                here_lanes = lane // EDGE == r
                left = jnp.where(here_lanes, pltpu.roll(tile, EDGE * r, 1), left)
                shift = (EDGE * r + EDGE) % cols
                right = jnp.where(here_lanes, pltpu.roll(tile, shift, 1), right)
            edges[0, g, p] = left
            edges[1, g, p] = right

    for g in range(groups):
        pack_edges(g)
    zero_row = jnp.zeros((1, SUB, 2 * cols), jnp.float32)
    for ref in (height, speed_n):
        ref[0:1] = zero_row
        ref[ref.shape[0] - 1 : ref.shape[0]] = zero_row
    pl.semaphore_wait(barrier, blocks - 1 + n_lat)

    def field_copy(i, d):
        return send(
            aux.at[0:3],
            fin.at[d % 3, lat],
            send_a.at[i, d % 3],
            recv_a.at[i, d % 3],
            at(lax.rem(lat + i, n_lat), east_of(-d), ens),
        )

    def line_copy(i):
        return send(
            aux.at[3],
            lin.at[me],
            send_l.at[i],
            recv_l.at[i],
            same_core(lax.rem(me + i, blocks)),
        )

    def param_copy(k, i):
        to = lax.rem(lat + i, n_lat)
        return send(
            own.at[to * groups_here + k],
            got.at[k, :, pl.ds(lat * rows, rows), :, pl.ds(0, cols)],
            send_p.at[k, i],
            recv_p.at[k, i],
            at(to, lon, ens),
        )

    def edge_copy(k, i, side):
        to = lax.rem(lat + i, n_lat)
        return send(
            edges.at[side, to * groups_here + k],
            goth.at[k, lat, side],
            send_h.at[k, i, side],
            recv_h.at[k, i, side],
            at(to, east_of(2 * side - 1), ens),
        )

    swap = send(own, other, send_o.at[0], recv_o.at[0], at(lat, lon, 1 - ens))

    if first:
        each(1, n_lat, lambda i: field_copy(i, 0).start())
        for d in (1, -1):
            each(0, n_lat, lambda i: field_copy(i, d).start())
    for k in range(groups_here):
        each(1, n_lat, lambda i: param_copy(k, i).start())
        for side in range(2):
            each(0, n_lat, lambda i: edge_copy(k, i, side).start())
        if first and k == 0:
            each(1, blocks, lambda i: line_copy(i).start())
    swap.start()

    own_rows = pl.ds(lat * rows, rows)
    for k in range(groups_here):
        got[k, :, own_rows, :, 0:cols] = own[lat * groups_here + k]

    if first:
        for i in range(3):
            fin[0, pl.ds(lat, 1), i] = aux[i : i + 1]
        lin[pl.ds(me, 1)] = aux[3:4]
        each(1, n_lat, lambda i: field_copy(i, 0).wait())
        for d in (1, -1):
            each(0, n_lat, lambda i: field_copy(i, d).wait())

        def whole(i):
            lines = []
            for a in range(n_lat):
                after, before = (fin[1, a, i], fin[2, a, i])
                outer = jnp.where(
                    lane < EDGE, after, jnp.where(lane >= cols - EDGE, before, 0.0)
                )
                lines.append(jnp.concatenate([fin[0, a, i], outer], axis=1))
            return jnp.concatenate(lines, axis=0)

        row_ids = lax.broadcasted_iota(jnp.int32, fields.shape[1:], 0)
        first_row, last_row = (row_ids == 0, row_ids == fields.shape[1] - 1)
        speed_e0, speed_n0 = (whole(1), whole(2))
        flow = east(speed_e0) + north(speed_n0, first_row, last_row)
        fields[0] = whole(0) - depth_step * flow
        fields[1] = speed_e0
        fields[2] = speed_n0

    for i in range(3):
        for r in range(fields.shape[1]):
            start[i, r] = jnp.broadcast_to(fields[i, r : r + 1, :], (SUB, 2 * cols))

    if first:
        each(1, blocks, lambda i: line_copy(i).wait())
        for t in range(ITERS):
            for a in range(n_lat):
                line = lin[a * n_lon + lon][t : t + 1].astype(jnp.int32)
                cells[t * n_lat + a : t * n_lat + a + 1] = line
        slots = cols // blocks
        heard = jnp.concatenate([lin[b] for b in range(blocks)], axis=0)
        kinds = lin.shape[1]
        square = (heard.shape[1], cols)
        from_ids = lax.broadcasted_iota(jnp.int32, square, 0)
        to_ids = lax.broadcasted_iota(jnp.int32, square, 1)
        line_ids = lax.broadcasted_iota(jnp.int32, heard.shape, 0)
        lane_ids = lax.broadcasted_iota(jnp.int32, heard.shape, 1)
        info[...] = jnp.zeros(info.shape, jnp.float32)
        for j in range(share):
            owner = (ens * share + j) * n_lon + lon
            chosen = from_ids == owner * slots + lax.rem(to_ids, slots)
            spread_out = jnp.dot(
                heard,
                chosen.astype(jnp.float32),
                precision=lax.Precision.HIGHEST,
                preferred_element_type=jnp.float32,
            )
            for kind in range(2 * ITERS):
                wanted = line_ids == (lane_ids // slots) * kinds + ITERS + kind
                info[kind : kind + 1, j * cols : (j + 1) * cols] = jnp.sum(
                    jnp.where(wanted, spread_out, 0.0), axis=0, keepdims=True
                )

    def answer_copy(k, i):
        to = lax.rem(here + i, column)
        part_rows = pl.ds(k * SUB, SUB)
        return send(
            outgoing.at[pl.ds((to // n_lat) * share, share), part_rows],
            arrived.at[:, here, part_rows],
            send_y.at[k, i],
            recv_y.at[k, i],
            same_column(to),
        )

    def group(k, carry):
        each(1, n_lat, lambda i: param_copy(k, i).wait())
        for side in range(2):
            each(0, n_lat, lambda i: edge_copy(k, i, side).wait())
        for a in range(n_lat):
            for p in range(2):
                after, before = (goth[k, a, 0, p], goth[k, a, 1, p])
                for r in range(rows):
                    shift = (cols - EDGE * r) % cols
                    right = pltpu.roll(after, shift, 1)
                    left = pltpu.roll(before, (shift + cols - EDGE) % cols, 1)
                    got[k, p, a * rows + r, :, cols : 2 * cols] = jnp.where(
                        lane < EDGE, right, jnp.where(lane >= cols - EDGE, left, 0.0)
                    )
        run_group(k, got, start, height, speed_e, speed_n)
        for a in range(n_lat):
            line = iteration * n_lat + a
            wanted = jnp.broadcast_to(cells[line : line + 1], (SUB, cols))
            lanes = jnp.bitwise_and(wanted, cols - 1)
            where_row = jnp.right_shift(wanted, cols.bit_length() - 1)
            found = jnp.zeros((SUB, cols), jnp.float32)
            for r in range(rows):
                tile = height[a * rows + r + 1, :, 0:cols]
                picked = jnp.take_along_axis(tile, lanes, axis=1)
                found = jnp.where(where_row == r, picked, found)
            outgoing[a, pl.ds(k * SUB, SUB)] = found
        each(1, column, lambda i: answer_copy(k, i).start())
        return carry

    lax.fori_loop(0, groups_here, group, 0)
    for j in range(share):
        arrived[j, pl.ds(here, 1)] = outgoing[pl.ds(ens * share + j, 1)]
    for k in range(groups_here):
        each(1, column, lambda i: answer_copy(k, i).wait())

    members = column * arrived.shape[2]
    predicted = jnp.concatenate(
        [
            jnp.concatenate([arrived[j, s] for s in range(column)], axis=0)
            for j in range(share)
        ],
        axis=1,
    )
    observed = info[iteration : iteration + 1]
    precision = info[ITERS + iteration : ITERS + iteration + 1]
    centre = jnp.sum(predicted, axis=0, keepdims=True) / members
    spread = predicted - centre
    weighted = spread * precision
    extra = lax.broadcasted_iota(jnp.int32, (SUB, share * cols), 0) == 0
    extra = jnp.where(extra, jnp.broadcast_to(observed - centre, extra.shape), 0.0)
    product = lax.dot_general(
        jnp.concatenate([spread, extra], axis=0),
        weighted,
        (((1,), (1,)), ((), ())),
        precision=lax.Precision.HIGHEST,
        preferred_element_type=jnp.float32,
    )
    lines = members // n_ens
    for e in range(n_ens):
        part[e, 0:lines] = product[e * lines : (e + 1) * lines]
        part[e, lines:] = product[members:]

    partner = at(lat, lon, 1 - ens)
    trade = send(part.at[1 - ens], partner_part, send_x.at[0], recv_x.at[0], partner)
    trade.start()
    trade.wait()
    half_sum[...] = part[ens] + partner_part[...]

    def half_copy(i):
        return send(
            half_sum, halves.at[lon], send_z.at[i], recv_z.at[i], at(lat, east_of(i), ens)
        )

    each(1, n_lon, lambda i: half_copy(i).start())
    halves[lon] = half_sum[...]
    each(1, n_lon, lambda i: half_copy(i).wait())
    total = halves[0]
    for b in range(1, n_lon):
        total = total + halves[b]
    part[ens] = total
    finish = send(part.at[ens], gx.at[ens], send_x.at[1], recv_x.at[1], partner)
    finish.start()
    gx[ens] = total
    finish.wait()
    swap.wait()


def ensemble_call(iteration, sizes, own_shape, *operands):
    n_lat, n_lon, n_ens = sizes
    blocks = n_lat * n_lon
    column = n_lat * n_ens
    groups, _, rows, _, cols = own_shape
    groups_here = groups // n_lat
    members = groups * SUB * n_ens
    share = n_lat // n_ens
    all_rows = n_lat * rows
    lines = members // n_ens + SUB
    f32 = jnp.float32
    dma = pltpu.SemaphoreType.DMA
    first = iteration == 0
    outs = [
        jax.ShapeDtypeStruct((n_ens, lines, members), f32),
        jax.ShapeDtypeStruct(own_shape, f32),
    ]
    scratch = []
    if first:
        outs += [
            jax.ShapeDtypeStruct(own_shape, f32),
            jax.ShapeDtypeStruct((3, all_rows, 2 * cols), f32),
            jax.ShapeDtypeStruct((ITERS * n_lat, cols), jnp.int32),
            jax.ShapeDtypeStruct((SUB, share * cols), f32),
        ]
        scratch += [
            VMEM((4, rows, cols), f32),
            VMEM((blocks, rows, cols), f32),
            VMEM((3, n_lat, 3, rows, cols), f32),
            dma((n_lat, 3)),
            dma((n_lat, 3)),
            dma((blocks,)),
            dma((blocks,)),
        ]
    scratch += [
        VMEM((groups_here, 2, all_rows, SUB, 2 * cols), f32),
        VMEM((2, groups, 2, SUB, cols), f32),
        VMEM((groups_here, n_lat, 2, 2, SUB, cols), f32),
        VMEM((3, all_rows, SUB, 2 * cols), f32),
        VMEM((all_rows + 2, SUB, 2 * cols), f32),
        VMEM((all_rows, SUB, 2 * cols), f32),
        VMEM((all_rows + 2, SUB, 2 * cols), f32),
        VMEM((n_lat, groups_here * SUB, cols), f32),
        VMEM((share, column, groups_here * SUB, cols), f32),
        VMEM((n_ens, lines, members), f32),
        VMEM((lines, members), f32),
        VMEM((lines, members), f32),
        VMEM((n_lon, lines, members), f32),
        dma((groups_here, n_lat)),
        dma((groups_here, n_lat)),
        dma((groups_here, n_lat, 2)),
        dma((groups_here, n_lat, 2)),
        dma((1,)),
        dma((1,)),
        dma((groups_here, column)),
        dma((groups_here, column)),
        dma((2,)),
        dma((2,)),
        dma((n_lon,)),
        dma((n_lon,)),
    ]
    return pl.pallas_call(
        functools.partial(ensemble_kernel, iteration, n_lat, n_lon, n_ens),
        out_shape=outs,
        in_specs=[pl.BlockSpec(memory_space=VMEM)] * len(operands),
        out_specs=[pl.BlockSpec(memory_space=VMEM)] * len(outs),
        scratch_shapes=scratch,
        compiler_params=pltpu.CompilerParams(
            collective_id=iteration, has_side_effects=True, vmem_limit_bytes=40 * 2**20
        ),
    )(*operands)


def with_rows(value, rows, start):
    end = start + rows.shape[0]
    pieces = [value[:start]] if start else []
    pieces.append(rows)
    if end < value.shape[0]:
        pieces.append(value[end:])
    return jnp.concatenate(pieces, axis=0)


def inverse_below(matrix):
    size = matrix.shape[1]
    panel = SUB
    row_ids = lax.broadcasted_iota(jnp.int32, (panel, size), 0)
    lane_ids = lax.broadcasted_iota(jnp.int32, (panel, size), 1)
    all_lanes = lax.broadcasted_iota(jnp.int32, matrix.shape, 1)
    for start in range(0, size, panel):
        end = start + panel
        rows = matrix[start:end]
        columns = [
            jnp.broadcast_to(rows[:, start + k : start + k + 1], (panel, size))
            for k in range(panel)
        ]
        inside = jnp.logical_and(lane_ids >= start, lane_ids < end)
        rows = jnp.where(inside, (lane_ids - start == row_ids).astype(jnp.float32), rows)
        for k in range(panel):
            column = columns[k]
            inverse = 1.0 / column[k : k + 1]
            here = row_ids == k

            def reduce(value):
                pivot_row = value[k : k + 1] * inverse
                return jnp.where(here, pivot_row, value - column * pivot_row)

            rows = reduce(rows)
            for later in range(k + 1, panel):
                columns[later] = reduce(columns[later])
        after = jnp.where(
            jnp.logical_and(all_lanes >= start, all_lanes < end), 0.0, matrix
        )
        for k in range(panel):
            after = after - matrix[:, start + k : start + k + 1] * rows[k : k + 1]
        matrix = with_rows(after, rows, start)
    return matrix


def update_kernel(gx, own, other, out):
    ens = lax.axis_index("ens")
    groups, _, rows, _, cols = own.shape
    members = gx.shape[2]
    lines = gx.shape[1] - SUB
    gram = jnp.concatenate([gx[e, 0:lines] for e in range(gx.shape[0])], axis=0)
    ids = [lax.broadcasted_iota(jnp.int32, gram.shape, axis) for axis in (0, 1)]
    unit = (ids[0] == ids[1]).astype(jnp.float32)
    swept = inverse_below(jnp.concatenate([gram / members + unit, gx[0, lines:]], axis=0))
    shift = swept[members : members + 1] / members
    weights = swept[:members] - unit - shift
    centred = weights - jnp.sum(weights, axis=1, keepdims=True) / members
    mine = jnp.where(ens == 0, centred[:lines], centred[lines:])
    mine = jnp.where(ens == 0, mine, pltpu.roll(mine, lines, 1))
    for p in range(2):
        for r in range(rows):
            local = jnp.concatenate([own[g, p, r] for g in range(groups)], axis=0)
            remote = jnp.concatenate([other[g, p, r] for g in range(groups)], axis=0)
            new = local + jnp.dot(
                mine,
                jnp.concatenate([local, remote], axis=0),
                precision=lax.Precision.HIGHEST,
                preferred_element_type=jnp.float32,
            )
            if len(out.shape) == 4:
                out[p, :, r, :] = new
            else:
                for g in range(groups):
                    out[g, p, r] = new[g * SUB : (g + 1) * SUB]


def update_call(shape, *operands):
    return pl.pallas_call(
        update_kernel,
        out_shape=jax.ShapeDtypeStruct(shape, jnp.float32),
        in_specs=[pl.BlockSpec(memory_space=VMEM)] * len(operands),
        out_specs=pl.BlockSpec(memory_space=VMEM),
        compiler_params=pltpu.CompilerParams(vmem_limit_bytes=40 * 2**20),
    )(*operands)


def per_device_columns(sizes, *arguments):
    shape = arguments[0].shape
    own_shape = (shape[1] // SUB, shape[0], shape[2], SUB, shape[3])
    gx, other, own, *known = ensemble_call(0, sizes, own_shape, *arguments)
    for iteration in range(1, ITERS):
        own = update_call(own_shape, gx, own, other)
        gx, other = ensemble_call(iteration, sizes, own_shape, own, *known)
    return update_call(shape, gx, own, other)


def by_members(sizes, parameters, initial_height, initial_speed, obs_slots, *rest):
    n_lat, n_lon, n_ens = sizes
    members_here, rows, cols = parameters.shape[1:]
    fits = (
        n_ens == 2
        and n_lat % n_ens == 0
        and n_lon >= 3
        and members_here % (SUB * n_lat) == 0
        and rows == SUB
        and members_here * n_ens == cols
        and cols == 128
        and EDGE * rows == cols
        and 2 * STEPS <= EDGE
        and ITERS * 3 <= rows
        and obs_slots.shape[2] * obs_slots.shape[3] == cols
    )
    arguments = (parameters, initial_height, initial_speed, obs_slots) + rest
    if fits:
        return per_device_columns(sizes, *arguments)
    return per_device_halo(*arguments)


def solution(mesh):
    placed = (
        P(None, "ens", "lat", "lon"),
        P("lat", "lon"),
        P(None, "lat", "lon"),
        P(None, ("lat", "lon"), None, None),
        P(None, ("lat", "lon"), None, None),
        P(None, ("lat", "lon"), None, None),
    )
    return jax.shard_map(
        functools.partial(by_members, tuple(mesh.shape[a] for a in ("lat", "lon", "ens"))),
        mesh=mesh,
        in_specs=placed,
        out_specs=P(None, "ens", "lat", "lon"),
        check_vma=False,
    )
```

```python
import math

import functools

import jax
import jax.numpy as jnp
from jax import lax
from jax.experimental import pallas as pl
from jax.experimental.pallas import tpu as pltpu
from jax.sharding import PartitionSpec as P

STEPS = 6
ITERS = 2


depth_step = 0.7
gravity_step = 0.7
coriolis = 0.1


def padded_2(value, sides, width, wrap):
    for axis, dim in sides:
        peers, length = (lax.axis_size(axis), value.shape[dim])
        up = [(i, (i + 1) % peers) for i in range(peers if wrap else peers - 1)]
        down = [(j, i) for i, j in up]
        last = lax.slice_in_dim(value, length - width, length, axis=dim)
        leading = lax.slice_in_dim(value, 0, width, axis=dim)
        before = lax.ppermute(last, axis, up)
        after = lax.ppermute(leading, axis, down)
        value = jnp.concatenate([before, value, after], axis=dim)
    return value


def wall_rows(padded):
    row_count = padded.shape[-2]
    position = lax.axis_index("lat")
    last_block = lax.axis_size("lat") - 1
    row_ids = lax.broadcasted_iota(jnp.int32, (row_count, 1), 0)
    lower_wall = jnp.logical_and(row_ids == 0, position == 0)
    upper_wall = jnp.logical_and(row_ids == row_count - 1, position == last_block)
    keep_rows = jnp.logical_not(jnp.logical_or(lower_wall, upper_wall))
    return padded * keep_rows.astype(padded.dtype)


def advance(height, speeds, friction, forcing):
    east_padded = padded_2(speeds[0], (("lon", 2),), 1, True)
    north_padded = padded_2(speeds[1], (("lat", 1),), 1, False)
    east_diff = east_padded[:, :, 2:] - east_padded[:, :, :-2]
    north_diff = north_padded[:, 2:, :] - north_padded[:, :-2, :]
    height = height - depth_step * (east_diff + north_diff) + forcing
    padded_height = padded_2(height, (("lat", 1), ("lon", 2)), 1, True)
    padded_height = wall_rows(padded_height)
    slope_east = padded_height[:, 1:-1, 2:] - padded_height[:, 1:-1, :-2]
    slope_north = padded_height[:, 2:, 1:-1] - padded_height[:, :-2, 1:-1]
    eastward = (1.0 - friction) * speeds[0] - gravity_step * slope_east + coriolis * speeds[1]
    northward = (1.0 - friction) * speeds[1] - gravity_step * slope_north - coriolis * speeds[0]
    return (height, jnp.stack([eastward, northward]))


def forward(parameters, initial_height, initial_speed):
    members = parameters.shape[1]
    height = jnp.broadcast_to(initial_height, (members,) + initial_height.shape)
    speeds = jnp.broadcast_to(initial_speed[:, None], (2, members) + initial_height.shape)
    for substep in range(STEPS):
        height, speeds = advance(height, speeds, parameters[0], parameters[1])
    return height


def predict(height, cells):
    flattened = height.reshape(height.shape[0], -1)
    wanted = cells.reshape(-1)
    picked = jnp.take(flattened, jnp.clip(wanted, 0, flattened.shape[1] - 1), axis=1)
    picked = jnp.where(wanted[None, :] >= 0, picked, jnp.float32(0.0))
    return picked.T.reshape(cells.shape[0], -1)


def gram_terms(predicted, observed, precision):
    members = predicted.shape[1]
    centre = jnp.mean(predicted, axis=1, keepdims=True)
    spread = predicted - centre
    weighted = spread * precision[:, None]
    misfit = observed[:, None] - predicted
    gram_part = jnp.dot(spread.T, weighted, precision=lax.Precision.HIGHEST) / members
    cross_part = jnp.dot(weighted.T, misfit, precision=lax.Precision.HIGHEST) / math.sqrt(members)
    return (gram_part, cross_part)


def solve_weights(gram_part, cross_part):
    members = gram_part.shape[0]
    system = jnp.eye(members, dtype=jnp.float32) + gram_part
    factor = jnp.linalg.cholesky(system)
    weights = jax.scipy.linalg.cho_solve((factor, True), cross_part) / math.sqrt(members)
    return weights - jnp.mean(weights, axis=0, keepdims=True)


def per_device_halo(parameters, initial_height, initial_speed, obs_slots, obs_values, obs_precision):
    owners = obs_slots.shape[2]
    slot_count = obs_slots.shape[3]
    members_here = parameters.shape[1]
    member_block = lax.axis_index("ens")
    owner_values, owner_precision = (
        lax.all_to_all(obs_values[:, 0], ("lat", "lon"), split_axis=1, concat_axis=1, tiled=True),
        lax.all_to_all(
            obs_precision[:, 0], ("lat", "lon"), split_axis=1, concat_axis=1, tiled=True
        ),
    )
    for iteration in range(ITERS):
        height = forward(parameters, initial_height, initial_speed)
        outgoing = predict(height, obs_slots[iteration, 0])
        received = outgoing
        observed = owner_values[iteration]
        precision = owner_precision[iteration]
        received = received.reshape(owners, slot_count, members_here)
        gathered = lax.all_gather(received, "ens", axis=2, tiled=True)
        members = gathered.shape[2]
        gram_part, cross_part = gram_terms(
            gathered.reshape(-1, members), observed.reshape(-1), precision.reshape(-1)
        )
        gram_part, cross_part = lax.psum((gram_part, cross_part), ("lat", "lon"))
        centred = solve_weights(gram_part, cross_part)
        local_weights = lax.dynamic_slice_in_dim(
            centred, member_block * members_here, members_here, 1
        )
        starting = jnp.zeros(
            (2, members_here, parameters.shape[2] * parameters.shape[3]), jnp.float32
        )
        pieces = lax.all_gather(parameters, "ens", axis=1, tiled=True)
        stacked = pieces.reshape(pieces.shape[0], pieces.shape[1], -1)
        increment = starting + jnp.einsum(
            "pjc,jm->pmc", stacked, local_weights, precision=lax.Precision.HIGHEST
        )
        parameters = parameters + increment.reshape(parameters.shape)
    return parameters


MESH = pl.DeviceIdType.MESH
VMEM = pltpu.VMEM
EDGE = 16
SUB = 8
CHUNK = 4
VMEM_LIMIT = 40 * 2**20


def east(field):
    width, axis = (field.shape[-1], field.ndim - 1)
    return pltpu.roll(field, width - 1, axis) - pltpu.roll(field, 1, axis)


def north(field, first_row, last_row):
    height = field.shape[0]
    after = jnp.where(last_row, 0.0, pltpu.roll(field, height - 1, 0))
    before = jnp.where(first_row, 0.0, pltpu.roll(field, 1, 0))
    return after - before


def flat_lines(blocks, width):
    count, groups = blocks[0].shape
    lanes = lax.broadcasted_iota(jnp.int32, (groups, width), 1)
    group_ids = lax.broadcasted_iota(jnp.int32, (groups, width), 0)
    spread_out = jnp.dot(
        jnp.concatenate(blocks, axis=0),
        (lanes // count == group_ids).astype(jnp.float32),
        precision=lax.Precision.HIGHEST,
        preferred_element_type=jnp.float32,
    )
    slots = lax.broadcasted_iota(jnp.int32, (count, width), 0)
    lanes = lax.broadcasted_iota(jnp.int32, (count, width), 1)
    keep = lax.rem(lanes, count) == slots
    lines = []
    for n in range(len(blocks)):
        block = spread_out[n * count : (n + 1) * count]
        lines.append(jnp.sum(jnp.where(keep, block, 0.0), axis=0, keepdims=True))
    return lines


def each(start, count, body):
    def step(i, carry):
        body(i)
        return carry

    lax.fori_loop(start, count, step, 0)


def send(src, dst, send_sem, recv_sem, device):
    return pltpu.make_async_remote_copy(
        src_ref=src,
        dst_ref=dst,
        send_sem=send_sem,
        recv_sem=recv_sem,
        device_id=device,
        device_id_type=MESH,
    )


def run_group(k, got, start, height, speed_e, speed_n):
    rows = start.shape[1]
    chunks = [pl.ds(c, CHUNK) for c in range(0, rows, CHUNK)]
    upper = [pl.ds(c + 2, CHUNK) for c in range(0, rows, CHUNK)]
    inner = [pl.ds(c + 1, CHUNK) for c in range(0, rows, CHUNK)]

    def new_speeds(n, keep, old_e, old_n):
        slope_e = east(height[inner[n]])
        slope_n = height[upper[n]] - height[chunks[n]]
        speed_e[chunks[n]] = keep * old_e - gravity_step * slope_e + coriolis * old_n
        speed_n[inner[n]] = keep * old_n - gravity_step * slope_n - coriolis * old_e

    def new_height():
        for n in range(len(chunks)):
            flow = east(speed_e[chunks[n]]) + (speed_n[upper[n]] - speed_n[chunks[n]])
            height[inner[n]] = height[inner[n]] - depth_step * flow + got[k, 1, chunks[n]]

    for n in range(len(chunks)):
        height[inner[n]] = start[0, chunks[n]] + got[k, 1, chunks[n]]
    for n in range(len(chunks)):
        keep = 1.0 - got[k, 0, chunks[n]]
        got[k, 0, chunks[n]] = keep
        new_speeds(n, keep, start[1, chunks[n]], start[2, chunks[n]])

    def middle(step, carry):
        new_height()
        for n in range(len(chunks)):
            new_speeds(n, got[k, 0, chunks[n]], speed_e[chunks[n]], speed_n[inner[n]])
        return carry

    lax.fori_loop(1, STEPS - 1, middle, 0)
    new_height()


def with_rows(value, rows, start):
    end = start + rows.shape[0]
    pieces = [value[:start]] if start else []
    pieces.append(rows)
    if end < value.shape[0]:
        pieces.append(value[end:])
    return jnp.concatenate(pieces, axis=0)


def inverse_below(matrix):
    size = matrix.shape[1]
    panel = SUB
    row_ids = lax.broadcasted_iota(jnp.int32, (panel, size), 0)
    lane_ids = lax.broadcasted_iota(jnp.int32, (panel, size), 1)
    all_lanes = lax.broadcasted_iota(jnp.int32, matrix.shape, 1)
    for start in range(0, size, panel):
        end = start + panel
        rows = matrix[start:end]
        columns = [
            jnp.broadcast_to(rows[:, start + k : start + k + 1], (panel, size))
            for k in range(panel)
        ]
        inside = jnp.logical_and(lane_ids >= start, lane_ids < end)
        rows = jnp.where(inside, (lane_ids - start == row_ids).astype(jnp.float32), rows)
        for k in range(panel):
            column = columns[k]
            inverse = 1.0 / column[k : k + 1]
            here = row_ids == k

            def reduce(value):
                pivot_row = value[k : k + 1] * inverse
                return jnp.where(here, pivot_row, value - column * pivot_row)

            rows = reduce(rows)
            for later in range(k + 1, panel):
                columns[later] = reduce(columns[later])
        after = jnp.where(
            jnp.logical_and(all_lanes >= start, all_lanes < end), 0.0, matrix
        )
        for k in range(panel):
            after = after - matrix[:, start + k : start + k + 1] * rows[k : k + 1]
        matrix = with_rows(after, rows, start)
    return matrix


def member_weights(gx, ens):
    members = gx.shape[2]
    lines = gx.shape[1] - SUB
    gram = jnp.concatenate([gx[e, 0:lines] for e in range(gx.shape[0])], axis=0)
    ids = [lax.broadcasted_iota(jnp.int32, gram.shape, axis) for axis in (0, 1)]
    unit = (ids[0] == ids[1]).astype(jnp.float32)
    swept = inverse_below(jnp.concatenate([gram / members + unit, gx[0, lines:]], axis=0))
    shift = swept[members : members + 1] / members
    weights = swept[:members] - unit - shift
    centred = weights - jnp.sum(weights, axis=1, keepdims=True) / members
    mine = jnp.where(ens == 0, centred[:lines], centred[lines:])
    return jnp.where(ens == 0, mine, pltpu.roll(mine, lines, 1))


def updated_rows(mine, own, other, store):
    groups, _, rows, _, cols = own.shape
    for p in range(2):
        for r in range(0, rows, 2):
            pair, local = ([], [])
            for q in (r, r + 1):
                local.append(jnp.concatenate([own[g, p, q] for g in range(groups)], axis=0))
                remote = [other[g, p, q] for g in range(groups)]
                pair.append(jnp.concatenate([local[-1]] + remote, axis=0))
            added = jnp.dot(
                mine,
                jnp.concatenate(pair, axis=1),
                precision=lax.Precision.HIGHEST,
                preferred_element_type=jnp.float32,
            )
            for q in range(2):
                store(p, r + q, local[q] + added[:, q * cols : (q + 1) * cols])


def ensemble_kernel(n_lat, n_lon, n_ens, *refs):
    params, start_height, start_speed, slots_in, values_in, precision_in = refs[:6]
    gx_out, own_out, other_out = refs[6:9]
    owns, others, gxs, aux, lin, fin, slots_here, values_here, precision_here = refs[9:18]
    cells, info, start, height, speed_e, speed_n = refs[18:24]
    gots, edges, goths, outgoing, arriveds, part, partner_parts, half_sum, halves_all = refs[24:33]
    load, send_a, recv_a, send_l, recv_l, send_p, recv_p, send_h, recv_h = refs[33:42]
    send_o, recv_o, send_y, recv_y, send_x, recv_x, send_z, recv_z = refs[42:]
    lat, lon, ens = (lax.axis_index("lat"), lax.axis_index("lon"), lax.axis_index("ens"))
    blocks = n_lat * n_lon
    me = lat * n_lon + lon
    column = n_lat * n_ens
    here = ens * n_lat + lat
    groups, _, rows, _, cols = own_out.shape
    all_rows = n_lat * rows
    groups_here = groups // n_lat
    share = n_lat // n_ens
    lane = lax.broadcasted_iota(jnp.int32, (SUB, cols), 1)
    own_rows = pl.ds(lat * rows, rows)

    def at(lat_to, lon_to, ens_to):
        return {"lat": lat_to, "lon": lon_to, "ens": ens_to}

    def same_column(flat):
        return at(lax.rem(flat, n_lat), lon, flat // n_lat)

    def same_core(block):
        return at(block // n_lon, lax.rem(block, n_lon), ens)

    def east_of(d):
        return lax.rem(lon + d + n_lon, n_lon)

    partner = at(lat, lon, 1 - ens)
    barrier = pltpu.get_barrier_semaphore()

    def greet(device):
        pl.semaphore_signal(barrier, inc=1, device_id=device, device_id_type=MESH)

    each(1, blocks, lambda i: greet(same_core(lax.rem(me + i, blocks))))
    each(0, n_lat, lambda i: greet(at(i, lon, 1 - ens)))

    small = [
        pltpu.make_async_copy(src, dst, load.at[n])
        for n, (src, dst) in enumerate(
            (
                (slots_in, slots_here),
                (values_in, values_here),
                (precision_in, precision_here),
                (start_height, aux.at[0]),
                (start_speed, aux.at[1:3]),
            )
        )
    ]
    large = [
        pltpu.make_async_copy(
            params.at[p, :, :, r, :], owns.at[0, :, p, r], load.at[len(small) + p * rows + r]
        )
        for p in range(2)
        for r in range(rows)
    ]
    for copy in small + large:
        copy.start()
    zero_row = jnp.zeros((1, SUB, 2 * cols), jnp.float32)
    for ref in (height, speed_n):
        ref[0:1] = zero_row
        ref[all_rows + 1 : all_rows + 2] = zero_row
    info[...] = jnp.zeros(info.shape, jnp.float32)
    for copy in small:
        copy.wait()
    lines = flat_lines(
        [
            ref[t, 0].astype(jnp.float32)
            for ref in (slots_here, values_here, precision_here)
            for t in range(ITERS)
        ],
        cols,
    )
    lines.append(jnp.zeros((rows - len(lines), cols), jnp.float32))
    aux[3] = jnp.concatenate(lines, axis=0)
    for copy in large:
        copy.wait()

    def field_copy(i, d):
        return send(
            aux.at[0:3],
            fin.at[d % 3, lat],
            send_a.at[i, d % 3],
            recv_a.at[i, d % 3],
            at(lax.rem(lat + i, n_lat), east_of(-d), ens),
        )

    def line_copy(i):
        return send(
            aux.at[3],
            lin.at[me],
            send_l.at[i],
            recv_l.at[i],
            same_core(lax.rem(me + i, blocks)),
        )

    def run_iteration(t, own, other, gx):
        got, goth, arrived = (gots.at[t], goths.at[t], arriveds.at[t])
        partner_part, halves = (partner_parts.at[t], halves_all.at[t])

        def param_copy(k, i):
            to = lax.rem(lat + i, n_lat)
            return send(
                own.at[to * groups_here + k],
                got.at[k, :, own_rows, :, pl.ds(0, cols)],
                send_p.at[t, k, i],
                recv_p.at[t, k, i],
                at(to, lon, ens),
            )

        def edge_copy(k, i, side):
            to = lax.rem(lat + i, n_lat)
            return send(
                edges.at[side, to * groups_here + k],
                goth.at[k, lat, side],
                send_h.at[t, k, i, side],
                recv_h.at[t, k, i, side],
                at(to, east_of(2 * side - 1), ens),
            )

        swap = send(own, other, send_o.at[t], recv_o.at[t], partner)

        def pack_edges(g):
            for p in range(2):
                left = jnp.zeros((SUB, cols), jnp.float32)
                right = left
                for r in range(rows):
                    tile = own[g, p, r]
                    here_lanes = lane // EDGE == r
                    left = jnp.where(here_lanes, pltpu.roll(tile, EDGE * r, 1), left)
                    shift = (EDGE * r + EDGE) % cols
                    right = jnp.where(here_lanes, pltpu.roll(tile, shift, 1), right)
                edges[0, g, p] = left
                edges[1, g, p] = right

        if t == 0:
            for g in range(groups):
                pack_edges(g)
            pl.semaphore_wait(barrier, blocks - 1 + n_lat)
            each(1, n_lat, lambda i: field_copy(i, 0).start())
            for d in (1, -1):
                each(0, n_lat, lambda i: field_copy(i, d).start())
        for k in range(groups_here):
            each(1, n_lat, lambda i: param_copy(k, i).start())
            if t and k == 0:
                for g in range(groups):
                    pack_edges(g)
            for side in range(2):
                each(0, n_lat, lambda i: edge_copy(k, i, side).start())
            if t == 0 and k == 0:
                each(1, blocks, lambda i: line_copy(i).start())
        swap.start()
        for k in range(groups_here):
            got[k, :, own_rows, :, 0:cols] = own[lat * groups_here + k]

        if t == 0:
            for i in range(3):
                fin[0, pl.ds(lat, 1), i] = aux[i : i + 1]
            lin[pl.ds(me, 1)] = aux[3:4]
            each(1, n_lat, lambda i: field_copy(i, 0).wait())
            for d in (1, -1):
                each(0, n_lat, lambda i: field_copy(i, d).wait())

            def whole(i):
                lines = []
                for a in range(n_lat):
                    after, before = (fin[1, a, i], fin[2, a, i])
                    outer = jnp.where(
                        lane < EDGE, after, jnp.where(lane >= cols - EDGE, before, 0.0)
                    )
                    lines.append(jnp.concatenate([fin[0, a, i], outer], axis=1))
                return jnp.concatenate(lines, axis=0)

            row_ids = lax.broadcasted_iota(jnp.int32, (all_rows, 2 * cols), 0)
            first_row, last_row = (row_ids == 0, row_ids == all_rows - 1)
            speed_e0, speed_n0 = (whole(1), whole(2))
            flow = east(speed_e0) + north(speed_n0, first_row, last_row)
            for i, field in enumerate((whole(0) - depth_step * flow, speed_e0, speed_n0)):
                for r in range(all_rows):
                    start[i, r] = jnp.broadcast_to(field[r : r + 1], (SUB, 2 * cols))
            each(1, blocks, lambda i: line_copy(i).wait())
            for n in range(ITERS):
                for a in range(n_lat):
                    line = lin[a * n_lon + lon][n : n + 1].astype(jnp.int32)
                    cells[n * n_lat + a : n * n_lat + a + 1] = line

        def answer_copy(k, i):
            to = lax.rem(here + i, column)
            part_rows = pl.ds(k * SUB, SUB)
            return send(
                outgoing.at[pl.ds((to // n_lat) * share, share), part_rows],
                arrived.at[:, here, part_rows],
                send_y.at[t, k, i],
                recv_y.at[t, k, i],
                same_column(to),
            )

        def group(k, carry):
            each(1, n_lat, lambda i: param_copy(k, i).wait())
            for side in range(2):
                each(0, n_lat, lambda i: edge_copy(k, i, side).wait())
            for a in range(n_lat):
                for p in range(2):
                    after, before = (goth[k, a, 0, p], goth[k, a, 1, p])
                    for r in range(rows):
                        shift = (cols - EDGE * r) % cols
                        right = pltpu.roll(after, shift, 1)
                        left = pltpu.roll(before, (shift + cols - EDGE) % cols, 1)
                        got[k, p, a * rows + r, :, cols : 2 * cols] = jnp.where(
                            lane < EDGE, right, jnp.where(lane >= cols - EDGE, left, 0.0)
                        )
            run_group(k, got, start, height, speed_e, speed_n)
            for a in range(n_lat):
                line = t * n_lat + a
                wanted = jnp.broadcast_to(cells[line : line + 1], (SUB, cols))
                lanes = jnp.bitwise_and(wanted, cols - 1)
                where_row = jnp.right_shift(wanted, cols.bit_length() - 1)
                found = jnp.zeros((SUB, cols), jnp.float32)
                for r in range(rows):
                    tile = height[a * rows + r + 1, :, 0:cols]
                    picked = jnp.take_along_axis(tile, lanes, axis=1)
                    found = jnp.where(where_row == r, picked, found)
                outgoing[a, pl.ds(k * SUB, SUB)] = found
            each(1, column, lambda i: answer_copy(k, i).start())
            return carry

        lax.fori_loop(0, groups_here, group, 0)
        for j in range(share):
            arrived[j, pl.ds(here, 1)] = outgoing[pl.ds(ens * share + j, 1)]
        if t == 0:
            slots = cols // blocks
            heard = jnp.concatenate([lin[b] for b in range(blocks)], axis=0)
            kinds = lin.shape[1]
            square = (heard.shape[1], cols)
            from_ids = lax.broadcasted_iota(jnp.int32, square, 0)
            to_ids = lax.broadcasted_iota(jnp.int32, square, 1)
            line_ids = lax.broadcasted_iota(jnp.int32, heard.shape, 0)
            lane_ids = lax.broadcasted_iota(jnp.int32, heard.shape, 1)
            for j in range(share):
                owner = (ens * share + j) * n_lon + lon
                chosen = from_ids == owner * slots + lax.rem(to_ids, slots)
                spread_out = jnp.dot(
                    heard,
                    chosen.astype(jnp.float32),
                    precision=lax.Precision.HIGHEST,
                    preferred_element_type=jnp.float32,
                )
                for kind in range(2 * ITERS):
                    wanted = line_ids == (lane_ids // slots) * kinds + ITERS + kind
                    info[kind : kind + 1, j * cols : (j + 1) * cols] = jnp.sum(
                        jnp.where(wanted, spread_out, 0.0), axis=0, keepdims=True
                    )
        for k in range(groups_here):
            each(1, column, lambda i: answer_copy(k, i).wait())

        members = column * arrived.shape[2]
        predicted = jnp.concatenate(
            [
                jnp.concatenate([arrived[j, s] for s in range(column)], axis=0)
                for j in range(share)
            ],
            axis=1,
        )
        observed = info[t : t + 1]
        precision = info[ITERS + t : ITERS + t + 1]
        centre = jnp.sum(predicted, axis=0, keepdims=True) / members
        spread = predicted - centre
        weighted = spread * precision
        extra = lax.broadcasted_iota(jnp.int32, (SUB, share * cols), 0) == 0
        extra = jnp.where(extra, jnp.broadcast_to(observed - centre, extra.shape), 0.0)
        product = lax.dot_general(
            jnp.concatenate([spread, extra], axis=0),
            weighted,
            (((1,), (1,)), ((), ())),
            precision=lax.Precision.HIGHEST,
            preferred_element_type=jnp.float32,
        )
        lines = members // n_ens
        for e in range(n_ens):
            part[e, 0:lines] = product[e * lines : (e + 1) * lines]
            part[e, lines:] = product[members:]

        trade = send(part.at[1 - ens], partner_part, send_x.at[t, 0], recv_x.at[t, 0], partner)
        trade.start()
        trade.wait()
        half_sum[...] = part[ens] + partner_part[...]

        def half_copy(i):
            return send(
                half_sum,
                halves.at[lon],
                send_z.at[t, i],
                recv_z.at[t, i],
                at(lat, east_of(i), ens),
            )

        each(1, n_lon, lambda i: half_copy(i).start())
        halves[lon] = half_sum[...]
        each(1, n_lon, lambda i: half_copy(i).wait())
        total = halves[0]
        for b in range(1, n_lon):
            total = total + halves[b]
        half_sum[...] = total
        finish = send(half_sum, gx.at[ens], send_x.at[t, 1], recv_x.at[t, 1], partner)
        finish.start()
        gx[ens] = total
        swap.wait()
        finish.wait()

    for t in range(ITERS):
        last = t == ITERS - 1
        own = own_out if last and t else owns.at[t]
        other, gx = (other_out, gx_out) if last else (others.at[t], gxs.at[t])
        run_iteration(t, own, other, gx)
        if not last:
            new = own_out if t + 1 == ITERS - 1 else owns.at[t + 1]

            def store(p, r, value, new=new):
                for g in range(groups):
                    new[g, p, r] = value[g * SUB : (g + 1) * SUB]

            updated_rows(member_weights(gx, ens), own, other, store)


def ensemble_call(sizes, own_shape, *operands):
    n_lat, n_lon, n_ens = sizes
    blocks = n_lat * n_lon
    column = n_lat * n_ens
    groups, _, rows, _, cols = own_shape
    groups_here = groups // n_lat
    members = groups * SUB * n_ens
    share = n_lat // n_ens
    all_rows = n_lat * rows
    lines = members // n_ens + SUB
    f32 = jnp.float32
    dma = pltpu.SemaphoreType.DMA
    gx_shape = (n_ens, lines, members)
    outs = [jax.ShapeDtypeStruct(shape, f32) for shape in (gx_shape, own_shape, own_shape)]

    def both(shape):
        return [dma(shape), dma(shape)]

    scratch = [
        VMEM((max(ITERS - 1, 1),) + own_shape, f32),
        VMEM((max(ITERS - 1, 1),) + own_shape, f32),
        VMEM((max(ITERS - 1, 1),) + gx_shape, f32),
        VMEM((4, rows, cols), f32),
        VMEM((blocks, rows, cols), f32),
        VMEM((3, n_lat, 3, rows, cols), f32),
    ]
    scratch += [VMEM(obs.shape, obs.dtype) for obs in operands[3:]]
    scratch += [
        VMEM((ITERS * n_lat, cols), jnp.int32),
        VMEM((SUB, share * cols), f32),
        VMEM((3, all_rows, SUB, 2 * cols), f32),
        VMEM((all_rows + 2, SUB, 2 * cols), f32),
        VMEM((all_rows, SUB, 2 * cols), f32),
        VMEM((all_rows + 2, SUB, 2 * cols), f32),
        VMEM((ITERS, groups_here, 2, all_rows, SUB, 2 * cols), f32),
        VMEM((2, groups, 2, SUB, cols), f32),
        VMEM((ITERS, groups_here, n_lat, 2, 2, SUB, cols), f32),
        VMEM((n_lat, groups_here * SUB, cols), f32),
        VMEM((ITERS, share, column, groups_here * SUB, cols), f32),
        VMEM(gx_shape, f32),
        VMEM((ITERS, lines, members), f32),
        VMEM((lines, members), f32),
        VMEM((ITERS, n_lon, lines, members), f32),
        dma((5 + 2 * rows,)),
    ]
    for shape in (
        (n_lat, 3),
        (blocks,),
        (ITERS, groups_here, n_lat),
        (ITERS, groups_here, n_lat, 2),
        (ITERS,),
        (ITERS, groups_here, column),
        (ITERS, 2),
        (ITERS, n_lon),
    ):
        scratch += both(shape)
    return pl.pallas_call(
        functools.partial(ensemble_kernel, n_lat, n_lon, n_ens),
        out_shape=outs,
        in_specs=[pl.BlockSpec(memory_space=pltpu.HBM)] * len(operands),
        out_specs=[pl.BlockSpec(memory_space=VMEM)] * len(outs),
        scratch_shapes=scratch,
        compiler_params=pltpu.CompilerParams(
            collective_id=0, has_side_effects=True, vmem_limit_bytes=VMEM_LIMIT
        ),
    )(*operands)


def update_kernel(gx, own, other, out):
    def store(p, r, value):
        out[p, :, r, :] = value

    updated_rows(member_weights(gx, lax.axis_index("ens")), own, other, store)


def update_call(shape, *operands):
    return pl.pallas_call(
        update_kernel,
        out_shape=jax.ShapeDtypeStruct(shape, jnp.float32),
        in_specs=[pl.BlockSpec(memory_space=VMEM)] * len(operands),
        out_specs=pl.BlockSpec(memory_space=VMEM),
        compiler_params=pltpu.CompilerParams(vmem_limit_bytes=40 * 2**20),
    )(*operands)


def per_device_columns(sizes, parameters, initial_height, initial_speed, *observations):
    shape = parameters.shape
    own_shape = (shape[1] // SUB, shape[0], shape[2], SUB, shape[3])
    grouped = parameters.reshape(shape[0], shape[1] // SUB, SUB, shape[2], shape[3])
    turned = [jnp.transpose(obs, (0, 1, 3, 2)) for obs in observations]
    operands = [grouped, initial_height, initial_speed] + turned
    operands = [pltpu.with_memory_space_constraint(x, pltpu.HBM) for x in operands]
    gathered = ensemble_call(sizes, own_shape, *operands)
    return update_call(shape, *gathered)


def by_members(sizes, parameters, initial_height, initial_speed, obs_slots, *rest):
    n_lat, n_lon, n_ens = sizes
    members_here, rows, cols = parameters.shape[1:]
    fits = (
        n_ens == 2
        and n_lat % n_ens == 0
        and n_lon >= 3
        and members_here % (SUB * n_lat) == 0
        and rows == SUB
        and members_here * n_ens == cols
        and cols == 128
        and EDGE * rows == cols
        and 2 * STEPS <= EDGE
        and ITERS * 3 <= rows
        and obs_slots.shape[2] * obs_slots.shape[3] == cols
        and obs_slots.shape[3] == SUB
        and ITERS > 1
    )
    arguments = (parameters, initial_height, initial_speed, obs_slots) + rest
    if fits:
        return per_device_columns(sizes, *arguments)
    return per_device_halo(*arguments)


def solution(mesh):
    placed = (
        P(None, "ens", "lat", "lon"),
        P("lat", "lon"),
        P(None, "lat", "lon"),
        P(None, ("lat", "lon"), None, None),
        P(None, ("lat", "lon"), None, None),
        P(None, ("lat", "lon"), None, None),
    )
    return jax.shard_map(
        functools.partial(by_members, tuple(mesh.shape[a] for a in ("lat", "lon", "ens"))),
        mesh=mesh,
        in_specs=placed,
        out_specs=P(None, "ens", "lat", "lon"),
        check_vma=False,
    )
```

```python
import math

import functools

import jax
import jax.numpy as jnp
from jax import lax
from jax.experimental import pallas as pl
from jax.experimental.pallas import tpu as pltpu
from jax.sharding import PartitionSpec as P

STEPS = 6
ITERS = 2


depth_step = 0.7
gravity_step = 0.7
coriolis = 0.1


def padded_2(value, sides, width, wrap):
    for axis, dim in sides:
        peers, length = (lax.axis_size(axis), value.shape[dim])
        up = [(i, (i + 1) % peers) for i in range(peers if wrap else peers - 1)]
        down = [(j, i) for i, j in up]
        last = lax.slice_in_dim(value, length - width, length, axis=dim)
        leading = lax.slice_in_dim(value, 0, width, axis=dim)
        before = lax.ppermute(last, axis, up)
        after = lax.ppermute(leading, axis, down)
        value = jnp.concatenate([before, value, after], axis=dim)
    return value


def wall_rows(padded):
    row_count = padded.shape[-2]
    position = lax.axis_index("lat")
    last_block = lax.axis_size("lat") - 1
    row_ids = lax.broadcasted_iota(jnp.int32, (row_count, 1), 0)
    lower_wall = jnp.logical_and(row_ids == 0, position == 0)
    upper_wall = jnp.logical_and(row_ids == row_count - 1, position == last_block)
    keep_rows = jnp.logical_not(jnp.logical_or(lower_wall, upper_wall))
    return padded * keep_rows.astype(padded.dtype)


def advance(height, speeds, friction, forcing):
    east_padded = padded_2(speeds[0], (("lon", 2),), 1, True)
    north_padded = padded_2(speeds[1], (("lat", 1),), 1, False)
    east_diff = east_padded[:, :, 2:] - east_padded[:, :, :-2]
    north_diff = north_padded[:, 2:, :] - north_padded[:, :-2, :]
    height = height - depth_step * (east_diff + north_diff) + forcing
    padded_height = padded_2(height, (("lat", 1), ("lon", 2)), 1, True)
    padded_height = wall_rows(padded_height)
    slope_east = padded_height[:, 1:-1, 2:] - padded_height[:, 1:-1, :-2]
    slope_north = padded_height[:, 2:, 1:-1] - padded_height[:, :-2, 1:-1]
    eastward = (1.0 - friction) * speeds[0] - gravity_step * slope_east + coriolis * speeds[1]
    northward = (1.0 - friction) * speeds[1] - gravity_step * slope_north - coriolis * speeds[0]
    return (height, jnp.stack([eastward, northward]))


def forward(parameters, initial_height, initial_speed):
    members = parameters.shape[1]
    height = jnp.broadcast_to(initial_height, (members,) + initial_height.shape)
    speeds = jnp.broadcast_to(initial_speed[:, None], (2, members) + initial_height.shape)
    for substep in range(STEPS):
        height, speeds = advance(height, speeds, parameters[0], parameters[1])
    return height


def predict(height, cells):
    flattened = height.reshape(height.shape[0], -1)
    wanted = cells.reshape(-1)
    picked = jnp.take(flattened, jnp.clip(wanted, 0, flattened.shape[1] - 1), axis=1)
    picked = jnp.where(wanted[None, :] >= 0, picked, jnp.float32(0.0))
    return picked.T.reshape(cells.shape[0], -1)


def gram_terms(predicted, observed, precision):
    members = predicted.shape[1]
    centre = jnp.mean(predicted, axis=1, keepdims=True)
    spread = predicted - centre
    weighted = spread * precision[:, None]
    misfit = observed[:, None] - predicted
    gram_part = jnp.dot(spread.T, weighted, precision=lax.Precision.HIGHEST) / members
    cross_part = jnp.dot(weighted.T, misfit, precision=lax.Precision.HIGHEST) / math.sqrt(members)
    return (gram_part, cross_part)


def solve_weights(gram_part, cross_part):
    members = gram_part.shape[0]
    system = jnp.eye(members, dtype=jnp.float32) + gram_part
    factor = jnp.linalg.cholesky(system)
    weights = jax.scipy.linalg.cho_solve((factor, True), cross_part) / math.sqrt(members)
    return weights - jnp.mean(weights, axis=0, keepdims=True)


def per_device_halo(parameters, initial_height, initial_speed, obs_slots, obs_values, obs_precision):
    owners = obs_slots.shape[2]
    slot_count = obs_slots.shape[3]
    members_here = parameters.shape[1]
    member_block = lax.axis_index("ens")
    owner_values, owner_precision = (
        lax.all_to_all(obs_values[:, 0], ("lat", "lon"), split_axis=1, concat_axis=1, tiled=True),
        lax.all_to_all(
            obs_precision[:, 0], ("lat", "lon"), split_axis=1, concat_axis=1, tiled=True
        ),
    )
    for iteration in range(ITERS):
        height = forward(parameters, initial_height, initial_speed)
        outgoing = predict(height, obs_slots[iteration, 0])
        received = outgoing
        observed = owner_values[iteration]
        precision = owner_precision[iteration]
        received = received.reshape(owners, slot_count, members_here)
        gathered = lax.all_gather(received, "ens", axis=2, tiled=True)
        members = gathered.shape[2]
        gram_part, cross_part = gram_terms(
            gathered.reshape(-1, members), observed.reshape(-1), precision.reshape(-1)
        )
        gram_part, cross_part = lax.psum((gram_part, cross_part), ("lat", "lon"))
        centred = solve_weights(gram_part, cross_part)
        local_weights = lax.dynamic_slice_in_dim(
            centred, member_block * members_here, members_here, 1
        )
        starting = jnp.zeros(
            (2, members_here, parameters.shape[2] * parameters.shape[3]), jnp.float32
        )
        pieces = lax.all_gather(parameters, "ens", axis=1, tiled=True)
        stacked = pieces.reshape(pieces.shape[0], pieces.shape[1], -1)
        increment = starting + jnp.einsum(
            "pjc,jm->pmc", stacked, local_weights, precision=lax.Precision.HIGHEST
        )
        parameters = parameters + increment.reshape(parameters.shape)
    return parameters


MESH = pl.DeviceIdType.MESH
VMEM = pltpu.VMEM
EDGE = 16
SUB = 8
CHUNK = 4
VMEM_LIMIT = 40 * 2**20


def east(field):
    width, axis = (field.shape[-1], field.ndim - 1)
    return pltpu.roll(field, width - 1, axis) - pltpu.roll(field, 1, axis)


def north(field, first_row, last_row):
    height = field.shape[0]
    after = jnp.where(last_row, 0.0, pltpu.roll(field, height - 1, 0))
    before = jnp.where(first_row, 0.0, pltpu.roll(field, 1, 0))
    return after - before


def flat_lines(blocks, width):
    count, groups = blocks[0].shape
    lanes = lax.broadcasted_iota(jnp.int32, (groups, width), 1)
    group_ids = lax.broadcasted_iota(jnp.int32, (groups, width), 0)
    spread_out = jnp.dot(
        jnp.concatenate(blocks, axis=0),
        (lanes // count == group_ids).astype(jnp.float32),
        precision=lax.Precision.HIGHEST,
        preferred_element_type=jnp.float32,
    )
    slots = lax.broadcasted_iota(jnp.int32, (count, width), 0)
    lanes = lax.broadcasted_iota(jnp.int32, (count, width), 1)
    keep = lax.rem(lanes, count) == slots
    lines = []
    for n in range(len(blocks)):
        block = spread_out[n * count : (n + 1) * count]
        lines.append(jnp.sum(jnp.where(keep, block, 0.0), axis=0, keepdims=True))
    return lines


def each(start, count, body):
    def step(i, carry):
        body(i)
        return carry

    lax.fori_loop(start, count, step, 0)


def send(src, dst, send_sem, recv_sem, device):
    return pltpu.make_async_remote_copy(
        src_ref=src,
        dst_ref=dst,
        send_sem=send_sem,
        recv_sem=recv_sem,
        device_id=device,
        device_id_type=MESH,
    )


def run_group(k, got, start, height, speed_e, speed_n):
    rows = start.shape[1]
    chunks = [pl.ds(c, CHUNK) for c in range(0, rows, CHUNK)]
    upper = [pl.ds(c + 2, CHUNK) for c in range(0, rows, CHUNK)]
    inner = [pl.ds(c + 1, CHUNK) for c in range(0, rows, CHUNK)]

    def new_speeds(n, keep, old_e, old_n):
        slope_e = east(height[inner[n]])
        slope_n = height[upper[n]] - height[chunks[n]]
        speed_e[chunks[n]] = keep * old_e - gravity_step * slope_e + coriolis * old_n
        speed_n[inner[n]] = keep * old_n - gravity_step * slope_n - coriolis * old_e

    def new_height():
        for n in range(len(chunks)):
            flow = east(speed_e[chunks[n]]) + (speed_n[upper[n]] - speed_n[chunks[n]])
            height[inner[n]] = height[inner[n]] - depth_step * flow + got[k, 1, chunks[n]]

    for n in range(len(chunks)):
        height[inner[n]] = start[0, chunks[n]] + got[k, 1, chunks[n]]
    for n in range(len(chunks)):
        keep = 1.0 - got[k, 0, chunks[n]]
        got[k, 0, chunks[n]] = keep
        new_speeds(n, keep, start[1, chunks[n]], start[2, chunks[n]])

    def middle(step, carry):
        new_height()
        for n in range(len(chunks)):
            new_speeds(n, got[k, 0, chunks[n]], speed_e[chunks[n]], speed_n[inner[n]])
        return carry

    lax.fori_loop(1, STEPS - 1, middle, 0)
    new_height()


def inverse_below(matrix):
    size = matrix.shape[1]
    strip = size // 2 // SUB
    row_ids = lax.broadcasted_iota(jnp.int32, (SUB, size), 0)
    lane_ids = lax.broadcasted_iota(jnp.int32, (SUB, size), 1)
    zero = jnp.zeros((SUB, size), jnp.float32)
    tiles = [matrix[n * SUB : (n + 1) * SUB] for n in range(matrix.shape[0] // SUB)]

    def columns_of(tile, start):
        return [
            jnp.broadcast_to(tile[:, start + k : start + k + 1], (SUB, size))
            for k in range(SUB)
        ]

    def less_rows(tile, band, columns, rows):
        tile = jnp.where(band, 0.0, tile)
        for k in range(SUB):
            tile = tile - columns[k] * rows[k : k + 1]
        return tile

    for base in range(0, size // SUB, strip):
        inner = tiles[base : base + strip]
        columns = columns_of(inner[0], base * SUB)
        for n in range(strip):
            start = (base + n) * SUB
            band = jnp.logical_and(lane_ids >= start, lane_ids < start + SUB)
            unit = (lane_ids - start == row_ids).astype(jnp.float32)
            rows = jnp.where(band, unit, inner[n])
            follows = n + 1 < strip
            ahead = []
            if follows:
                ahead = columns_of(inner[n], start + SUB)
                below = columns_of(inner[n + 1], start)
                later = columns_of(inner[n + 1], start + SUB)
            for k in range(SUB):
                column = columns[k]
                inverse = 1.0 / column[k : k + 1]
                here = row_ids == k

                def reduce(value):
                    pivot_row = value[k : k + 1] * inverse
                    return jnp.where(here, pivot_row, value - column * pivot_row)

                for other in range(k + 1, SUB):
                    columns[other] = reduce(columns[other])
                ahead = [reduce(value) for value in ahead]
                rows = reduce(rows)
            after = list(inner)
            after[n] = rows
            if follows:
                after[n + 1] = less_rows(inner[n + 1], band, below, rows)
                for k in range(SUB):
                    later = [
                        value - below[k] * line[k : k + 1] for value, line in zip(later, ahead)
                    ]
                columns = later
            for m in range(strip):
                if m != n and not (follows and m == n + 1):
                    after[m] = less_rows(inner[m], band, columns_of(inner[m], start), rows)
            inner = after
        outer = [m for m in range(len(tiles)) if not base <= m < base + strip]
        lines = [
            inner[m - base] if base <= m < base + strip else zero for m in range(size // SUB)
        ]
        product = jnp.dot(
            jnp.concatenate([tiles[m] for m in outer], axis=0),
            jnp.concatenate(lines, axis=0),
            precision=lax.Precision.HIGHEST,
            preferred_element_type=jnp.float32,
        )
        band = jnp.logical_and(lane_ids >= base * SUB, lane_ids < (base + strip) * SUB)
        for n, m in enumerate(outer):
            tiles[m] = jnp.where(band, 0.0, tiles[m]) - product[n * SUB : (n + 1) * SUB]
        tiles[base : base + strip] = inner
    return jnp.concatenate(tiles, axis=0)


def packed_halves(product, n_ens):
    half = product.shape[1] // 2
    row_ids = lax.broadcasted_iota(jnp.int32, (half, 2 * half), 0)
    lane_ids = lax.broadcasted_iota(jnp.int32, (half, 2 * half), 1)
    top, bottom = (product[0:half], product[half : 2 * half])
    dense = jnp.where(lane_ids <= row_ids + half, bottom, pltpu.roll(top, half, 1))
    diagonal = jnp.sum(jnp.where(lane_ids == row_ids, top, 0.0), axis=0, keepdims=True)
    tail = jnp.where(row_ids[0:SUB] == 1, diagonal, product[2 * half :])
    lines = half // n_ens
    return [
        jnp.concatenate([dense[e * lines : (e + 1) * lines], tail], axis=0)
        for e in range(n_ens)
    ]


def unpacked(parts):
    half = sum(part.shape[0] - SUB for part in parts)
    dense = jnp.concatenate([part[: part.shape[0] - SUB] for part in parts], axis=0)
    tail = parts[0][parts[0].shape[0] - SUB :]
    row_ids = lax.broadcasted_iota(jnp.int32, (half, 2 * half), 0)
    lane_ids = lax.broadcasted_iota(jnp.int32, (half, 2 * half), 1)
    turned = jnp.concatenate([dense, dense], axis=0).T
    upper = jnp.where(lane_ids > row_ids, pltpu.roll(dense, half, 1), turned[half:])
    upper = jnp.where(lane_ids == row_ids, tail[1:2], upper)
    top = jnp.where(lane_ids >= half, turned[:half], upper)
    bottom = jnp.where(lane_ids <= row_ids + half, dense, turned[half:])
    return jnp.concatenate([top, bottom], axis=0), tail[0:1]


def member_weights(gx, ens):
    members = gx.shape[2]
    half = members // 2
    gram, line = unpacked([gx[e] for e in range(gx.shape[0])])
    ids = [lax.broadcasted_iota(jnp.int32, gram.shape, axis) for axis in (0, 1)]
    unit = (ids[0] == ids[1]).astype(jnp.float32)
    line = jnp.broadcast_to(line, (SUB, members))
    swept = inverse_below(jnp.concatenate([gram / members + unit, line], axis=0))
    shift = swept[members : members + 1] / members
    weights = swept[:members] - unit - shift
    centred = weights - jnp.sum(weights, axis=1, keepdims=True) / members
    mine = jnp.where(ens == 0, centred[:half], centred[half:])
    return jnp.where(ens == 0, mine, pltpu.roll(mine, half, 1))


def updated_rows(mine, own, other, store):
    groups, _, rows, _, cols = own.shape
    for p in range(2):
        for r in range(0, rows, 2):
            pair, local = ([], [])
            for q in (r, r + 1):
                local.append(jnp.concatenate([own[g, p, q] for g in range(groups)], axis=0))
                remote = [other[g, p, q] for g in range(groups)]
                pair.append(jnp.concatenate([local[-1]] + remote, axis=0))
            added = jnp.dot(
                mine,
                jnp.concatenate(pair, axis=1),
                precision=lax.Precision.HIGHEST,
                preferred_element_type=jnp.float32,
            )
            for q in range(2):
                store(p, r + q, local[q] + added[:, q * cols : (q + 1) * cols])


def ensemble_kernel(n_lat, n_lon, n_ens, *refs):
    params, start_height, start_speed, slots_in, values_in, precision_in = refs[:6]
    gx_out, own_out, other_out = refs[6:9]
    owns, others, gxs, aux, lin, fin, slots_here, values_here, precision_here = refs[9:18]
    cells, info, start, height, speed_e, speed_n = refs[18:24]
    gots, edges, goths, outgoing, arriveds, part, partner_parts, half_sum, halves_all = refs[24:33]
    load, send_a, recv_a, send_l, recv_l, send_p, recv_p, send_h, recv_h = refs[33:42]
    send_o, recv_o, send_y, recv_y, send_x, recv_x, send_z, recv_z = refs[42:]
    lat, lon, ens = (lax.axis_index("lat"), lax.axis_index("lon"), lax.axis_index("ens"))
    blocks = n_lat * n_lon
    me = lat * n_lon + lon
    column = n_lat * n_ens
    here = ens * n_lat + lat
    groups, _, rows, _, cols = own_out.shape
    all_rows = n_lat * rows
    groups_here = groups // n_lat
    share = n_lat // n_ens
    lane = lax.broadcasted_iota(jnp.int32, (SUB, cols), 1)
    own_rows = pl.ds(lat * rows, rows)

    def at(lat_to, lon_to, ens_to):
        return {"lat": lat_to, "lon": lon_to, "ens": ens_to}

    def same_column(flat):
        return at(lax.rem(flat, n_lat), lon, flat // n_lat)

    def same_core(block):
        return at(block // n_lon, lax.rem(block, n_lon), ens)

    def east_of(d):
        return lax.rem(lon + d + n_lon, n_lon)

    partner = at(lat, lon, 1 - ens)
    barrier = pltpu.get_barrier_semaphore()

    def greet(device):
        pl.semaphore_signal(barrier, inc=1, device_id=device, device_id_type=MESH)

    each(1, blocks, lambda i: greet(same_core(lax.rem(me + i, blocks))))
    each(0, n_lat, lambda i: greet(at(i, lon, 1 - ens)))

    small = [
        pltpu.make_async_copy(src, dst, load.at[n])
        for n, (src, dst) in enumerate(
            (
                (slots_in, slots_here),
                (values_in, values_here),
                (precision_in, precision_here),
                (start_height, aux.at[0]),
                (start_speed, aux.at[1:3]),
            )
        )
    ]
    large = [
        pltpu.make_async_copy(
            params.at[p, :, :, r, :], owns.at[0, :, p, r], load.at[len(small) + p * rows + r]
        )
        for p in range(2)
        for r in range(rows)
    ]
    for copy in small + large:
        copy.start()
    zero_row = jnp.zeros((1, SUB, 2 * cols), jnp.float32)
    for ref in (height, speed_n):
        ref[0:1] = zero_row
        ref[all_rows + 1 : all_rows + 2] = zero_row
    info[...] = jnp.zeros(info.shape, jnp.float32)
    for copy in small:
        copy.wait()
    lines = flat_lines(
        [
            ref[t, 0].astype(jnp.float32)
            for ref in (slots_here, values_here, precision_here)
            for t in range(ITERS)
        ],
        cols,
    )
    lines.append(jnp.zeros((rows - len(lines), cols), jnp.float32))
    aux[3] = jnp.concatenate(lines, axis=0)
    for copy in large:
        copy.wait()

    def field_copy(i, d):
        return send(
            aux.at[0:3],
            fin.at[d % 3, lat],
            send_a.at[i, d % 3],
            recv_a.at[i, d % 3],
            at(lax.rem(lat + i, n_lat), east_of(-d), ens),
        )

    def line_copy(i):
        return send(
            aux.at[3],
            lin.at[me],
            send_l.at[i],
            recv_l.at[i],
            same_core(lax.rem(me + i, blocks)),
        )

    def run_iteration(t, own, other, gx):
        got, goth, arrived = (gots.at[t], goths.at[t], arriveds.at[t])
        partner_part, halves = (partner_parts.at[t], halves_all.at[t])

        def param_copy(k, i):
            to = lax.rem(lat + i, n_lat)
            return send(
                own.at[to * groups_here + k],
                got.at[k, :, own_rows, :, pl.ds(0, cols)],
                send_p.at[t, k, i],
                recv_p.at[t, k, i],
                at(to, lon, ens),
            )

        def edge_copy(k, i, side):
            to = lax.rem(lat + i, n_lat)
            return send(
                edges.at[side, to * groups_here + k],
                goth.at[k, lat, side],
                send_h.at[t, k, i, side],
                recv_h.at[t, k, i, side],
                at(to, east_of(2 * side - 1), ens),
            )

        swap = send(own, other, send_o.at[t], recv_o.at[t], partner)

        def pack_edges(g):
            for p in range(2):
                left = jnp.zeros((SUB, cols), jnp.float32)
                right = left
                for r in range(rows):
                    tile = own[g, p, r]
                    here_lanes = lane // EDGE == r
                    left = jnp.where(here_lanes, pltpu.roll(tile, EDGE * r, 1), left)
                    shift = (EDGE * r + EDGE) % cols
                    right = jnp.where(here_lanes, pltpu.roll(tile, shift, 1), right)
                edges[0, g, p] = left
                edges[1, g, p] = right

        if t == 0:
            for g in range(groups):
                pack_edges(g)
            pl.semaphore_wait(barrier, blocks - 1 + n_lat)
            each(1, n_lat, lambda i: field_copy(i, 0).start())
            for d in (1, -1):
                each(0, n_lat, lambda i: field_copy(i, d).start())
        for k in range(groups_here):
            each(1, n_lat, lambda i: param_copy(k, i).start())
            if t and k == 0:
                for g in range(groups):
                    pack_edges(g)
            for side in range(2):
                each(0, n_lat, lambda i: edge_copy(k, i, side).start())
            if t == 0 and k == 0:
                each(1, blocks, lambda i: line_copy(i).start())
        swap.start()
        for k in range(groups_here):
            got[k, :, own_rows, :, 0:cols] = own[lat * groups_here + k]

        if t == 0:
            for i in range(3):
                fin[0, pl.ds(lat, 1), i] = aux[i : i + 1]
            lin[pl.ds(me, 1)] = aux[3:4]
            each(1, n_lat, lambda i: field_copy(i, 0).wait())
            for d in (1, -1):
                each(0, n_lat, lambda i: field_copy(i, d).wait())

            def whole(i):
                lines = []
                for a in range(n_lat):
                    after, before = (fin[1, a, i], fin[2, a, i])
                    outer = jnp.where(
                        lane < EDGE, after, jnp.where(lane >= cols - EDGE, before, 0.0)
                    )
                    lines.append(jnp.concatenate([fin[0, a, i], outer], axis=1))
                return jnp.concatenate(lines, axis=0)

            row_ids = lax.broadcasted_iota(jnp.int32, (all_rows, 2 * cols), 0)
            first_row, last_row = (row_ids == 0, row_ids == all_rows - 1)
            speed_e0, speed_n0 = (whole(1), whole(2))
            flow = east(speed_e0) + north(speed_n0, first_row, last_row)
            for i, field in enumerate((whole(0) - depth_step * flow, speed_e0, speed_n0)):
                for r in range(all_rows):
                    start[i, r] = jnp.broadcast_to(field[r : r + 1], (SUB, 2 * cols))
            each(1, blocks, lambda i: line_copy(i).wait())
            for n in range(ITERS):
                for a in range(n_lat):
                    line = lin[a * n_lon + lon][n : n + 1].astype(jnp.int32)
                    cells[n * n_lat + a : n * n_lat + a + 1] = line

        def answer_copy(k, i):
            to = lax.rem(here + i, column)
            part_rows = pl.ds(k * SUB, SUB)
            return send(
                outgoing.at[pl.ds((to // n_lat) * share, share), part_rows],
                arrived.at[:, here, part_rows],
                send_y.at[t, k, i],
                recv_y.at[t, k, i],
                same_column(to),
            )

        def group(k, carry):
            each(1, n_lat, lambda i: param_copy(k, i).wait())
            for side in range(2):
                each(0, n_lat, lambda i: edge_copy(k, i, side).wait())
            for a in range(n_lat):
                for p in range(2):
                    after, before = (goth[k, a, 0, p], goth[k, a, 1, p])
                    for r in range(rows):
                        shift = (cols - EDGE * r) % cols
                        right = pltpu.roll(after, shift, 1)
                        left = pltpu.roll(before, (shift + cols - EDGE) % cols, 1)
                        got[k, p, a * rows + r, :, cols : 2 * cols] = jnp.where(
                            lane < EDGE, right, jnp.where(lane >= cols - EDGE, left, 0.0)
                        )
            run_group(k, got, start, height, speed_e, speed_n)
            for a in range(n_lat):
                line = t * n_lat + a
                wanted = jnp.broadcast_to(cells[line : line + 1], (SUB, cols))
                lanes = jnp.bitwise_and(wanted, cols - 1)
                where_row = jnp.right_shift(wanted, cols.bit_length() - 1)
                found = jnp.zeros((SUB, cols), jnp.float32)
                for r in range(rows):
                    tile = height[a * rows + r + 1, :, 0:cols]
                    picked = jnp.take_along_axis(tile, lanes, axis=1)
                    found = jnp.where(where_row == r, picked, found)
                outgoing[a, pl.ds(k * SUB, SUB)] = found
            each(1, column, lambda i: answer_copy(k, i).start())
            return carry

        lax.fori_loop(0, groups_here, group, 0)
        for j in range(share):
            arrived[j, pl.ds(here, 1)] = outgoing[pl.ds(ens * share + j, 1)]
        if t == 0:
            slots = cols // blocks
            heard = jnp.concatenate([lin[b] for b in range(blocks)], axis=0)
            kinds = lin.shape[1]
            square = (heard.shape[1], cols)
            from_ids = lax.broadcasted_iota(jnp.int32, square, 0)
            to_ids = lax.broadcasted_iota(jnp.int32, square, 1)
            line_ids = lax.broadcasted_iota(jnp.int32, heard.shape, 0)
            lane_ids = lax.broadcasted_iota(jnp.int32, heard.shape, 1)
            for j in range(share):
                owner = (ens * share + j) * n_lon + lon
                chosen = from_ids == owner * slots + lax.rem(to_ids, slots)
                spread_out = jnp.dot(
                    heard,
                    chosen.astype(jnp.float32),
                    precision=lax.Precision.HIGHEST,
                    preferred_element_type=jnp.float32,
                )
                for kind in range(2 * ITERS):
                    wanted = line_ids == (lane_ids // slots) * kinds + ITERS + kind
                    info[kind : kind + 1, j * cols : (j + 1) * cols] = jnp.sum(
                        jnp.where(wanted, spread_out, 0.0), axis=0, keepdims=True
                    )
        for k in range(groups_here):
            each(1, column, lambda i: answer_copy(k, i).wait())

        members = column * arrived.shape[2]
        predicted = jnp.concatenate(
            [
                jnp.concatenate([arrived[j, s] for s in range(column)], axis=0)
                for j in range(share)
            ],
            axis=1,
        )
        observed = info[t : t + 1]
        precision = info[ITERS + t : ITERS + t + 1]
        centre = jnp.sum(predicted, axis=0, keepdims=True) / members
        spread = predicted - centre
        weighted = spread * precision
        extra = lax.broadcasted_iota(jnp.int32, (SUB, share * cols), 0) == 0
        extra = jnp.where(extra, jnp.broadcast_to(observed - centre, extra.shape), 0.0)
        product = lax.dot_general(
            jnp.concatenate([spread, extra], axis=0),
            weighted,
            (((1,), (1,)), ((), ())),
            precision=lax.Precision.HIGHEST,
            preferred_element_type=jnp.float32,
        )
        for e, piece in enumerate(packed_halves(product, n_ens)):
            part[e] = piece

        trade = send(part.at[1 - ens], partner_part, send_x.at[t, 0], recv_x.at[t, 0], partner)
        trade.start()
        trade.wait()
        half_sum[...] = part[ens] + partner_part[...]

        def half_copy(i):
            return send(
                half_sum,
                halves.at[lon],
                send_z.at[t, i],
                recv_z.at[t, i],
                at(lat, east_of(i), ens),
            )

        each(1, n_lon, lambda i: half_copy(i).start())
        halves[lon] = half_sum[...]
        each(1, n_lon, lambda i: half_copy(i).wait())
        total = halves[0]
        for b in range(1, n_lon):
            total = total + halves[b]
        half_sum[...] = total
        finish = send(half_sum, gx.at[ens], send_x.at[t, 1], recv_x.at[t, 1], partner)
        finish.start()
        gx[ens] = total
        swap.wait()
        finish.wait()

    for t in range(ITERS):
        last = t == ITERS - 1
        own = own_out if last and t else owns.at[t]
        other, gx = (other_out, gx_out) if last else (others.at[t], gxs.at[t])
        run_iteration(t, own, other, gx)
        if not last:
            new = own_out if t + 1 == ITERS - 1 else owns.at[t + 1]

            def store(p, r, value, new=new):
                for g in range(groups):
                    new[g, p, r] = value[g * SUB : (g + 1) * SUB]

            updated_rows(member_weights(gx, ens), own, other, store)


def ensemble_call(sizes, own_shape, *operands):
    n_lat, n_lon, n_ens = sizes
    blocks = n_lat * n_lon
    column = n_lat * n_ens
    groups, _, rows, _, cols = own_shape
    groups_here = groups // n_lat
    members = groups * SUB * n_ens
    share = n_lat // n_ens
    all_rows = n_lat * rows
    lines = members // 2 // n_ens + SUB
    f32 = jnp.float32
    dma = pltpu.SemaphoreType.DMA
    gx_shape = (n_ens, lines, members)
    outs = [jax.ShapeDtypeStruct(shape, f32) for shape in (gx_shape, own_shape, own_shape)]

    def both(shape):
        return [dma(shape), dma(shape)]

    scratch = [
        VMEM((max(ITERS - 1, 1),) + own_shape, f32),
        VMEM((max(ITERS - 1, 1),) + own_shape, f32),
        VMEM((max(ITERS - 1, 1),) + gx_shape, f32),
        VMEM((4, rows, cols), f32),
        VMEM((blocks, rows, cols), f32),
        VMEM((3, n_lat, 3, rows, cols), f32),
    ]
    scratch += [VMEM(obs.shape, obs.dtype) for obs in operands[3:]]
    scratch += [
        VMEM((ITERS * n_lat, cols), jnp.int32),
        VMEM((SUB, share * cols), f32),
        VMEM((3, all_rows, SUB, 2 * cols), f32),
        VMEM((all_rows + 2, SUB, 2 * cols), f32),
        VMEM((all_rows, SUB, 2 * cols), f32),
        VMEM((all_rows + 2, SUB, 2 * cols), f32),
        VMEM((ITERS, groups_here, 2, all_rows, SUB, 2 * cols), f32),
        VMEM((2, groups, 2, SUB, cols), f32),
        VMEM((ITERS, groups_here, n_lat, 2, 2, SUB, cols), f32),
        VMEM((n_lat, groups_here * SUB, cols), f32),
        VMEM((ITERS, share, column, groups_here * SUB, cols), f32),
        VMEM(gx_shape, f32),
        VMEM((ITERS, lines, members), f32),
        VMEM((lines, members), f32),
        VMEM((ITERS, n_lon, lines, members), f32),
        dma((5 + 2 * rows,)),
    ]
    for shape in (
        (n_lat, 3),
        (blocks,),
        (ITERS, groups_here, n_lat),
        (ITERS, groups_here, n_lat, 2),
        (ITERS,),
        (ITERS, groups_here, column),
        (ITERS, 2),
        (ITERS, n_lon),
    ):
        scratch += both(shape)
    return pl.pallas_call(
        functools.partial(ensemble_kernel, n_lat, n_lon, n_ens),
        out_shape=outs,
        in_specs=[pl.BlockSpec(memory_space=pltpu.HBM)] * len(operands),
        out_specs=[pl.BlockSpec(memory_space=VMEM)] * len(outs),
        scratch_shapes=scratch,
        compiler_params=pltpu.CompilerParams(
            collective_id=0, has_side_effects=True, vmem_limit_bytes=VMEM_LIMIT
        ),
    )(*operands)


def update_kernel(gx, own, other, out, new, sems):
    copies = [pltpu.make_async_copy(new.at[p], out.at[p], sems.at[p]) for p in range(2)]
    rows = own.shape[2]

    def store(p, r, value):
        new[p, :, r, :] = value
        if r == rows - 1:
            copies[p].start()

    updated_rows(member_weights(gx, lax.axis_index("ens")), own, other, store)
    for copy in copies:
        copy.wait()


def update_call(shape, *operands):
    return pl.pallas_call(
        update_kernel,
        out_shape=jax.ShapeDtypeStruct(shape, jnp.float32),
        in_specs=[pl.BlockSpec(memory_space=VMEM)] * len(operands),
        out_specs=pl.BlockSpec(memory_space=pltpu.HBM),
        scratch_shapes=[VMEM(shape, jnp.float32), pltpu.SemaphoreType.DMA((2,))],
        compiler_params=pltpu.CompilerParams(vmem_limit_bytes=VMEM_LIMIT),
    )(*operands)


def per_device_columns(sizes, parameters, initial_height, initial_speed, *observations):
    shape = parameters.shape
    own_shape = (shape[1] // SUB, shape[0], shape[2], SUB, shape[3])
    grouped = parameters.reshape(shape[0], shape[1] // SUB, SUB, shape[2], shape[3])
    turned = [jnp.transpose(obs, (0, 1, 3, 2)) for obs in observations]
    operands = [grouped, initial_height, initial_speed] + turned
    operands = [pltpu.with_memory_space_constraint(x, pltpu.HBM) for x in operands]
    gathered = ensemble_call(sizes, own_shape, *operands)
    return update_call(shape, *gathered)


def by_members(sizes, parameters, initial_height, initial_speed, obs_slots, *rest):
    n_lat, n_lon, n_ens = sizes
    members_here, rows, cols = parameters.shape[1:]
    fits = (
        n_ens == 2
        and n_lat % n_ens == 0
        and n_lon >= 3
        and members_here % (SUB * n_lat) == 0
        and rows == SUB
        and members_here * n_ens == cols
        and cols == 128
        and EDGE * rows == cols
        and 2 * STEPS <= EDGE
        and ITERS * 3 <= rows
        and obs_slots.shape[2] * obs_slots.shape[3] == cols
        and obs_slots.shape[3] == SUB
        and ITERS > 1
    )
    arguments = (parameters, initial_height, initial_speed, obs_slots) + rest
    if fits:
        return per_device_columns(sizes, *arguments)
    return per_device_halo(*arguments)


def solution(mesh):
    placed = (
        P(None, "ens", "lat", "lon"),
        P("lat", "lon"),
        P(None, "lat", "lon"),
        P(None, ("lat", "lon"), None, None),
        P(None, ("lat", "lon"), None, None),
        P(None, ("lat", "lon"), None, None),
    )
    return jax.shard_map(
        functools.partial(by_members, tuple(mesh.shape[a] for a in ("lat", "lon", "ens"))),
        mesh=mesh,
        in_specs=placed,
        out_specs=P(None, "ens", "lat", "lon"),
        check_vma=False,
    )
```

```python
import math

import functools

import jax
import jax.numpy as jnp
from jax import lax
from jax.experimental import pallas as pl
from jax.experimental.pallas import tpu as pltpu
from jax.sharding import PartitionSpec as P

STEPS = 6
ITERS = 2


depth_step = 0.7
gravity_step = 0.7
coriolis = 0.1


def padded_2(value, sides, width, wrap):
    for axis, dim in sides:
        peers, length = (lax.axis_size(axis), value.shape[dim])
        up = [(i, (i + 1) % peers) for i in range(peers if wrap else peers - 1)]
        down = [(j, i) for i, j in up]
        last = lax.slice_in_dim(value, length - width, length, axis=dim)
        leading = lax.slice_in_dim(value, 0, width, axis=dim)
        before = lax.ppermute(last, axis, up)
        after = lax.ppermute(leading, axis, down)
        value = jnp.concatenate([before, value, after], axis=dim)
    return value


def wall_rows(padded):
    row_count = padded.shape[-2]
    position = lax.axis_index("lat")
    last_block = lax.axis_size("lat") - 1
    row_ids = lax.broadcasted_iota(jnp.int32, (row_count, 1), 0)
    lower_wall = jnp.logical_and(row_ids == 0, position == 0)
    upper_wall = jnp.logical_and(row_ids == row_count - 1, position == last_block)
    keep_rows = jnp.logical_not(jnp.logical_or(lower_wall, upper_wall))
    return padded * keep_rows.astype(padded.dtype)


def advance(height, speeds, friction, forcing):
    east_padded = padded_2(speeds[0], (("lon", 2),), 1, True)
    north_padded = padded_2(speeds[1], (("lat", 1),), 1, False)
    east_diff = east_padded[:, :, 2:] - east_padded[:, :, :-2]
    north_diff = north_padded[:, 2:, :] - north_padded[:, :-2, :]
    height = height - depth_step * (east_diff + north_diff) + forcing
    padded_height = padded_2(height, (("lat", 1), ("lon", 2)), 1, True)
    padded_height = wall_rows(padded_height)
    slope_east = padded_height[:, 1:-1, 2:] - padded_height[:, 1:-1, :-2]
    slope_north = padded_height[:, 2:, 1:-1] - padded_height[:, :-2, 1:-1]
    eastward = (1.0 - friction) * speeds[0] - gravity_step * slope_east + coriolis * speeds[1]
    northward = (1.0 - friction) * speeds[1] - gravity_step * slope_north - coriolis * speeds[0]
    return (height, jnp.stack([eastward, northward]))


def forward(parameters, initial_height, initial_speed):
    members = parameters.shape[1]
    height = jnp.broadcast_to(initial_height, (members,) + initial_height.shape)
    speeds = jnp.broadcast_to(initial_speed[:, None], (2, members) + initial_height.shape)
    for substep in range(STEPS):
        height, speeds = advance(height, speeds, parameters[0], parameters[1])
    return height


def predict(height, cells):
    flattened = height.reshape(height.shape[0], -1)
    wanted = cells.reshape(-1)
    picked = jnp.take(flattened, jnp.clip(wanted, 0, flattened.shape[1] - 1), axis=1)
    picked = jnp.where(wanted[None, :] >= 0, picked, jnp.float32(0.0))
    return picked.T.reshape(cells.shape[0], -1)


def gram_terms(predicted, observed, precision):
    members = predicted.shape[1]
    centre = jnp.mean(predicted, axis=1, keepdims=True)
    spread = predicted - centre
    weighted = spread * precision[:, None]
    misfit = observed[:, None] - predicted
    gram_part = jnp.dot(spread.T, weighted, precision=lax.Precision.HIGHEST) / members
    cross_part = jnp.dot(weighted.T, misfit, precision=lax.Precision.HIGHEST) / math.sqrt(members)
    return (gram_part, cross_part)


def solve_weights(gram_part, cross_part):
    members = gram_part.shape[0]
    system = jnp.eye(members, dtype=jnp.float32) + gram_part
    factor = jnp.linalg.cholesky(system)
    weights = jax.scipy.linalg.cho_solve((factor, True), cross_part) / math.sqrt(members)
    return weights - jnp.mean(weights, axis=0, keepdims=True)


def per_device_halo(parameters, initial_height, initial_speed, obs_slots, obs_values, obs_precision):
    owners = obs_slots.shape[2]
    slot_count = obs_slots.shape[3]
    members_here = parameters.shape[1]
    member_block = lax.axis_index("ens")
    owner_values, owner_precision = (
        lax.all_to_all(obs_values[:, 0], ("lat", "lon"), split_axis=1, concat_axis=1, tiled=True),
        lax.all_to_all(
            obs_precision[:, 0], ("lat", "lon"), split_axis=1, concat_axis=1, tiled=True
        ),
    )
    for iteration in range(ITERS):
        height = forward(parameters, initial_height, initial_speed)
        outgoing = predict(height, obs_slots[iteration, 0])
        received = outgoing
        observed = owner_values[iteration]
        precision = owner_precision[iteration]
        received = received.reshape(owners, slot_count, members_here)
        gathered = lax.all_gather(received, "ens", axis=2, tiled=True)
        members = gathered.shape[2]
        gram_part, cross_part = gram_terms(
            gathered.reshape(-1, members), observed.reshape(-1), precision.reshape(-1)
        )
        gram_part, cross_part = lax.psum((gram_part, cross_part), ("lat", "lon"))
        centred = solve_weights(gram_part, cross_part)
        local_weights = lax.dynamic_slice_in_dim(
            centred, member_block * members_here, members_here, 1
        )
        starting = jnp.zeros(
            (2, members_here, parameters.shape[2] * parameters.shape[3]), jnp.float32
        )
        pieces = lax.all_gather(parameters, "ens", axis=1, tiled=True)
        stacked = pieces.reshape(pieces.shape[0], pieces.shape[1], -1)
        increment = starting + jnp.einsum(
            "pjc,jm->pmc", stacked, local_weights, precision=lax.Precision.HIGHEST
        )
        parameters = parameters + increment.reshape(parameters.shape)
    return parameters


MESH = pl.DeviceIdType.MESH
VMEM = pltpu.VMEM
EDGE = 16
SUB = 8
CHUNK = 2
VMEM_LIMIT = 40 * 2**20


def segment_of(shape, tiles):
    lane = lax.broadcasted_iota(jnp.int32, shape, len(shape) - 1)
    width = shape[-1] // tiles
    return lax.rem(lane + width // 2, shape[-1]) // width


def east(field):
    tiles, cols = (field.shape[1] - 1, field.shape[3])
    width = cols // tiles
    lane = lax.broadcasted_iota(jnp.int32, field.shape[2:], 1)

    def moved(shift, seam):
        turned = pltpu.roll(field, shift % cols, 3)
        halo = turned[:, tiles]
        parts = []
        for a in range(tiles):
            here = lane == (a * width + seam) % cols
            parts.append(jnp.where(here, turned[:, tiles], turned[:, a]))
            halo = jnp.where(here, turned[:, a], halo)
        return parts + [halo]

    return jnp.stack(
        [after - before for after, before in zip(moved(-1, -1), moved(1, 0))], axis=1
    )


def set_edges(ref):
    tiles, cols = (ref.shape[1] - 1, ref.shape[3])
    width = cols // tiles
    segment = segment_of(ref.shape[2:], tiles)
    zero = jnp.zeros(ref.shape[2:], jnp.float32)
    first, last = (1, ref.shape[0] - 2)
    for a in range(tiles):
        ref[0, a] = pltpu.roll(ref[last, a - 1], width, 1) if a else zero
        ref[last + 1, a] = (
            pltpu.roll(ref[first, a + 1], cols - width, 1) if a + 1 < tiles else zero
        )
    ref[0, tiles] = jnp.where(segment == 0, 0.0, pltpu.roll(ref[last, tiles], width, 1))
    ref[last + 1, tiles] = jnp.where(
        segment == tiles - 1, 0.0, pltpu.roll(ref[first, tiles], cols - width, 1)
    )


def flat_lines(blocks, width):
    count, groups = blocks[0].shape
    lanes = lax.broadcasted_iota(jnp.int32, (groups, width), 1)
    group_ids = lax.broadcasted_iota(jnp.int32, (groups, width), 0)
    spread_out = jnp.dot(
        jnp.concatenate(blocks, axis=0),
        (lanes // count == group_ids).astype(jnp.float32),
        precision=lax.Precision.HIGHEST,
        preferred_element_type=jnp.float32,
    )
    slots = lax.broadcasted_iota(jnp.int32, (count, width), 0)
    lanes = lax.broadcasted_iota(jnp.int32, (count, width), 1)
    keep = lax.rem(lanes, count) == slots
    lines = []
    for n in range(len(blocks)):
        block = spread_out[n * count : (n + 1) * count]
        lines.append(jnp.sum(jnp.where(keep, block, 0.0), axis=0, keepdims=True))
    return lines


def send(src, dst, send_sem, recv_sem, device):
    return pltpu.make_async_remote_copy(
        src_ref=src,
        dst_ref=dst,
        send_sem=send_sem,
        recv_sem=recv_sem,
        device_id=device,
        device_id_type=MESH,
    )


def run_group(k, got, start, height, speed_e, speed_n):
    rows = start.shape[1]
    chunks = [pl.ds(c, CHUNK) for c in range(0, rows, CHUNK)]
    upper = [pl.ds(c + 2, CHUNK) for c in range(0, rows, CHUNK)]
    inner = [pl.ds(c + 1, CHUNK) for c in range(0, rows, CHUNK)]

    def new_speeds(n, keep, old_e, old_n):
        slope_e = east(height[inner[n]])
        slope_n = height[upper[n]] - height[chunks[n]]
        speed_e[chunks[n]] = keep * old_e - gravity_step * slope_e + coriolis * old_n
        speed_n[inner[n]] = keep * old_n - gravity_step * slope_n - coriolis * old_e

    def new_height():
        for n in range(len(chunks)):
            flow = east(speed_e[chunks[n]]) + (speed_n[upper[n]] - speed_n[chunks[n]])
            height[inner[n]] = height[inner[n]] - depth_step * flow + got[k, 1, chunks[n]]

    for n in range(len(chunks)):
        height[inner[n]] = start[0, chunks[n]] + got[k, 1, chunks[n]]
    set_edges(height)
    for n in range(len(chunks)):
        keep = 1.0 - got[k, 0, chunks[n]]
        got[k, 0, chunks[n]] = keep
        new_speeds(n, keep, start[1, chunks[n]], start[2, chunks[n]])
    set_edges(speed_n)

    def middle(step, carry):
        new_height()
        set_edges(height)
        for n in range(len(chunks)):
            new_speeds(n, got[k, 0, chunks[n]], speed_e[chunks[n]], speed_n[inner[n]])
        set_edges(speed_n)
        return carry

    lax.fori_loop(1, STEPS - 1, middle, 0)
    tiles = start.shape[2] - 1
    for n in range(len(chunks)):
        flow = east(speed_e[chunks[n]])[:, 0:tiles] + (
            speed_n[upper[n], 0:tiles] - speed_n[chunks[n], 0:tiles]
        )
        height[inner[n], 0:tiles] = (
            height[inner[n], 0:tiles] - depth_step * flow + got[k, 1, chunks[n], 0:tiles]
        )


def inverse_below(matrix):
    size = matrix.shape[1]
    strip = size // 2 // SUB
    row_ids = lax.broadcasted_iota(jnp.int32, (SUB, size), 0)
    lane_ids = lax.broadcasted_iota(jnp.int32, (SUB, size), 1)
    zero = jnp.zeros((SUB, size), jnp.float32)
    tiles = [matrix[n * SUB : (n + 1) * SUB] for n in range(matrix.shape[0] // SUB)]

    def columns_of(tile, start):
        return [
            jnp.broadcast_to(tile[:, start + k : start + k + 1], (SUB, size))
            for k in range(SUB)
        ]

    def less_rows(tile, band, columns, rows):
        tile = jnp.where(band, 0.0, tile)
        for k in range(SUB):
            tile = tile - columns[k] * rows[k : k + 1]
        return tile

    for base in range(0, size // SUB, strip):
        inner = tiles[base : base + strip]
        columns = columns_of(inner[0], base * SUB)
        for n in range(strip):
            start = (base + n) * SUB
            band = jnp.logical_and(lane_ids >= start, lane_ids < start + SUB)
            unit = (lane_ids - start == row_ids).astype(jnp.float32)
            rows = jnp.where(band, unit, inner[n])
            follows = n + 1 < strip
            ahead = []
            if follows:
                ahead = columns_of(inner[n], start + SUB)
                below = columns_of(inner[n + 1], start)
                later = columns_of(inner[n + 1], start + SUB)
            for k in range(SUB):
                column = columns[k]
                inverse = 1.0 / column[k : k + 1]
                here = row_ids == k

                def reduce(value):
                    pivot_row = value[k : k + 1] * inverse
                    return jnp.where(here, pivot_row, value - column * pivot_row)

                for other in range(k + 1, SUB):
                    columns[other] = reduce(columns[other])
                ahead = [reduce(value) for value in ahead]
                rows = reduce(rows)
            after = list(inner)
            after[n] = rows
            if follows:
                after[n + 1] = less_rows(inner[n + 1], band, below, rows)
                for k in range(SUB):
                    later = [
                        value - below[k] * line[k : k + 1] for value, line in zip(later, ahead)
                    ]
                columns = later
            for m in range(strip):
                if m != n and not (follows and m == n + 1):
                    after[m] = less_rows(inner[m], band, columns_of(inner[m], start), rows)
            inner = after
        outer = [m for m in range(len(tiles)) if not base <= m < base + strip]
        lines = [
            inner[m - base] if base <= m < base + strip else zero for m in range(size // SUB)
        ]
        product = jnp.dot(
            jnp.concatenate([tiles[m] for m in outer], axis=0),
            jnp.concatenate(lines, axis=0),
            precision=lax.Precision.HIGHEST,
            preferred_element_type=jnp.float32,
        )
        band = jnp.logical_and(lane_ids >= base * SUB, lane_ids < (base + strip) * SUB)
        for n, m in enumerate(outer):
            tiles[m] = jnp.where(band, 0.0, tiles[m]) - product[n * SUB : (n + 1) * SUB]
        tiles[base : base + strip] = inner
    return jnp.concatenate(tiles, axis=0)


def packed_halves(product, n_ens):
    half = product.shape[1] // 2
    row_ids = lax.broadcasted_iota(jnp.int32, (half, 2 * half), 0)
    lane_ids = lax.broadcasted_iota(jnp.int32, (half, 2 * half), 1)
    top, bottom = (product[0:half], product[half : 2 * half])
    dense = jnp.where(lane_ids <= row_ids + half, bottom, pltpu.roll(top, half, 1))
    diagonal = jnp.sum(jnp.where(lane_ids == row_ids, top, 0.0), axis=0, keepdims=True)
    tail = jnp.where(row_ids[0:SUB] == 1, diagonal, product[2 * half :])
    lines = half // n_ens
    return [
        jnp.concatenate([dense[e * lines : (e + 1) * lines], tail], axis=0)
        for e in range(n_ens)
    ]


def unpacked(parts):
    half = sum(part.shape[0] - SUB for part in parts)
    dense = jnp.concatenate([part[: part.shape[0] - SUB] for part in parts], axis=0)
    tail = parts[0][parts[0].shape[0] - SUB :]
    row_ids = lax.broadcasted_iota(jnp.int32, (half, 2 * half), 0)
    lane_ids = lax.broadcasted_iota(jnp.int32, (half, 2 * half), 1)
    turned = jnp.concatenate([dense, dense], axis=0).T
    upper = jnp.where(lane_ids > row_ids, pltpu.roll(dense, half, 1), turned[half:])
    upper = jnp.where(lane_ids == row_ids, tail[1:2], upper)
    top = jnp.where(lane_ids >= half, turned[:half], upper)
    bottom = jnp.where(lane_ids <= row_ids + half, dense, turned[half:])
    return jnp.concatenate([top, bottom], axis=0), tail[0:1]


def member_weights(gx, ens):
    members = gx.shape[2]
    half = members // 2
    gram, line = unpacked([gx[e] for e in range(gx.shape[0])])
    ids = [lax.broadcasted_iota(jnp.int32, gram.shape, axis) for axis in (0, 1)]
    unit = (ids[0] == ids[1]).astype(jnp.float32)
    line = jnp.broadcast_to(line, (SUB, members))
    swept = inverse_below(jnp.concatenate([gram / members + unit, line], axis=0))
    shift = swept[members : members + 1] / members
    weights = swept[:members] - unit - shift
    centred = weights - jnp.sum(weights, axis=1, keepdims=True) / members
    mine = jnp.where(ens == 0, centred[:half], centred[half:])
    return jnp.where(ens == 0, mine, pltpu.roll(mine, half, 1))


def updated_rows(mine, own, other, store):
    groups, _, rows, _, cols = own.shape
    for p in range(2):
        for r in range(0, rows, 2):
            pair, local = ([], [])
            for q in (r, r + 1):
                local.append(jnp.concatenate([own[g, p, q] for g in range(groups)], axis=0))
                remote = [other[g, p, q] for g in range(groups)]
                pair.append(jnp.concatenate([local[-1]] + remote, axis=0))
            added = jnp.dot(
                mine,
                jnp.concatenate(pair, axis=1),
                precision=lax.Precision.HIGHEST,
                preferred_element_type=jnp.float32,
            )
            for q in range(2):
                store(p, r + q, local[q] + added[:, q * cols : (q + 1) * cols])


def ensemble_kernel(n_lat, n_lon, n_ens, *refs):
    params, start_height, start_speed, slots_in, values_in, precision_in = refs[:6]
    gx_out, own_out, other_out = refs[6:9]
    owns, others, gxs, aux, lin, fin, slots_here, values_here, precision_here = refs[9:18]
    cells, info, start, height, speed_e, speed_n = refs[18:24]
    gots, edges, goths, outgoing, arriveds, part, partner_parts, half_sum, halves_all = refs[24:33]
    load, send_a, recv_a, send_p, recv_p, send_h, recv_h = refs[33:40]
    send_y, recv_y, send_x, recv_x = refs[40:]
    lat, lon, ens = (lax.axis_index("lat"), lax.axis_index("lon"), lax.axis_index("ens"))
    blocks = n_lat * n_lon
    me = lat * n_lon + lon
    column = n_lat * n_ens
    here = ens * n_lat + lat
    groups, _, rows, _, cols = own_out.shape
    groups_here = groups // n_lat
    share = n_lat // n_ens
    lane = lax.broadcasted_iota(jnp.int32, (SUB, cols), 1)

    def at(lat_to, lon_to, ens_to):
        return {"lat": lat_to, "lon": lon_to, "ens": ens_to}

    def same_column(flat):
        return at(lax.rem(flat, n_lat), lon, flat // n_lat)

    def same_core(block):
        return at(block // n_lon, lax.rem(block, n_lon), ens)

    def east_of(d):
        return lax.rem(lon + d + n_lon, n_lon)

    partner = at(lat, lon, 1 - ens)
    barrier = pltpu.get_barrier_semaphore()

    def greet(device):
        pl.semaphore_signal(barrier, inc=1, device_id=device, device_id_type=MESH)

    for i in range(1, blocks):
        greet(same_core(lax.rem(me + i, blocks)))
    for i in range(n_lat):
        greet(at(i, lon, 1 - ens))

    def landed(ref, sem):
        pltpu.make_async_copy(ref, ref, sem).wait()

    small = [
        pltpu.make_async_copy(src, dst, load.at[n])
        for n, (src, dst) in enumerate(
            (
                (slots_in, slots_here),
                (values_in, values_here),
                (precision_in, precision_here),
                (start_height, aux.at[0]),
                (start_speed, aux.at[1:3]),
            )
        )
    ]
    for copy in small:
        copy.start()
    for p in range(2):
        for r in range(rows):
            pltpu.make_async_copy(
                params.at[p, :, :, r, :], owns.at[0, :, p, r], load.at[len(small)]
            ).start()
    info[...] = jnp.zeros(info.shape, jnp.float32)
    for copy in small:
        copy.wait()
    lines = flat_lines(
        [
            ref[t, 0].astype(jnp.float32)
            for ref in (slots_here, values_here, precision_here)
            for t in range(ITERS)
        ],
        cols,
    )
    lines.append(jnp.zeros((rows - len(lines), cols), jnp.float32))
    aux[3] = jnp.concatenate(lines, axis=0)
    landed(owns.at[0], load.at[len(small)])

    def field_copy(i, d):
        return send(
            aux.at[0:3],
            fin.at[(d % 3) * n_lat + lat],
            send_a.at[0],
            recv_a.at[0],
            at(lax.rem(lat + i, n_lat), east_of(-d), ens),
        )

    def line_copy(i):
        return send(
            aux.at[3],
            lin.at[me],
            send_a.at[1],
            recv_a.at[1],
            same_core(lax.rem(me + i, blocks)),
        )

    def run_iteration(t, own, other, gx):
        got, goth, arrived = (gots.at[t], goths.at[t], arriveds.at[t])
        partner_part, halves = (partner_parts.at[t], halves_all.at[t])

        def param_copy(k, i):
            to = lax.rem(lat + i, n_lat)
            return send(
                own.at[to * groups_here + k],
                got.at[k, :, :, lat],
                send_p.at[k],
                recv_p.at[k],
                at(to, lon, ens),
            )

        def edge_copy(k, i, side):
            to = lax.rem(lat + i, n_lat)
            return send(
                edges.at[side, to * groups_here + k],
                goth.at[k, lat, side],
                send_h.at[k],
                recv_h.at[k],
                at(to, east_of(2 * side - 1), ens),
            )

        swap = send(own, other, send_x.at[t, 0], recv_x.at[t, 0], partner)

        def pack_edges(g):
            slot = lane // EDGE
            for p in range(2):
                left = jnp.zeros((SUB, cols), jnp.float32)
                right = left
                for r in range(rows):
                    tile = pltpu.roll(own[g, p, r], EDGE * r, 1)
                    left = jnp.where(slot == r, tile, left)
                    right = jnp.where(slot == (r + rows - 1) % rows, tile, right)
                edges[0, g, p] = pltpu.roll(left, 2 * EDGE * lat, 1)
                edges[1, g, p] = pltpu.roll(right, 2 * EDGE * lat, 1)

        if t == 0:
            for g in range(groups):
                pack_edges(g)
            pl.semaphore_wait(barrier, blocks - 1 + n_lat)
            for d in (0, 1, -1):
                for i in range(0 if d else 1, n_lat):
                    field_copy(i, d).start()
        for k in range(groups_here):
            for i in range(1, n_lat):
                param_copy(k, i).start()
            if t and k == 0:
                for g in range(groups):
                    pack_edges(g)
            for side in range(2):
                for i in range(n_lat):
                    edge_copy(k, i, side).start()
            if t == 0 and k == 0:
                for i in range(1, blocks):
                    line_copy(i).start()
        swap.start()
        for k in range(groups_here):
            got[k, :, :, pl.ds(lat, 1)] = own[pl.ds(lat * groups_here + k, 1)].reshape(
                2, rows, 1, SUB, cols
            )

        if t == 0:
            fin[pl.ds(lat, 1)] = aux[0:3].reshape(1, 3, rows, cols)
            lin[pl.ds(me, 1)] = aux[3:4]
            landed(fin.at[0 : 3 * n_lat - 1], recv_a.at[0])
            segment = segment_of((rows, cols), n_lat)
            inside = lax.rem(lane + EDGE, 2 * EDGE) < EDGE
            for i in range(3):
                halo = jnp.zeros((rows, cols), jnp.float32)
                tiles = []
                for a in range(n_lat):
                    turned = [
                        pltpu.roll(fin[d * n_lat + a, i], 2 * EDGE * a, 1) for d in range(3)
                    ]
                    tiles.append(turned[0])
                    outer = jnp.where(inside, turned[2], turned[1])
                    halo = jnp.where(segment == a, outer, halo)
                for a, tile in enumerate(tiles + [halo]):
                    for r in range(rows):
                        start[i, r, a] = jnp.broadcast_to(tile[r : r + 1], (SUB, cols))
            for r in range(rows):
                speed_n[r + 1] = start[2, r]
            set_edges(speed_n)
            for r in range(0, rows, CHUNK):
                flow = east(start[1, r : r + CHUNK]) + (
                    speed_n[r + 2 : r + 2 + CHUNK] - speed_n[r : r + CHUNK]
                )
                start[0, r : r + CHUNK] = start[0, r : r + CHUNK] - depth_step * flow
            landed(lin.at[0 : blocks - 1], recv_a.at[1])
            for n in range(ITERS):
                for a in range(n_lat):
                    line = lin[a * n_lon + lon][n : n + 1].astype(jnp.int32)
                    cells[n * n_lat + a : n * n_lat + a + 1] = line

        def answer_copy(k, i):
            to = lax.rem(here + i, column)
            part_rows = pl.ds(k * SUB, SUB)
            return send(
                outgoing.at[pl.ds((to // n_lat) * share, share), part_rows],
                arrived.at[:, here, part_rows],
                send_y.at[k],
                recv_y.at[k],
                same_column(to),
            )

        def group(k, carry):
            landed(got.at[k, :, :, 0 : n_lat - 1], recv_p.at[k])
            for p in range(2):
                for r in range(rows):
                    for a in range(1, n_lat):
                        got[k, p, r, a] = pltpu.roll(got[k, p, r, a], 2 * EDGE * a, 1)
            landed(goth.at[k], recv_h.at[k])
            slot = lane // EDGE
            for p in range(2):
                for r in range(rows):
                    halo = jnp.zeros((SUB, cols), jnp.float32)
                    for a in range(n_lat):
                        after, before = (goth[k, a, 0, p], goth[k, a, 1, p])
                        halo = jnp.where(slot == (2 * a + r) % rows, after, halo)
                        halo = jnp.where(slot == (2 * a + r + rows - 1) % rows, before, halo)
                    got[k, p, r, n_lat] = pltpu.roll(halo, (cols - EDGE * r) % cols, 1)
            run_group(k, got, start, height, speed_e, speed_n)
            for a in range(n_lat):
                line = t * n_lat + a
                wanted = jnp.broadcast_to(cells[line : line + 1], (SUB, cols))
                lanes = jnp.bitwise_and(wanted + 2 * EDGE * a, cols - 1)
                where_row = jnp.right_shift(wanted, cols.bit_length() - 1)
                found = jnp.zeros((SUB, cols), jnp.float32)
                for r in range(rows):
                    tile = height[r + 1, a]
                    picked = jnp.take_along_axis(tile, lanes, axis=1)
                    found = jnp.where(where_row == r, picked, found)
                outgoing[a, pl.ds(k * SUB, SUB)] = found
            for i in range(1, column):
                answer_copy(k, i).start()
            return carry

        lax.fori_loop(0, groups_here, group, 0)
        for j in range(share):
            arrived[j, pl.ds(here, 1)] = outgoing[pl.ds(ens * share + j, 1)]
        if t == 0:
            slots = cols // blocks
            heard = jnp.concatenate([lin[b] for b in range(blocks)], axis=0)
            kinds = lin.shape[1]
            square = (heard.shape[1], cols)
            from_ids = lax.broadcasted_iota(jnp.int32, square, 0)
            to_ids = lax.broadcasted_iota(jnp.int32, square, 1)
            line_ids = lax.broadcasted_iota(jnp.int32, heard.shape, 0)
            lane_ids = lax.broadcasted_iota(jnp.int32, heard.shape, 1)
            for j in range(share):
                owner = (ens * share + j) * n_lon + lon
                chosen = from_ids == owner * slots + lax.rem(to_ids, slots)
                spread_out = jnp.dot(
                    heard,
                    chosen.astype(jnp.float32),
                    precision=lax.Precision.HIGHEST,
                    preferred_element_type=jnp.float32,
                )
                for kind in range(2 * ITERS):
                    wanted = line_ids == (lane_ids // slots) * kinds + ITERS + kind
                    info[kind : kind + 1, j * cols : (j + 1) * cols] = jnp.sum(
                        jnp.where(wanted, spread_out, 0.0), axis=0, keepdims=True
                    )
        for k in range(groups_here):
            landed(arrived.at[:, 0 : column - 1, k * SUB : (k + 1) * SUB], recv_y.at[k])

        members = column * arrived.shape[2]
        predicted = jnp.concatenate(
            [
                jnp.concatenate([arrived[j, s] for s in range(column)], axis=0)
                for j in range(share)
            ],
            axis=1,
        )
        observed = info[t : t + 1]
        precision = info[ITERS + t : ITERS + t + 1]
        centre = jnp.sum(predicted, axis=0, keepdims=True) / members
        spread = predicted - centre
        weighted = spread * precision
        extra = lax.broadcasted_iota(jnp.int32, (SUB, share * cols), 0) == 0
        extra = jnp.where(extra, jnp.broadcast_to(observed - centre, extra.shape), 0.0)
        product = lax.dot_general(
            jnp.concatenate([spread, extra], axis=0),
            weighted,
            (((1,), (1,)), ((), ())),
            precision=lax.Precision.HIGHEST,
            preferred_element_type=jnp.float32,
        )
        for e, piece in enumerate(packed_halves(product, n_ens)):
            part[e] = piece

        trade = send(part.at[1 - ens], partner_part, send_x.at[t, 1], recv_x.at[t, 1], partner)
        trade.start()
        trade.wait()
        half_sum[...] = part[ens] + partner_part[...]

        def half_copy(i):
            return send(
                half_sum,
                halves.at[lon],
                send_x.at[t, 3],
                recv_x.at[t, 3],
                at(lat, east_of(i), ens),
            )

        for i in range(1, n_lon):
            half_copy(i).start()
        halves[lon] = half_sum[...]
        landed(halves.at[0 : n_lon - 1], recv_x.at[t, 3])
        landed(halves.at[0 : n_lon - 1], send_x.at[t, 3])
        total = halves[0]
        for b in range(1, n_lon):
            total = total + halves[b]
        half_sum[...] = total
        finish = send(half_sum, gx.at[ens], send_x.at[t, 2], recv_x.at[t, 2], partner)
        finish.start()
        gx[ens] = total
        swap.wait()
        for k in range(groups_here):
            landed(got.at[k, :, :, 0 : n_lat - 1], send_p.at[k])
            landed(goth.at[k], send_h.at[k])
            landed(arrived.at[:, 0 : column - 1, k * SUB : (k + 1) * SUB], send_y.at[k])
        if t == 0:
            landed(fin.at[0 : 3 * n_lat - 1], send_a.at[0])
            landed(lin.at[0 : blocks - 1], send_a.at[1])
        finish.wait()

    for t in range(ITERS):
        last = t == ITERS - 1
        own = own_out if last and t else owns.at[t]
        other, gx = (other_out, gx_out) if last else (others.at[t], gxs.at[t])
        run_iteration(t, own, other, gx)
        if not last:
            new = own_out if t + 1 == ITERS - 1 else owns.at[t + 1]

            def store(p, r, value, new=new):
                for g in range(groups):
                    new[g, p, r] = value[g * SUB : (g + 1) * SUB]

            updated_rows(member_weights(gx, ens), own, other, store)


def ensemble_call(sizes, own_shape, *operands):
    n_lat, n_lon, n_ens = sizes
    blocks = n_lat * n_lon
    column = n_lat * n_ens
    groups, _, rows, _, cols = own_shape
    groups_here = groups // n_lat
    members = groups * SUB * n_ens
    share = n_lat // n_ens
    lines = members // 2 // n_ens + SUB
    f32 = jnp.float32
    dma = pltpu.SemaphoreType.DMA
    gx_shape = (n_ens, lines, members)
    outs = [jax.ShapeDtypeStruct(shape, f32) for shape in (gx_shape, own_shape, own_shape)]

    def both(shape):
        return [dma(shape), dma(shape)]

    scratch = [
        VMEM((max(ITERS - 1, 1),) + own_shape, f32),
        VMEM((max(ITERS - 1, 1),) + own_shape, f32),
        VMEM((max(ITERS - 1, 1),) + gx_shape, f32),
        VMEM((4, rows, cols), f32),
        VMEM((blocks, rows, cols), f32),
        VMEM((3 * n_lat, 3, rows, cols), f32),
    ]
    scratch += [VMEM(obs.shape, obs.dtype) for obs in operands[3:]]
    scratch += [
        VMEM((ITERS * n_lat, cols), jnp.int32),
        VMEM((SUB, share * cols), f32),
        VMEM((3, rows, n_lat + 1, SUB, cols), f32),
        VMEM((rows + 2, n_lat + 1, SUB, cols), f32),
        VMEM((rows, n_lat + 1, SUB, cols), f32),
        VMEM((rows + 2, n_lat + 1, SUB, cols), f32),
        VMEM((ITERS, groups_here, 2, rows, n_lat + 1, SUB, cols), f32),
        VMEM((2, groups, 2, SUB, cols), f32),
        VMEM((ITERS, groups_here, n_lat, 2, 2, SUB, cols), f32),
        VMEM((n_lat, groups_here * SUB, cols), f32),
        VMEM((ITERS, share, column, groups_here * SUB, cols), f32),
        VMEM(gx_shape, f32),
        VMEM((ITERS, lines, members), f32),
        VMEM((lines, members), f32),
        VMEM((ITERS, n_lon, lines, members), f32),
        dma((6,)),
    ]
    for shape in ((2,), (groups_here,), (groups_here,), (groups_here,), (ITERS, 4)):
        scratch += both(shape)
    return pl.pallas_call(
        functools.partial(ensemble_kernel, n_lat, n_lon, n_ens),
        out_shape=outs,
        in_specs=[pl.BlockSpec(memory_space=pltpu.HBM)] * len(operands),
        out_specs=[pl.BlockSpec(memory_space=VMEM)] * len(outs),
        scratch_shapes=scratch,
        compiler_params=pltpu.CompilerParams(
            collective_id=0, has_side_effects=True, vmem_limit_bytes=VMEM_LIMIT
        ),
    )(*operands)


def update_kernel(gx, own, other, out, new, sems):
    copies = [pltpu.make_async_copy(new.at[p], out.at[p], sems.at[p]) for p in range(2)]
    rows = own.shape[2]

    def store(p, r, value):
        new[p, :, r, :] = value
        if r == rows - 1:
            copies[p].start()

    updated_rows(member_weights(gx, lax.axis_index("ens")), own, other, store)
    for copy in copies:
        copy.wait()


def update_call(shape, *operands):
    return pl.pallas_call(
        update_kernel,
        out_shape=jax.ShapeDtypeStruct(shape, jnp.float32),
        in_specs=[pl.BlockSpec(memory_space=VMEM)] * len(operands),
        out_specs=pl.BlockSpec(memory_space=pltpu.HBM),
        scratch_shapes=[VMEM(shape, jnp.float32), pltpu.SemaphoreType.DMA((2,))],
        compiler_params=pltpu.CompilerParams(vmem_limit_bytes=VMEM_LIMIT),
    )(*operands)


def per_device_columns(sizes, parameters, initial_height, initial_speed, *observations):
    shape = parameters.shape
    own_shape = (shape[1] // SUB, shape[0], shape[2], SUB, shape[3])
    grouped = parameters.reshape(shape[0], shape[1] // SUB, SUB, shape[2], shape[3])
    turned = [jnp.transpose(obs, (0, 1, 3, 2)) for obs in observations]
    operands = [grouped, initial_height, initial_speed] + turned
    operands = [pltpu.with_memory_space_constraint(x, pltpu.HBM) for x in operands]
    gathered = ensemble_call(sizes, own_shape, *operands)
    return update_call(shape, *gathered)


def by_members(sizes, parameters, initial_height, initial_speed, obs_slots, *rest):
    n_lat, n_lon, n_ens = sizes
    members_here, rows, cols = parameters.shape[1:]
    fits = (
        n_ens == 2
        and n_lat % n_ens == 0
        and n_lon >= 3
        and members_here % (SUB * n_lat) == 0
        and rows == SUB
        and members_here * n_ens == cols
        and cols == 128
        and EDGE * rows == cols
        and 2 * EDGE * n_lat == cols
        and 2 * STEPS <= EDGE
        and ITERS * 3 <= rows
        and obs_slots.shape[2] * obs_slots.shape[3] == cols
        and obs_slots.shape[3] == SUB
        and ITERS > 1
    )
    arguments = (parameters, initial_height, initial_speed, obs_slots) + rest
    if fits:
        return per_device_columns(sizes, *arguments)
    return per_device_halo(*arguments)


def solution(mesh):
    placed = (
        P(None, "ens", "lat", "lon"),
        P("lat", "lon"),
        P(None, "lat", "lon"),
        P(None, ("lat", "lon"), None, None),
        P(None, ("lat", "lon"), None, None),
        P(None, ("lat", "lon"), None, None),
    )
    return jax.shard_map(
        functools.partial(by_members, tuple(mesh.shape[a] for a in ("lat", "lon", "ens"))),
        mesh=mesh,
        in_specs=placed,
        out_specs=P(None, "ens", "lat", "lon"),
        check_vma=False,
    )
```

```python
import math

import functools

import jax
import jax.numpy as jnp
from jax import lax
from jax.experimental import pallas as pl
from jax.experimental.pallas import tpu as pltpu
from jax.sharding import PartitionSpec as P

STEPS = 6
ITERS = 2


depth_step = 0.7
gravity_step = 0.7
coriolis = 0.1


def padded_2(value, sides, width, wrap):
    for axis, dim in sides:
        peers, length = (lax.axis_size(axis), value.shape[dim])
        up = [(i, (i + 1) % peers) for i in range(peers if wrap else peers - 1)]
        down = [(j, i) for i, j in up]
        last = lax.slice_in_dim(value, length - width, length, axis=dim)
        leading = lax.slice_in_dim(value, 0, width, axis=dim)
        before = lax.ppermute(last, axis, up)
        after = lax.ppermute(leading, axis, down)
        value = jnp.concatenate([before, value, after], axis=dim)
    return value


def wall_rows(padded):
    row_count = padded.shape[-2]
    position = lax.axis_index("lat")
    last_block = lax.axis_size("lat") - 1
    row_ids = lax.broadcasted_iota(jnp.int32, (row_count, 1), 0)
    lower_wall = jnp.logical_and(row_ids == 0, position == 0)
    upper_wall = jnp.logical_and(row_ids == row_count - 1, position == last_block)
    keep_rows = jnp.logical_not(jnp.logical_or(lower_wall, upper_wall))
    return padded * keep_rows.astype(padded.dtype)


def advance(height, speeds, friction, forcing):
    east_padded = padded_2(speeds[0], (("lon", 2),), 1, True)
    north_padded = padded_2(speeds[1], (("lat", 1),), 1, False)
    east_diff = east_padded[:, :, 2:] - east_padded[:, :, :-2]
    north_diff = north_padded[:, 2:, :] - north_padded[:, :-2, :]
    height = height - depth_step * (east_diff + north_diff) + forcing
    padded_height = padded_2(height, (("lat", 1), ("lon", 2)), 1, True)
    padded_height = wall_rows(padded_height)
    slope_east = padded_height[:, 1:-1, 2:] - padded_height[:, 1:-1, :-2]
    slope_north = padded_height[:, 2:, 1:-1] - padded_height[:, :-2, 1:-1]
    eastward = (1.0 - friction) * speeds[0] - gravity_step * slope_east + coriolis * speeds[1]
    northward = (1.0 - friction) * speeds[1] - gravity_step * slope_north - coriolis * speeds[0]
    return (height, jnp.stack([eastward, northward]))


def forward(parameters, initial_height, initial_speed):
    members = parameters.shape[1]
    height = jnp.broadcast_to(initial_height, (members,) + initial_height.shape)
    speeds = jnp.broadcast_to(initial_speed[:, None], (2, members) + initial_height.shape)
    for substep in range(STEPS):
        height, speeds = advance(height, speeds, parameters[0], parameters[1])
    return height


def predict(height, cells):
    flattened = height.reshape(height.shape[0], -1)
    wanted = cells.reshape(-1)
    picked = jnp.take(flattened, jnp.clip(wanted, 0, flattened.shape[1] - 1), axis=1)
    picked = jnp.where(wanted[None, :] >= 0, picked, jnp.float32(0.0))
    return picked.T.reshape(cells.shape[0], -1)


def gram_terms(predicted, observed, precision):
    members = predicted.shape[1]
    centre = jnp.mean(predicted, axis=1, keepdims=True)
    spread = predicted - centre
    weighted = spread * precision[:, None]
    misfit = observed[:, None] - predicted
    gram_part = jnp.dot(spread.T, weighted, precision=lax.Precision.HIGHEST) / members
    cross_part = jnp.dot(weighted.T, misfit, precision=lax.Precision.HIGHEST) / math.sqrt(members)
    return (gram_part, cross_part)


def solve_weights(gram_part, cross_part):
    members = gram_part.shape[0]
    system = jnp.eye(members, dtype=jnp.float32) + gram_part
    factor = jnp.linalg.cholesky(system)
    weights = jax.scipy.linalg.cho_solve((factor, True), cross_part) / math.sqrt(members)
    return weights - jnp.mean(weights, axis=0, keepdims=True)


def per_device_halo(parameters, initial_height, initial_speed, obs_slots, obs_values, obs_precision):
    owners = obs_slots.shape[2]
    slot_count = obs_slots.shape[3]
    members_here = parameters.shape[1]
    member_block = lax.axis_index("ens")
    owner_values, owner_precision = (
        lax.all_to_all(obs_values[:, 0], ("lat", "lon"), split_axis=1, concat_axis=1, tiled=True),
        lax.all_to_all(
            obs_precision[:, 0], ("lat", "lon"), split_axis=1, concat_axis=1, tiled=True
        ),
    )
    for iteration in range(ITERS):
        height = forward(parameters, initial_height, initial_speed)
        outgoing = predict(height, obs_slots[iteration, 0])
        received = outgoing
        observed = owner_values[iteration]
        precision = owner_precision[iteration]
        received = received.reshape(owners, slot_count, members_here)
        gathered = lax.all_gather(received, "ens", axis=2, tiled=True)
        members = gathered.shape[2]
        gram_part, cross_part = gram_terms(
            gathered.reshape(-1, members), observed.reshape(-1), precision.reshape(-1)
        )
        gram_part, cross_part = lax.psum((gram_part, cross_part), ("lat", "lon"))
        centred = solve_weights(gram_part, cross_part)
        local_weights = lax.dynamic_slice_in_dim(
            centred, member_block * members_here, members_here, 1
        )
        starting = jnp.zeros(
            (2, members_here, parameters.shape[2] * parameters.shape[3]), jnp.float32
        )
        pieces = lax.all_gather(parameters, "ens", axis=1, tiled=True)
        stacked = pieces.reshape(pieces.shape[0], pieces.shape[1], -1)
        increment = starting + jnp.einsum(
            "pjc,jm->pmc", stacked, local_weights, precision=lax.Precision.HIGHEST
        )
        parameters = parameters + increment.reshape(parameters.shape)
    return parameters


MESH = pl.DeviceIdType.MESH
VMEM = pltpu.VMEM
EDGE = 16
SUB = 8
CHUNK = 2
VMEM_LIMIT = 40 * 2**20


def segment_of(shape, tiles):
    lane = lax.broadcasted_iota(jnp.int32, shape, len(shape) - 1)
    width = shape[-1] // tiles
    return lax.rem(lane + width // 2, shape[-1]) // width


def east(field):
    tiles, cols = (field.shape[1] - 1, field.shape[3])
    width = cols // tiles
    lane = lax.broadcasted_iota(jnp.int32, field.shape[2:], 1)

    def moved(shift, seam):
        turned = pltpu.roll(field, shift % cols, 3)
        halo = turned[:, tiles]
        parts = []
        for a in range(tiles):
            here = lane == (a * width + seam) % cols
            parts.append(jnp.where(here, turned[:, tiles], turned[:, a]))
            halo = jnp.where(here, turned[:, a], halo)
        return parts + [halo]

    return jnp.stack(
        [after - before for after, before in zip(moved(-1, -1), moved(1, 0))], axis=1
    )


def set_edges(ref):
    tiles, cols = (ref.shape[1] - 1, ref.shape[3])
    width = cols // tiles
    segment = segment_of(ref.shape[2:], tiles)
    zero = jnp.zeros(ref.shape[2:], jnp.float32)
    first, last = (1, ref.shape[0] - 2)
    for a in range(tiles):
        ref[0, a] = pltpu.roll(ref[last, a - 1], width, 1) if a else zero
        ref[last + 1, a] = (
            pltpu.roll(ref[first, a + 1], cols - width, 1) if a + 1 < tiles else zero
        )
    ref[0, tiles] = jnp.where(segment == 0, 0.0, pltpu.roll(ref[last, tiles], width, 1))
    ref[last + 1, tiles] = jnp.where(
        segment == tiles - 1, 0.0, pltpu.roll(ref[first, tiles], cols - width, 1)
    )


def flat_lines(blocks, width):
    count, groups = blocks[0].shape
    lanes = lax.broadcasted_iota(jnp.int32, (groups, width), 1)
    group_ids = lax.broadcasted_iota(jnp.int32, (groups, width), 0)
    spread_out = jnp.dot(
        jnp.concatenate(blocks, axis=0),
        (lanes // count == group_ids).astype(jnp.float32),
        precision=lax.Precision.HIGHEST,
        preferred_element_type=jnp.float32,
    )
    slots = lax.broadcasted_iota(jnp.int32, (count, width), 0)
    lanes = lax.broadcasted_iota(jnp.int32, (count, width), 1)
    keep = lax.rem(lanes, count) == slots
    lines = []
    for n in range(len(blocks)):
        block = spread_out[n * count : (n + 1) * count]
        lines.append(jnp.sum(jnp.where(keep, block, 0.0), axis=0, keepdims=True))
    return lines


def send(src, dst, send_sem, recv_sem, device):
    return pltpu.make_async_remote_copy(
        src_ref=src,
        dst_ref=dst,
        send_sem=send_sem,
        recv_sem=recv_sem,
        device_id=device,
        device_id_type=MESH,
    )


def run_group(k, got, start, height, speed_e, speed_n):
    rows = start.shape[1]
    chunks = [pl.ds(c, CHUNK) for c in range(0, rows, CHUNK)]
    upper = [pl.ds(c + 2, CHUNK) for c in range(0, rows, CHUNK)]
    inner = [pl.ds(c + 1, CHUNK) for c in range(0, rows, CHUNK)]

    def new_speeds(n, keep, old_e, old_n):
        slope_e = east(height[inner[n]])
        slope_n = height[upper[n]] - height[chunks[n]]
        speed_e[chunks[n]] = keep * old_e - gravity_step * slope_e + coriolis * old_n
        speed_n[inner[n]] = keep * old_n - gravity_step * slope_n - coriolis * old_e

    def new_height():
        for n in range(len(chunks)):
            flow = east(speed_e[chunks[n]]) + (speed_n[upper[n]] - speed_n[chunks[n]])
            height[inner[n]] = height[inner[n]] - depth_step * flow + got[k, 1, chunks[n]]

    for n in range(len(chunks)):
        height[inner[n]] = start[0, chunks[n]] + got[k, 1, chunks[n]]
    set_edges(height)
    for n in range(len(chunks)):
        keep = 1.0 - got[k, 0, chunks[n]]
        got[k, 0, chunks[n]] = keep
        new_speeds(n, keep, start[1, chunks[n]], start[2, chunks[n]])
    set_edges(speed_n)

    def middle(step, carry):
        new_height()
        set_edges(height)
        for n in range(len(chunks)):
            new_speeds(n, got[k, 0, chunks[n]], speed_e[chunks[n]], speed_n[inner[n]])
        set_edges(speed_n)
        return carry

    lax.fori_loop(1, STEPS - 1, middle, 0)
    tiles = start.shape[2] - 1
    for n in range(len(chunks)):
        flow = east(speed_e[chunks[n]])[:, 0:tiles] + (
            speed_n[upper[n], 0:tiles] - speed_n[chunks[n], 0:tiles]
        )
        height[inner[n], 0:tiles] = (
            height[inner[n], 0:tiles] - depth_step * flow + got[k, 1, chunks[n], 0:tiles]
        )


def inverse_rows(matrix):
    size = matrix.shape[1]
    strip = size // 2 // SUB
    row_ids = lax.broadcasted_iota(jnp.int32, (SUB, size), 0)
    lane_ids = lax.broadcasted_iota(jnp.int32, (SUB, size), 1)
    zero = jnp.zeros((SUB, size), jnp.float32)
    tiles = [matrix[n * SUB : (n + 1) * SUB] for n in range(matrix.shape[0] // SUB)]

    def columns_of(tile, start):
        return [
            jnp.broadcast_to(tile[:, start + k : start + k + 1], (SUB, size))
            for k in range(SUB)
        ]

    def less_rows(tile, band, columns, rows):
        tile = jnp.where(band, 0.0, tile)
        for k in range(SUB):
            tile = tile - columns[k] * rows[k : k + 1]
        return tile

    for base in range(0, size // SUB, strip):
        last = base + strip == size // SUB
        inner = tiles[base:] if last else tiles[base : base + strip]
        columns = columns_of(inner[0], base * SUB)
        for n in range(strip):
            start = (base + n) * SUB
            band = jnp.logical_and(lane_ids >= start, lane_ids < start + SUB)
            unit = (lane_ids - start == row_ids).astype(jnp.float32)
            rows = jnp.where(band, unit, inner[n])
            follows = n + 1 < strip
            ahead = []
            if follows:
                ahead = columns_of(inner[n], start + SUB)
                below = columns_of(inner[n + 1], start)
                later = columns_of(inner[n + 1], start + SUB)
            for k in range(SUB):
                column = columns[k]
                inverse = 1.0 / column[k : k + 1]
                here = row_ids == k

                def reduce(value):
                    pivot_row = value[k : k + 1] * inverse
                    return jnp.where(here, pivot_row, value - column * pivot_row)

                for other in range(k + 1, SUB):
                    columns[other] = reduce(columns[other])
                ahead = [reduce(value) for value in ahead]
                rows = reduce(rows)
            after = list(inner)
            after[n] = rows
            if follows:
                after[n + 1] = less_rows(inner[n + 1], band, below, rows)
                for k in range(SUB):
                    later = [
                        value - below[k] * line[k : k + 1] for value, line in zip(later, ahead)
                    ]
                columns = later
            for m in range(len(inner)):
                if m != n and not (follows and m == n + 1):
                    after[m] = less_rows(inner[m], band, columns_of(inner[m], start), rows)
            inner = after
        if last:
            return inner[:strip], inner[strip]
        outer = [m for m in range(len(tiles)) if not base <= m < base + strip]
        lines = [
            inner[m - base] if base <= m < base + strip else zero for m in range(size // SUB)
        ]
        product = jnp.dot(
            jnp.concatenate([tiles[m] for m in outer], axis=0),
            jnp.concatenate(lines, axis=0),
            precision=lax.Precision.HIGHEST,
            preferred_element_type=jnp.float32,
        )
        band = jnp.logical_and(lane_ids >= base * SUB, lane_ids < (base + strip) * SUB)
        for n, m in enumerate(outer):
            tiles[m] = jnp.where(band, 0.0, tiles[m]) - product[n * SUB : (n + 1) * SUB]
        tiles[base : base + strip] = inner


def packed(e, rows, tail):
    lines, width = (rows.shape[0] // 2, rows.shape[1])
    half = width // 2
    row_ids = lax.broadcasted_iota(jnp.int32, (lines, width), 0) + e * lines
    lane_ids = lax.broadcasted_iota(jnp.int32, (lines, width), 1)
    top, bottom = (rows[:lines], rows[lines:])
    dense = jnp.where(lane_ids <= row_ids + half, bottom, pltpu.roll(top, half, 1))
    diagonal = jnp.sum(jnp.where(lane_ids == row_ids, top, 0.0), axis=0, keepdims=True)
    tail_ids = lax.broadcasted_iota(jnp.int32, tail.shape, 0)
    return jnp.concatenate([dense, jnp.where(tail_ids == 1, diagonal, tail)], axis=0)


def unpacked(parts):
    half = sum(part.shape[0] - SUB for part in parts)
    dense = jnp.concatenate([part[: part.shape[0] - SUB] for part in parts], axis=0)
    tails = [part[part.shape[0] - SUB :] for part in parts]
    diagonal = sum(tail[1:2] for tail in tails)
    row_ids = lax.broadcasted_iota(jnp.int32, (half, 2 * half), 0)
    lane_ids = lax.broadcasted_iota(jnp.int32, (half, 2 * half), 1)
    turned = jnp.concatenate([dense, dense], axis=0).T
    upper = jnp.where(lane_ids > row_ids, pltpu.roll(dense, half, 1), turned[half:])
    upper = jnp.where(lane_ids == row_ids, diagonal, upper)
    top = jnp.where(lane_ids >= half, turned[:half], upper)
    bottom = jnp.where(lane_ids <= row_ids + half, dense, turned[half:])
    return top, bottom, tails[0][0:1]


def member_weights(gx, ens):
    members = gx.shape[2]
    half = members // 2
    top, bottom, line = unpacked([gx[e] for e in range(gx.shape[0])])

    def turned(value):
        return pltpu.roll(value, half, 1)

    swap = ens == 0
    line = jnp.broadcast_to(line, (SUB, members))
    line = jnp.where(swap, turned(line), line)
    upper = jnp.where(swap, turned(bottom), top) / members
    lower = jnp.where(swap, turned(top), bottom) / members
    row_ids = lax.broadcasted_iota(jnp.int32, (half, members), 0)
    lane_ids = lax.broadcasted_iota(jnp.int32, (half, members), 1)
    unit = (lane_ids == row_ids + half).astype(jnp.float32)
    upper = upper + (lane_ids == row_ids).astype(jnp.float32)
    rows, below = inverse_rows(jnp.concatenate([upper, lower + unit, line], axis=0))
    weights = jnp.concatenate(rows, axis=0) - unit - below[0:1] / members
    return weights - jnp.sum(weights, axis=1, keepdims=True) / members


def updated_rows(mine, own, other, store):
    groups, _, rows, _, cols = own.shape
    for p in range(2):
        for r in range(0, rows, 2):
            pair, local = ([], [])
            for q in (r, r + 1):
                local.append(jnp.concatenate([own[g, p, q] for g in range(groups)], axis=0))
                remote = [other[g, p, q] for g in range(groups)]
                pair.append(jnp.concatenate(remote + [local[-1]], axis=0))
            added = jnp.dot(
                mine,
                jnp.concatenate(pair, axis=1),
                precision=lax.Precision.HIGHEST,
                preferred_element_type=jnp.float32,
            )
            for q in range(2):
                store(p, r + q, local[q] + added[:, q * cols : (q + 1) * cols])


def ensemble_kernel(n_lat, n_lon, n_ens, *refs):
    params, start_height, start_speed, slots_in, values_in, precision_in = refs[:6]
    gx_out, own_out, other_out = refs[6:9]
    owns, others, gxs, aux, lin, fin, slots_here, values_here, precision_here = refs[9:18]
    cells, info, start, height, speed_e, speed_n = refs[18:24]
    gots, edges, goths, outgoing, arriveds, part, partner_parts, half_sum, halves_all = refs[24:33]
    load, send_a, recv_a, send_p, recv_p, send_h, recv_h = refs[33:40]
    send_y, recv_y, send_x, recv_x = refs[40:]
    lat, lon, ens = (lax.axis_index("lat"), lax.axis_index("lon"), lax.axis_index("ens"))
    blocks = n_lat * n_lon
    me = lat * n_lon + lon
    column = n_lat * n_ens
    here = ens * n_lat + lat
    groups, _, rows, _, cols = own_out.shape
    groups_here = groups // n_lat
    share = n_lat // n_ens
    lane = lax.broadcasted_iota(jnp.int32, (SUB, cols), 1)

    def at(lat_to, lon_to, ens_to):
        return {"lat": lat_to, "lon": lon_to, "ens": ens_to}

    def same_column(flat):
        return at(lax.rem(flat, n_lat), lon, flat // n_lat)

    def same_core(block):
        return at(block // n_lon, lax.rem(block, n_lon), ens)

    def east_of(d):
        return lax.rem(lon + d + n_lon, n_lon)

    partner = at(lat, lon, 1 - ens)
    barrier = pltpu.get_barrier_semaphore()

    def greet(device):
        pl.semaphore_signal(barrier, inc=1, device_id=device, device_id_type=MESH)

    for i in range(1, blocks):
        greet(same_core(lax.rem(me + i, blocks)))
    for i in range(n_lat):
        greet(at(i, lon, 1 - ens))

    def landed(ref, sem):
        pltpu.make_async_copy(ref, ref, sem).wait()

    small = [
        pltpu.make_async_copy(src, dst, load.at[n])
        for n, (src, dst) in enumerate(
            (
                (slots_in, slots_here),
                (values_in, values_here),
                (precision_in, precision_here),
                (start_height, aux.at[0]),
                (start_speed, aux.at[1:3]),
            )
        )
    ]
    for copy in small:
        copy.start()
    for p in range(2):
        for r in range(rows):
            pltpu.make_async_copy(
                params.at[p, :, :, r, :], owns.at[0, :, p, r], load.at[len(small)]
            ).start()
    info[...] = jnp.zeros(info.shape, jnp.float32)
    for copy in small:
        copy.wait()
    lines = flat_lines(
        [
            ref[t, 0].astype(jnp.float32)
            for ref in (slots_here, values_here, precision_here)
            for t in range(ITERS)
        ],
        cols,
    )
    lines.append(jnp.zeros((rows - len(lines), cols), jnp.float32))
    aux[3] = jnp.concatenate(lines, axis=0)
    landed(owns.at[0], load.at[len(small)])

    def field_copy(i, d):
        return send(
            aux.at[0:3],
            fin.at[(d % 3) * n_lat + lat],
            send_a.at[0],
            recv_a.at[0],
            at(lax.rem(lat + i, n_lat), east_of(-d), ens),
        )

    def line_copy(i):
        return send(
            aux.at[3],
            lin.at[me],
            send_a.at[1],
            recv_a.at[1],
            same_core(lax.rem(me + i, blocks)),
        )

    def run_iteration(t, own, other, gx):
        got, goth, arrived = (gots.at[t], goths.at[t], arriveds.at[t])
        partner_part, halves = (partner_parts.at[t], halves_all.at[t])

        def param_copy(k, i):
            to = lax.rem(lat + i, n_lat)
            return send(
                own.at[to * groups_here + k],
                got.at[k, :, :, lat],
                send_p.at[k],
                recv_p.at[k],
                at(to, lon, ens),
            )

        def edge_copy(k, i, side):
            to = lax.rem(lat + i, n_lat)
            return send(
                edges.at[side, to * groups_here + k],
                goth.at[k, lat, side],
                send_h.at[k],
                recv_h.at[k],
                at(to, east_of(2 * side - 1), ens),
            )

        swap = send(own, other, send_x.at[t, 0], recv_x.at[t, 0], partner)

        def pack_edges(g):
            slot = lane // EDGE
            for p in range(2):
                left = jnp.zeros((SUB, cols), jnp.float32)
                right = left
                for r in range(rows):
                    tile = pltpu.roll(own[g, p, r], EDGE * r, 1)
                    left = jnp.where(slot == r, tile, left)
                    right = jnp.where(slot == (r + rows - 1) % rows, tile, right)
                edges[0, g, p] = pltpu.roll(left, 2 * EDGE * lat, 1)
                edges[1, g, p] = pltpu.roll(right, 2 * EDGE * lat, 1)

        if t == 0:
            for g in range(groups):
                pack_edges(g)
            pl.semaphore_wait(barrier, blocks - 1 + n_lat)
            for d in (0, 1, -1):
                for i in range(0 if d else 1, n_lat):
                    field_copy(i, d).start()
        for k in range(groups_here):
            for i in range(1, n_lat):
                param_copy(k, i).start()
            if t and k == 0:
                for g in range(groups):
                    pack_edges(g)
            for side in range(2):
                for i in range(n_lat):
                    edge_copy(k, i, side).start()
            if t == 0 and k == 0:
                for i in range(1, blocks):
                    line_copy(i).start()
        swap.start()
        for k in range(groups_here):
            got[k, :, :, pl.ds(lat, 1)] = own[pl.ds(lat * groups_here + k, 1)].reshape(
                2, rows, 1, SUB, cols
            )

        if t == 0:
            fin[pl.ds(lat, 1)] = aux[0:3].reshape(1, 3, rows, cols)
            lin[pl.ds(me, 1)] = aux[3:4]
            landed(fin.at[0 : 3 * n_lat - 1], recv_a.at[0])
            segment = segment_of((rows, cols), n_lat)
            inside = lax.rem(lane + EDGE, 2 * EDGE) < EDGE
            for i in range(3):
                halo = jnp.zeros((rows, cols), jnp.float32)
                tiles = []
                for a in range(n_lat):
                    turned = [
                        pltpu.roll(fin[d * n_lat + a, i], 2 * EDGE * a, 1) for d in range(3)
                    ]
                    tiles.append(turned[0])
                    outer = jnp.where(inside, turned[2], turned[1])
                    halo = jnp.where(segment == a, outer, halo)
                for a, tile in enumerate(tiles + [halo]):
                    for r in range(rows):
                        start[i, r, a] = jnp.broadcast_to(tile[r : r + 1], (SUB, cols))
            for r in range(rows):
                speed_n[r + 1] = start[2, r]
            set_edges(speed_n)
            for r in range(0, rows, CHUNK):
                flow = east(start[1, r : r + CHUNK]) + (
                    speed_n[r + 2 : r + 2 + CHUNK] - speed_n[r : r + CHUNK]
                )
                start[0, r : r + CHUNK] = start[0, r : r + CHUNK] - depth_step * flow
            landed(lin.at[0 : blocks - 1], recv_a.at[1])
            for n in range(ITERS):
                for a in range(n_lat):
                    line = lin[a * n_lon + lon][n : n + 1].astype(jnp.int32)
                    cells[n * n_lat + a : n * n_lat + a + 1] = line

        def answer_copy(k, i):
            to = lax.rem(here + i, column)
            part_rows = pl.ds(k * SUB, SUB)
            return send(
                outgoing.at[pl.ds((to // n_lat) * share, share), part_rows],
                arrived.at[:, here, part_rows],
                send_y.at[k],
                recv_y.at[k],
                same_column(to),
            )

        def group(k, carry):
            landed(got.at[k, :, :, 0 : n_lat - 1], recv_p.at[k])
            for p in range(2):
                for r in range(rows):
                    for a in range(1, n_lat):
                        got[k, p, r, a] = pltpu.roll(got[k, p, r, a], 2 * EDGE * a, 1)
            landed(goth.at[k], recv_h.at[k])
            slot = lane // EDGE
            for p in range(2):
                for r in range(rows):
                    halo = jnp.zeros((SUB, cols), jnp.float32)
                    for a in range(n_lat):
                        after, before = (goth[k, a, 0, p], goth[k, a, 1, p])
                        halo = jnp.where(slot == (2 * a + r) % rows, after, halo)
                        halo = jnp.where(slot == (2 * a + r + rows - 1) % rows, before, halo)
                    got[k, p, r, n_lat] = pltpu.roll(halo, (cols - EDGE * r) % cols, 1)
            run_group(k, got, start, height, speed_e, speed_n)
            for a in range(n_lat):
                line = t * n_lat + a
                wanted = jnp.broadcast_to(cells[line : line + 1], (SUB, cols))
                lanes = jnp.bitwise_and(wanted + 2 * EDGE * a, cols - 1)
                where_row = jnp.right_shift(wanted, cols.bit_length() - 1)
                found = jnp.zeros((SUB, cols), jnp.float32)
                for r in range(rows):
                    tile = height[r + 1, a]
                    picked = jnp.take_along_axis(tile, lanes, axis=1)
                    found = jnp.where(where_row == r, picked, found)
                outgoing[a, pl.ds(k * SUB, SUB)] = found
            for i in range(1, column):
                answer_copy(k, i).start()
            return carry

        lax.fori_loop(0, groups_here, group, 0)
        for j in range(share):
            arrived[j, pl.ds(here, 1)] = outgoing[pl.ds(ens * share + j, 1)]
        if t == 0:
            slots = cols // blocks
            heard = jnp.concatenate([lin[b] for b in range(blocks)], axis=0)
            kinds = lin.shape[1]
            square = (heard.shape[1], cols)
            from_ids = lax.broadcasted_iota(jnp.int32, square, 0)
            to_ids = lax.broadcasted_iota(jnp.int32, square, 1)
            line_ids = lax.broadcasted_iota(jnp.int32, heard.shape, 0)
            lane_ids = lax.broadcasted_iota(jnp.int32, heard.shape, 1)
            for j in range(share):
                owner = (ens * share + j) * n_lon + lon
                chosen = from_ids == owner * slots + lax.rem(to_ids, slots)
                spread_out = jnp.dot(
                    heard,
                    chosen.astype(jnp.float32),
                    precision=lax.Precision.HIGHEST,
                    preferred_element_type=jnp.float32,
                )
                for kind in range(2 * ITERS):
                    wanted = line_ids == (lane_ids // slots) * kinds + ITERS + kind
                    info[kind : kind + 1, j * cols : (j + 1) * cols] = jnp.sum(
                        jnp.where(wanted, spread_out, 0.0), axis=0, keepdims=True
                    )
        for k in range(groups_here):
            landed(arrived.at[:, 0 : column - 1, k * SUB : (k + 1) * SUB], recv_y.at[k])

        members = column * arrived.shape[2]
        predicted = jnp.concatenate(
            [
                jnp.concatenate([arrived[j, s] for s in range(column)], axis=0)
                for j in range(share)
            ],
            axis=1,
        )
        observed = info[t : t + 1]
        precision = info[ITERS + t : ITERS + t + 1]
        centre = jnp.sum(predicted, axis=0, keepdims=True) / members
        spread = predicted - centre
        weighted = spread * precision
        extra = lax.broadcasted_iota(jnp.int32, (SUB, share * cols), 0) == 0
        extra = jnp.where(extra, jnp.broadcast_to(observed - centre, extra.shape), 0.0)

        def products(rows):
            return lax.dot_general(
                rows,
                weighted,
                (((1,), (1,)), ((), ())),
                precision=lax.Precision.HIGHEST,
                preferred_element_type=jnp.float32,
            )

        lines = members // 2 // n_ens
        quarters = [spread[n * lines : (n + 1) * lines] for n in range(2 * n_ens)]
        by_core = [
            jnp.concatenate([quarters[e], quarters[n_ens + e]], axis=0) for e in range(n_ens)
        ]
        theirs = jnp.where(ens == 0, by_core[1], by_core[0])
        product = products(jnp.concatenate([theirs, extra], axis=0))
        tail = product[2 * lines :]
        part[...] = packed(1 - ens, product[: 2 * lines], tail)
        trade = send(part, partner_part, send_x.at[t, 1], recv_x.at[t, 1], partner)
        trade.start()
        mine = packed(ens, products(jnp.where(ens == 0, by_core[0], by_core[1])), tail)
        trade.wait()
        half_sum[...] = mine + partner_part[...]

        def half_copy(i):
            return send(
                half_sum,
                halves.at[lon],
                send_x.at[t, 3],
                recv_x.at[t, 3],
                at(lat, east_of(i), ens),
            )

        for i in range(1, n_lon):
            half_copy(i).start()
        halves[lon] = half_sum[...]
        landed(halves.at[0 : n_lon - 1], recv_x.at[t, 3])
        landed(halves.at[0 : n_lon - 1], send_x.at[t, 3])
        total = halves[0]
        for b in range(1, n_lon):
            total = total + halves[b]
        half_sum[...] = total
        finish = send(half_sum, gx.at[ens], send_x.at[t, 2], recv_x.at[t, 2], partner)
        finish.start()
        gx[ens] = total
        swap.wait()
        for k in range(groups_here):
            landed(got.at[k, :, :, 0 : n_lat - 1], send_p.at[k])
            landed(goth.at[k], send_h.at[k])
            landed(arrived.at[:, 0 : column - 1, k * SUB : (k + 1) * SUB], send_y.at[k])
        if t == 0:
            landed(fin.at[0 : 3 * n_lat - 1], send_a.at[0])
            landed(lin.at[0 : blocks - 1], send_a.at[1])
        finish.wait()

    for t in range(ITERS):
        last = t == ITERS - 1
        own = own_out if last and t else owns.at[t]
        other, gx = (other_out, gx_out) if last else (others.at[t], gxs.at[t])
        run_iteration(t, own, other, gx)
        if not last:
            new = own_out if t + 1 == ITERS - 1 else owns.at[t + 1]

            def store(p, r, value, new=new):
                for g in range(groups):
                    new[g, p, r] = value[g * SUB : (g + 1) * SUB]

            updated_rows(member_weights(gx, ens), own, other, store)


def ensemble_call(sizes, own_shape, *operands):
    n_lat, n_lon, n_ens = sizes
    blocks = n_lat * n_lon
    column = n_lat * n_ens
    groups, _, rows, _, cols = own_shape
    groups_here = groups // n_lat
    members = groups * SUB * n_ens
    share = n_lat // n_ens
    lines = members // 2 // n_ens + SUB
    f32 = jnp.float32
    dma = pltpu.SemaphoreType.DMA
    gx_shape = (n_ens, lines, members)
    outs = [jax.ShapeDtypeStruct(shape, f32) for shape in (gx_shape, own_shape, own_shape)]

    def both(shape):
        return [dma(shape), dma(shape)]

    scratch = [
        VMEM((max(ITERS - 1, 1),) + own_shape, f32),
        VMEM((max(ITERS - 1, 1),) + own_shape, f32),
        VMEM((max(ITERS - 1, 1),) + gx_shape, f32),
        VMEM((4, rows, cols), f32),
        VMEM((blocks, rows, cols), f32),
        VMEM((3 * n_lat, 3, rows, cols), f32),
    ]
    scratch += [VMEM(obs.shape, obs.dtype) for obs in operands[3:]]
    scratch += [
        VMEM((ITERS * n_lat, cols), jnp.int32),
        VMEM((SUB, share * cols), f32),
        VMEM((3, rows, n_lat + 1, SUB, cols), f32),
        VMEM((rows + 2, n_lat + 1, SUB, cols), f32),
        VMEM((rows, n_lat + 1, SUB, cols), f32),
        VMEM((rows + 2, n_lat + 1, SUB, cols), f32),
        VMEM((ITERS, groups_here, 2, rows, n_lat + 1, SUB, cols), f32),
        VMEM((2, groups, 2, SUB, cols), f32),
        VMEM((ITERS, groups_here, n_lat, 2, 2, SUB, cols), f32),
        VMEM((n_lat, groups_here * SUB, cols), f32),
        VMEM((ITERS, share, column, groups_here * SUB, cols), f32),
        VMEM(gx_shape[1:], f32),
        VMEM((ITERS, lines, members), f32),
        VMEM((lines, members), f32),
        VMEM((ITERS, n_lon, lines, members), f32),
        dma((6,)),
    ]
    for shape in ((2,), (groups_here,), (groups_here,), (groups_here,), (ITERS, 4)):
        scratch += both(shape)
    return pl.pallas_call(
        functools.partial(ensemble_kernel, n_lat, n_lon, n_ens),
        out_shape=outs,
        in_specs=[pl.BlockSpec(memory_space=pltpu.HBM)] * len(operands),
        out_specs=[pl.BlockSpec(memory_space=VMEM)] * len(outs),
        scratch_shapes=scratch,
        compiler_params=pltpu.CompilerParams(
            collective_id=0, has_side_effects=True, vmem_limit_bytes=VMEM_LIMIT
        ),
    )(*operands)


def update_kernel(gx, own, other, out, new, sems):
    copies = [pltpu.make_async_copy(new.at[p], out.at[p], sems.at[p]) for p in range(2)]
    rows = own.shape[2]

    def store(p, r, value):
        new[p, :, r, :] = value
        if r == rows - 1:
            copies[p].start()

    updated_rows(member_weights(gx, lax.axis_index("ens")), own, other, store)
    for copy in copies:
        copy.wait()


def update_call(shape, *operands):
    return pl.pallas_call(
        update_kernel,
        out_shape=jax.ShapeDtypeStruct(shape, jnp.float32),
        in_specs=[pl.BlockSpec(memory_space=VMEM)] * len(operands),
        out_specs=pl.BlockSpec(memory_space=pltpu.HBM),
        scratch_shapes=[VMEM(shape, jnp.float32), pltpu.SemaphoreType.DMA((2,))],
        compiler_params=pltpu.CompilerParams(vmem_limit_bytes=VMEM_LIMIT),
    )(*operands)


def per_device_columns(sizes, parameters, initial_height, initial_speed, *observations):
    shape = parameters.shape
    own_shape = (shape[1] // SUB, shape[0], shape[2], SUB, shape[3])
    grouped = parameters.reshape(shape[0], shape[1] // SUB, SUB, shape[2], shape[3])
    turned = [jnp.transpose(obs, (0, 1, 3, 2)) for obs in observations]
    operands = [grouped, initial_height, initial_speed] + turned
    operands = [pltpu.with_memory_space_constraint(x, pltpu.HBM) for x in operands]
    gathered = ensemble_call(sizes, own_shape, *operands)
    return update_call(shape, *gathered)


def by_members(sizes, parameters, initial_height, initial_speed, obs_slots, *rest):
    n_lat, n_lon, n_ens = sizes
    members_here, rows, cols = parameters.shape[1:]
    fits = (
        n_ens == 2
        and n_lat % n_ens == 0
        and n_lon >= 3
        and members_here % (SUB * n_lat) == 0
        and rows == SUB
        and members_here * n_ens == cols
        and cols == 128
        and EDGE * rows == cols
        and 2 * EDGE * n_lat == cols
        and 2 * STEPS <= EDGE
        and ITERS * 3 <= rows
        and obs_slots.shape[2] * obs_slots.shape[3] == cols
        and obs_slots.shape[3] == SUB
        and ITERS > 1
    )
    arguments = (parameters, initial_height, initial_speed, obs_slots) + rest
    if fits:
        return per_device_columns(sizes, *arguments)
    return per_device_halo(*arguments)


def solution(mesh):
    placed = (
        P(None, "ens", "lat", "lon"),
        P("lat", "lon"),
        P(None, "lat", "lon"),
        P(None, ("lat", "lon"), None, None),
        P(None, ("lat", "lon"), None, None),
        P(None, ("lat", "lon"), None, None),
    )
    return jax.shard_map(
        functools.partial(by_members, tuple(mesh.shape[a] for a in ("lat", "lon", "ens"))),
        mesh=mesh,
        in_specs=placed,
        out_specs=P(None, "ens", "lat", "lon"),
        check_vma=False,
    )
```

```python
import math

import functools

import jax
import jax.numpy as jnp
from jax import lax
from jax.experimental import pallas as pl
from jax.experimental.pallas import tpu as pltpu
from jax.sharding import PartitionSpec as P

STEPS = 6
ITERS = 2


depth_step = 0.7
gravity_step = 0.7
coriolis = 0.1


def padded_2(value, sides, width, wrap):
    for axis, dim in sides:
        peers, length = (lax.axis_size(axis), value.shape[dim])
        up = [(i, (i + 1) % peers) for i in range(peers if wrap else peers - 1)]
        down = [(j, i) for i, j in up]
        last = lax.slice_in_dim(value, length - width, length, axis=dim)
        leading = lax.slice_in_dim(value, 0, width, axis=dim)
        before = lax.ppermute(last, axis, up)
        after = lax.ppermute(leading, axis, down)
        value = jnp.concatenate([before, value, after], axis=dim)
    return value


def wall_rows(padded):
    row_count = padded.shape[-2]
    position = lax.axis_index("lat")
    last_block = lax.axis_size("lat") - 1
    row_ids = lax.broadcasted_iota(jnp.int32, (row_count, 1), 0)
    lower_wall = jnp.logical_and(row_ids == 0, position == 0)
    upper_wall = jnp.logical_and(row_ids == row_count - 1, position == last_block)
    keep_rows = jnp.logical_not(jnp.logical_or(lower_wall, upper_wall))
    return padded * keep_rows.astype(padded.dtype)


def advance(height, speeds, friction, forcing):
    east_padded = padded_2(speeds[0], (("lon", 2),), 1, True)
    north_padded = padded_2(speeds[1], (("lat", 1),), 1, False)
    east_diff = east_padded[:, :, 2:] - east_padded[:, :, :-2]
    north_diff = north_padded[:, 2:, :] - north_padded[:, :-2, :]
    height = height - depth_step * (east_diff + north_diff) + forcing
    padded_height = padded_2(height, (("lat", 1), ("lon", 2)), 1, True)
    padded_height = wall_rows(padded_height)
    slope_east = padded_height[:, 1:-1, 2:] - padded_height[:, 1:-1, :-2]
    slope_north = padded_height[:, 2:, 1:-1] - padded_height[:, :-2, 1:-1]
    eastward = (1.0 - friction) * speeds[0] - gravity_step * slope_east + coriolis * speeds[1]
    northward = (1.0 - friction) * speeds[1] - gravity_step * slope_north - coriolis * speeds[0]
    return (height, jnp.stack([eastward, northward]))


def forward(parameters, initial_height, initial_speed):
    members = parameters.shape[1]
    height = jnp.broadcast_to(initial_height, (members,) + initial_height.shape)
    speeds = jnp.broadcast_to(initial_speed[:, None], (2, members) + initial_height.shape)
    for substep in range(STEPS):
        height, speeds = advance(height, speeds, parameters[0], parameters[1])
    return height


def predict(height, cells):
    flattened = height.reshape(height.shape[0], -1)
    wanted = cells.reshape(-1)
    picked = jnp.take(flattened, jnp.clip(wanted, 0, flattened.shape[1] - 1), axis=1)
    picked = jnp.where(wanted[None, :] >= 0, picked, jnp.float32(0.0))
    return picked.T.reshape(cells.shape[0], -1)


def gram_terms(predicted, observed, precision):
    members = predicted.shape[1]
    centre = jnp.mean(predicted, axis=1, keepdims=True)
    spread = predicted - centre
    weighted = spread * precision[:, None]
    misfit = observed[:, None] - predicted
    gram_part = jnp.dot(spread.T, weighted, precision=lax.Precision.HIGHEST) / members
    cross_part = jnp.dot(weighted.T, misfit, precision=lax.Precision.HIGHEST) / math.sqrt(members)
    return (gram_part, cross_part)


def solve_weights(gram_part, cross_part):
    members = gram_part.shape[0]
    system = jnp.eye(members, dtype=jnp.float32) + gram_part
    factor = jnp.linalg.cholesky(system)
    weights = jax.scipy.linalg.cho_solve((factor, True), cross_part) / math.sqrt(members)
    return weights - jnp.mean(weights, axis=0, keepdims=True)


def per_device_halo(parameters, initial_height, initial_speed, obs_slots, obs_values, obs_precision):
    owners = obs_slots.shape[2]
    slot_count = obs_slots.shape[3]
    members_here = parameters.shape[1]
    member_block = lax.axis_index("ens")
    owner_values, owner_precision = (
        lax.all_to_all(obs_values[:, 0], ("lat", "lon"), split_axis=1, concat_axis=1, tiled=True),
        lax.all_to_all(
            obs_precision[:, 0], ("lat", "lon"), split_axis=1, concat_axis=1, tiled=True
        ),
    )
    for iteration in range(ITERS):
        height = forward(parameters, initial_height, initial_speed)
        outgoing = predict(height, obs_slots[iteration, 0])
        received = outgoing
        observed = owner_values[iteration]
        precision = owner_precision[iteration]
        received = received.reshape(owners, slot_count, members_here)
        gathered = lax.all_gather(received, "ens", axis=2, tiled=True)
        members = gathered.shape[2]
        gram_part, cross_part = gram_terms(
            gathered.reshape(-1, members), observed.reshape(-1), precision.reshape(-1)
        )
        gram_part, cross_part = lax.psum((gram_part, cross_part), ("lat", "lon"))
        centred = solve_weights(gram_part, cross_part)
        local_weights = lax.dynamic_slice_in_dim(
            centred, member_block * members_here, members_here, 1
        )
        starting = jnp.zeros(
            (2, members_here, parameters.shape[2] * parameters.shape[3]), jnp.float32
        )
        pieces = lax.all_gather(parameters, "ens", axis=1, tiled=True)
        stacked = pieces.reshape(pieces.shape[0], pieces.shape[1], -1)
        increment = starting + jnp.einsum(
            "pjc,jm->pmc", stacked, local_weights, precision=lax.Precision.HIGHEST
        )
        parameters = parameters + increment.reshape(parameters.shape)
    return parameters


MESH = pl.DeviceIdType.MESH
VMEM = pltpu.VMEM
EDGE = 16
SUB = 8
AHEAD = 6
CHUNK = 2
VMEM_LIMIT = 40 * 2**20


def segment_of(shape, tiles):
    lane = lax.broadcasted_iota(jnp.int32, shape, len(shape) - 1)
    width = shape[-1] // tiles
    return lax.rem(lane + width // 2, shape[-1]) // width


def east(field):
    tiles, cols = (field.shape[1] - 1, field.shape[3])
    width = cols // tiles
    lane = lax.broadcasted_iota(jnp.int32, field.shape[2:], 1)

    def moved(shift, seam):
        turned = pltpu.roll(field, shift % cols, 3)
        halo = turned[:, tiles]
        parts = []
        for a in range(tiles):
            here = lane == (a * width + seam) % cols
            parts.append(jnp.where(here, turned[:, tiles], turned[:, a]))
            halo = jnp.where(here, turned[:, a], halo)
        return parts + [halo]

    return jnp.stack(
        [after - before for after, before in zip(moved(-1, -1), moved(1, 0))], axis=1
    )


def set_edges(ref):
    tiles, cols = (ref.shape[1] - 1, ref.shape[3])
    width = cols // tiles
    segment = segment_of(ref.shape[2:], tiles)
    zero = jnp.zeros(ref.shape[2:], jnp.float32)
    first, last = (1, ref.shape[0] - 2)
    for a in range(tiles):
        ref[0, a] = pltpu.roll(ref[last, a - 1], width, 1) if a else zero
        ref[last + 1, a] = (
            pltpu.roll(ref[first, a + 1], cols - width, 1) if a + 1 < tiles else zero
        )
    ref[0, tiles] = jnp.where(segment == 0, 0.0, pltpu.roll(ref[last, tiles], width, 1))
    ref[last + 1, tiles] = jnp.where(
        segment == tiles - 1, 0.0, pltpu.roll(ref[first, tiles], cols - width, 1)
    )


def flat_lines(blocks, width):
    count, groups = blocks[0].shape
    lanes = lax.broadcasted_iota(jnp.int32, (groups, width), 1)
    group_ids = lax.broadcasted_iota(jnp.int32, (groups, width), 0)
    spread_out = jnp.dot(
        jnp.concatenate(blocks, axis=0),
        (lanes // count == group_ids).astype(jnp.float32),
        precision=lax.Precision.HIGHEST,
        preferred_element_type=jnp.float32,
    )
    slots = lax.broadcasted_iota(jnp.int32, (count, width), 0)
    lanes = lax.broadcasted_iota(jnp.int32, (count, width), 1)
    keep = lax.rem(lanes, count) == slots
    lines = []
    for n in range(len(blocks)):
        block = spread_out[n * count : (n + 1) * count]
        lines.append(jnp.sum(jnp.where(keep, block, 0.0), axis=0, keepdims=True))
    return lines


def send(src, dst, send_sem, recv_sem, device):
    return pltpu.make_async_remote_copy(
        src_ref=src,
        dst_ref=dst,
        send_sem=send_sem,
        recv_sem=recv_sem,
        device_id=device,
        device_id_type=MESH,
    )


def run_group(k, got, start, height, speed_e, speed_n):
    rows = start.shape[1]
    chunks = [pl.ds(c, CHUNK) for c in range(0, rows, CHUNK)]
    upper = [pl.ds(c + 2, CHUNK) for c in range(0, rows, CHUNK)]
    inner = [pl.ds(c + 1, CHUNK) for c in range(0, rows, CHUNK)]

    def new_speeds(n, keep, old_e, old_n):
        slope_e = east(height[inner[n]])
        slope_n = height[upper[n]] - height[chunks[n]]
        speed_e[chunks[n]] = keep * old_e - gravity_step * slope_e + coriolis * old_n
        speed_n[inner[n]] = keep * old_n - gravity_step * slope_n - coriolis * old_e

    def new_height():
        for n in range(len(chunks)):
            flow = east(speed_e[chunks[n]]) + (speed_n[upper[n]] - speed_n[chunks[n]])
            height[inner[n]] = height[inner[n]] - depth_step * flow + got[k, 1, chunks[n]]

    for n in range(len(chunks)):
        height[inner[n]] = start[0, chunks[n]] + got[k, 1, chunks[n]]
    set_edges(height)
    for n in range(len(chunks)):
        keep = 1.0 - got[k, 0, chunks[n]]
        got[k, 0, chunks[n]] = keep
        new_speeds(n, keep, start[1, chunks[n]], start[2, chunks[n]])
    set_edges(speed_n)

    def middle(step, carry):
        new_height()
        set_edges(height)
        for n in range(len(chunks)):
            new_speeds(n, got[k, 0, chunks[n]], speed_e[chunks[n]], speed_n[inner[n]])
        set_edges(speed_n)
        return carry

    lax.fori_loop(1, STEPS - 1, middle, 0)
    tiles = start.shape[2] - 1
    for n in range(len(chunks)):
        flow = east(speed_e[chunks[n]])[:, 0:tiles] + (
            speed_n[upper[n], 0:tiles] - speed_n[chunks[n], 0:tiles]
        )
        height[inner[n], 0:tiles] = (
            height[inner[n], 0:tiles] - depth_step * flow + got[k, 1, chunks[n], 0:tiles]
        )


def inverse_rows(matrix):
    size = matrix.shape[1]
    strip = size // 2 // SUB
    row_ids = lax.broadcasted_iota(jnp.int32, (SUB, size), 0)
    lane_ids = lax.broadcasted_iota(jnp.int32, (SUB, size), 1)
    zero = jnp.zeros((SUB, size), jnp.float32)
    tiles = [matrix[n * SUB : (n + 1) * SUB] for n in range(matrix.shape[0] // SUB)]

    def columns_of(tile, start):
        return [
            jnp.broadcast_to(tile[:, start + k : start + k + 1], (SUB, size))
            for k in range(SUB)
        ]

    def less_rows(tile, band, columns, rows):
        tile = jnp.where(band, 0.0, tile)
        for k in range(SUB):
            tile = tile - columns[k] * rows[k : k + 1]
        return tile

    for base in range(0, size // SUB, strip):
        last = base + strip == size // SUB
        inner = tiles[base:] if last else tiles[base : base + strip]
        columns = columns_of(inner[0], base * SUB)
        for n in range(strip):
            start = (base + n) * SUB
            band = jnp.logical_and(lane_ids >= start, lane_ids < start + SUB)
            unit = (lane_ids - start == row_ids).astype(jnp.float32)
            rows = jnp.where(band, unit, inner[n])
            follows = n + 1 < strip
            ahead = []
            if follows:
                ahead = columns_of(inner[n], start + SUB)[:AHEAD]
                below = columns_of(inner[n + 1], start)
                later = columns_of(inner[n + 1], start + SUB)[:AHEAD]
            for k in range(SUB):
                column = columns[k]
                inverse = 1.0 / column[k : k + 1]
                here = row_ids == k

                def reduce(value):
                    pivot_row = value[k : k + 1] * inverse
                    return jnp.where(here, pivot_row, value - column * pivot_row)

                for other in range(k + 1, SUB):
                    columns[other] = reduce(columns[other])
                ahead = [reduce(value) for value in ahead]
                rows = reduce(rows)
            after = list(inner)
            after[n] = rows
            if follows:
                after[n + 1] = less_rows(inner[n + 1], band, below, rows)
                for k in range(SUB):
                    later = [
                        value - below[k] * line[k : k + 1] for value, line in zip(later, ahead)
                    ]
                columns = later + columns_of(after[n + 1], start + SUB)[AHEAD:]
            for m in range(len(inner)):
                if m != n and not (follows and m == n + 1):
                    after[m] = less_rows(inner[m], band, columns_of(inner[m], start), rows)
            inner = after
        if last:
            return inner[:strip], inner[strip]
        outer = [m for m in range(len(tiles)) if not base <= m < base + strip]
        lines = [
            inner[m - base] if base <= m < base + strip else zero for m in range(size // SUB)
        ]
        product = jnp.dot(
            jnp.concatenate([tiles[m] for m in outer], axis=0),
            jnp.concatenate(lines, axis=0),
            precision=lax.Precision.HIGHEST,
            preferred_element_type=jnp.float32,
        )
        band = jnp.logical_and(lane_ids >= base * SUB, lane_ids < (base + strip) * SUB)
        for n, m in enumerate(outer):
            tiles[m] = jnp.where(band, 0.0, tiles[m]) - product[n * SUB : (n + 1) * SUB]
        tiles[base : base + strip] = inner


def packed(e, rows, tail):
    lines, width = (rows.shape[0] // 2, rows.shape[1])
    half = width // 2
    row_ids = lax.broadcasted_iota(jnp.int32, (lines, width), 0) + e * lines
    lane_ids = lax.broadcasted_iota(jnp.int32, (lines, width), 1)
    top, bottom = (rows[:lines], rows[lines:])
    dense = jnp.where(lane_ids <= row_ids + half, bottom, pltpu.roll(top, half, 1))
    diagonal = jnp.sum(jnp.where(lane_ids == row_ids, top, 0.0), axis=0, keepdims=True)
    tail_ids = lax.broadcasted_iota(jnp.int32, tail.shape, 0)
    return jnp.concatenate([dense, jnp.where(tail_ids == 1, diagonal, tail)], axis=0)


def unpacked(parts):
    half = sum(part.shape[0] - SUB for part in parts)
    dense = jnp.concatenate([part[: part.shape[0] - SUB] for part in parts], axis=0)
    tails = [part[part.shape[0] - SUB :] for part in parts]
    diagonal = sum(tail[1:2] for tail in tails)
    row_ids = lax.broadcasted_iota(jnp.int32, (half, 2 * half), 0)
    lane_ids = lax.broadcasted_iota(jnp.int32, (half, 2 * half), 1)
    turned = jnp.concatenate([dense, dense], axis=0).T
    upper = jnp.where(lane_ids > row_ids, pltpu.roll(dense, half, 1), turned[half:])
    upper = jnp.where(lane_ids == row_ids, diagonal, upper)
    top = jnp.where(lane_ids >= half, turned[:half], upper)
    bottom = jnp.where(lane_ids <= row_ids + half, dense, turned[half:])
    return top, bottom, tails[0][0:1]


def member_weights(gx, ens):
    members = gx.shape[2]
    half = members // 2
    top, bottom, line = unpacked([gx[e] for e in range(gx.shape[0])])

    def turned(value):
        return pltpu.roll(value, half, 1)

    swap = ens == 0
    line = jnp.broadcast_to(line, (SUB, members))
    line = jnp.where(swap, turned(line), line)
    upper = jnp.where(swap, turned(bottom), top) / members
    lower = jnp.where(swap, turned(top), bottom) / members
    row_ids = lax.broadcasted_iota(jnp.int32, (half, members), 0)
    lane_ids = lax.broadcasted_iota(jnp.int32, (half, members), 1)
    unit = (lane_ids == row_ids + half).astype(jnp.float32)
    upper = upper + (lane_ids == row_ids).astype(jnp.float32)
    rows, below = inverse_rows(jnp.concatenate([upper, lower + unit, line], axis=0))
    weights = jnp.concatenate(rows, axis=0) - unit - below[0:1] / members
    return weights - jnp.sum(weights, axis=1, keepdims=True) / members


def updated_rows(mine, own, other, store):
    groups, _, rows, _, cols = own.shape
    for p in range(2):
        for r in range(0, rows, 2):
            pair, local = ([], [])
            for q in (r, r + 1):
                local.append(jnp.concatenate([own[g, p, q] for g in range(groups)], axis=0))
                remote = [other[g, p, q] for g in range(groups)]
                pair.append(jnp.concatenate(remote + [local[-1]], axis=0))
            added = jnp.dot(
                mine,
                jnp.concatenate(pair, axis=1),
                precision=lax.Precision.HIGHEST,
                preferred_element_type=jnp.float32,
            )
            for q in range(2):
                store(p, r + q, local[q] + added[:, q * cols : (q + 1) * cols])


def ensemble_kernel(n_lat, n_lon, n_ens, *refs):
    params, start_height, start_speed, slots_in, values_in, precision_in = refs[:6]
    gx_out, own_out, other_out = refs[6:9]
    owns, others, gxs, aux, lin, fin, slots_here, values_here, precision_here = refs[9:18]
    outer_fields, refs = (refs[18], refs[:18] + refs[19:])
    cells, info, start, height, speed_e, speed_n = refs[18:24]
    gots, edges, goths, outgoing, arriveds, part, partner_parts, half_sum, halves_all = refs[24:33]
    load, send_a, recv_a, send_p, recv_p, send_h, recv_h = refs[33:40]
    send_y, recv_y, send_x, recv_x = refs[40:]
    lat, lon, ens = (lax.axis_index("lat"), lax.axis_index("lon"), lax.axis_index("ens"))
    blocks = n_lat * n_lon
    me = lat * n_lon + lon
    column = n_lat * n_ens
    here = ens * n_lat + lat
    groups, _, rows, _, cols = own_out.shape
    groups_here = groups // n_lat
    share = n_lat // n_ens
    lane = lax.broadcasted_iota(jnp.int32, (SUB, cols), 1)

    def at(lat_to, lon_to, ens_to):
        return {"lat": lat_to, "lon": lon_to, "ens": ens_to}

    def same_column(flat):
        return at(lax.rem(flat, n_lat), lon, flat // n_lat)

    def same_core(block):
        return at(block // n_lon, lax.rem(block, n_lon), ens)

    def east_of(d):
        return lax.rem(lon + d + n_lon, n_lon)

    partner = at(lat, lon, 1 - ens)
    barrier = pltpu.get_barrier_semaphore()

    def greet(device):
        pl.semaphore_signal(barrier, inc=1, device_id=device, device_id_type=MESH)

    for i in range(1, blocks):
        greet(same_core(lax.rem(me + i, blocks)))
    for i in range(n_lat):
        greet(at(i, lon, 1 - ens))

    def landed(ref, sem):
        pltpu.make_async_copy(ref, ref, sem).wait()

    small = [
        pltpu.make_async_copy(src, dst, load.at[n])
        for n, (src, dst) in enumerate(
            (
                (slots_in, slots_here),
                (values_in, values_here),
                (precision_in, precision_here),
                (start_height, aux.at[0]),
                (start_speed, aux.at[1:3]),
            )
        )
    ]
    for copy in small:
        copy.start()
    for p in range(2):
        for r in range(rows):
            pltpu.make_async_copy(
                params.at[p, :, :, r, :], owns.at[0, :, p, r], load.at[len(small)]
            ).start()
    info[...] = jnp.zeros(info.shape, jnp.float32)
    for copy in small:
        copy.wait()
    lines = flat_lines(
        [
            ref[t, 0].astype(jnp.float32)
            for ref in (slots_here, values_here, precision_here)
            for t in range(ITERS)
        ],
        cols,
    )
    lines.append(jnp.zeros((rows - len(lines), cols), jnp.float32))
    aux[3] = jnp.concatenate(lines, axis=0)
    slot = lane // EDGE
    packed_fields = jnp.zeros((rows, cols), jnp.float32)
    for i in range(3):
        left = pltpu.roll(aux[i], EDGE * i, 1)
        right = pltpu.roll(aux[i], (EDGE * (i + 5)) % cols, 1)
        packed_fields = jnp.where(slot == i, left, packed_fields)
        packed_fields = jnp.where(slot == i + 4, right, packed_fields)
    aux[4] = packed_fields
    landed(owns.at[0], load.at[len(small)])

    def field_copy(i, d):
        pick = 2 if d else 0
        return send(
            aux.at[4] if d else aux.at[0:3],
            outer_fields.at[(d % 3 - 1) * n_lat + lat] if d else fin.at[lat],
            send_a.at[pick],
            recv_a.at[pick],
            at(lax.rem(lat + i, n_lat), east_of(-d), ens),
        )

    def line_copy(i):
        return send(
            aux.at[3],
            lin.at[me],
            send_a.at[1],
            recv_a.at[1],
            same_core(lax.rem(me + i, blocks)),
        )

    def param_copy(t, own, k, i, which):
        to = lax.rem(lat + i, n_lat)
        return send(
            own.at[to * groups_here + k, which],
            gots.at[t, k, which, :, lat],
            send_p.at[k],
            recv_p.at[k],
            at(to, lon, ens),
        )

    def run_iteration(t, own, other, gx):
        got, goth, arrived = (gots.at[t], goths.at[t], arriveds.at[t])
        partner_part, halves = (partner_parts.at[t], halves_all.at[t])

        def edge_copy(k, i, side):
            to = lax.rem(lat + i, n_lat)
            return send(
                edges.at[side, to * groups_here + k],
                goth.at[k, lat, side],
                send_h.at[k],
                recv_h.at[k],
                at(to, east_of(2 * side - 1), ens),
            )

        swap = send(own, other, send_x.at[t, 0], recv_x.at[t, 0], partner)

        def pack_edges(g):
            slot = lane // EDGE
            for p in range(2):
                left = jnp.zeros((SUB, cols), jnp.float32)
                right = left
                for r in range(rows):
                    tile = pltpu.roll(own[g, p, r], EDGE * r, 1)
                    left = jnp.where(slot == r, tile, left)
                    right = jnp.where(slot == (r + rows - 1) % rows, tile, right)
                edges[0, g, p] = pltpu.roll(left, 2 * EDGE * lat, 1)
                edges[1, g, p] = pltpu.roll(right, 2 * EDGE * lat, 1)

        if t == 0:
            for g in range(groups):
                pack_edges(g)
            pl.semaphore_wait(barrier, blocks - 1 + n_lat)
            for d in (0, 1, -1):
                for i in range(0 if d else 1, n_lat):
                    field_copy(i, d).start()
        for k in range(groups_here):
            for i in range(1, n_lat):
                param_copy(t, own, k, i, pl.ds(1, 1) if t and k == 0 else pl.ds(0, 2)).start()
            if t and k == 0:
                for g in range(groups):
                    pack_edges(g)
            for side in range(2):
                for i in range(n_lat):
                    edge_copy(k, i, side).start()
            if t == 0 and k == 0:
                for i in range(1, blocks):
                    line_copy(i).start()
        swap.start()
        for k in range(groups_here):
            got[k, :, :, pl.ds(lat, 1)] = own[pl.ds(lat * groups_here + k, 1)].reshape(
                2, rows, 1, SUB, cols
            )

        if t == 0:
            fin[pl.ds(lat, 1)] = aux[0:3].reshape(1, 3, rows, cols)
            lin[pl.ds(me, 1)] = aux[3:4]
            landed(fin.at[0 : n_lat - 1], recv_a.at[0])
            landed(outer_fields, recv_a.at[2])
            segment = segment_of((rows, cols), n_lat)
            inside = lax.rem(lane + EDGE, 2 * EDGE) < EDGE
            for i in range(3):
                halo = jnp.zeros((rows, cols), jnp.float32)
                tiles = []
                for a in range(n_lat):
                    tiles.append(pltpu.roll(fin[a, i], 2 * EDGE * a, 1))
                    shift = 2 * EDGE * a - EDGE * i
                    after = pltpu.roll(outer_fields[a], shift % cols, 1)
                    before = pltpu.roll(
                        outer_fields[n_lat + a], (shift - 5 * EDGE) % cols, 1
                    )
                    outer = jnp.where(inside, before, after)
                    halo = jnp.where(segment == a, outer, halo)
                for a, tile in enumerate(tiles + [halo]):
                    for r in range(rows):
                        start[i, r, a] = jnp.broadcast_to(tile[r : r + 1], (SUB, cols))
            for r in range(rows):
                speed_n[r + 1] = start[2, r]
            set_edges(speed_n)
            for r in range(0, rows, CHUNK):
                flow = east(start[1, r : r + CHUNK]) + (
                    speed_n[r + 2 : r + 2 + CHUNK] - speed_n[r : r + CHUNK]
                )
                start[0, r : r + CHUNK] = start[0, r : r + CHUNK] - depth_step * flow
            landed(lin.at[0 : blocks - 1], recv_a.at[1])
            for n in range(ITERS):
                for a in range(n_lat):
                    line = lin[a * n_lon + lon][n : n + 1].astype(jnp.int32)
                    cells[n * n_lat + a : n * n_lat + a + 1] = line

        def answer_copy(k, i):
            to = lax.rem(here + i, column)
            part_rows = pl.ds(k * SUB, SUB)
            return send(
                outgoing.at[pl.ds((to // n_lat) * share, share), part_rows],
                arrived.at[:, here, part_rows],
                send_y.at[k],
                recv_y.at[k],
                same_column(to),
            )

        def group(k, carry):
            landed(got.at[k, :, :, 0 : n_lat - 1], recv_p.at[k])
            for p in range(2):
                for r in range(rows):
                    for a in range(1, n_lat):
                        got[k, p, r, a] = pltpu.roll(got[k, p, r, a], 2 * EDGE * a, 1)
            landed(goth.at[k], recv_h.at[k])
            slot = lane // EDGE
            for p in range(2):
                for r in range(rows):
                    halo = jnp.zeros((SUB, cols), jnp.float32)
                    for a in range(n_lat):
                        after, before = (goth[k, a, 0, p], goth[k, a, 1, p])
                        halo = jnp.where(slot == (2 * a + r) % rows, after, halo)
                        halo = jnp.where(slot == (2 * a + r + rows - 1) % rows, before, halo)
                    got[k, p, r, n_lat] = pltpu.roll(halo, (cols - EDGE * r) % cols, 1)
            run_group(k, got, start, height, speed_e, speed_n)
            for a in range(n_lat):
                line = t * n_lat + a
                wanted = jnp.broadcast_to(cells[line : line + 1], (SUB, cols))
                lanes = jnp.bitwise_and(wanted + 2 * EDGE * a, cols - 1)
                where_row = jnp.right_shift(wanted, cols.bit_length() - 1)
                found = jnp.zeros((SUB, cols), jnp.float32)
                for r in range(rows):
                    tile = height[r + 1, a]
                    picked = jnp.take_along_axis(tile, lanes, axis=1)
                    found = jnp.where(where_row == r, picked, found)
                outgoing[a, pl.ds(k * SUB, SUB)] = found
            for i in range(1, column):
                answer_copy(k, i).start()
            return carry

        lax.fori_loop(0, groups_here, group, 0)
        for j in range(share):
            arrived[j, pl.ds(here, 1)] = outgoing[pl.ds(ens * share + j, 1)]
        if t == 0:
            slots = cols // blocks
            heard = jnp.concatenate([lin[b] for b in range(blocks)], axis=0)
            kinds = lin.shape[1]
            square = (heard.shape[1], cols)
            from_ids = lax.broadcasted_iota(jnp.int32, square, 0)
            to_ids = lax.broadcasted_iota(jnp.int32, square, 1)
            line_ids = lax.broadcasted_iota(jnp.int32, heard.shape, 0)
            lane_ids = lax.broadcasted_iota(jnp.int32, heard.shape, 1)
            for j in range(share):
                owner = (ens * share + j) * n_lon + lon
                chosen = from_ids == owner * slots + lax.rem(to_ids, slots)
                spread_out = jnp.dot(
                    heard,
                    chosen.astype(jnp.float32),
                    precision=lax.Precision.HIGHEST,
                    preferred_element_type=jnp.float32,
                )
                for kind in range(2 * ITERS):
                    wanted = line_ids == (lane_ids // slots) * kinds + ITERS + kind
                    info[kind : kind + 1, j * cols : (j + 1) * cols] = jnp.sum(
                        jnp.where(wanted, spread_out, 0.0), axis=0, keepdims=True
                    )
        for k in range(groups_here):
            landed(arrived.at[:, 0 : column - 1, k * SUB : (k + 1) * SUB], recv_y.at[k])

        members = column * arrived.shape[2]
        predicted = jnp.concatenate(
            [
                jnp.concatenate([arrived[j, s] for s in range(column)], axis=0)
                for j in range(share)
            ],
            axis=1,
        )
        observed = info[t : t + 1]
        precision = info[ITERS + t : ITERS + t + 1]
        centre = jnp.sum(predicted, axis=0, keepdims=True) / members
        spread = predicted - centre
        weighted = spread * precision
        extra = lax.broadcasted_iota(jnp.int32, (SUB, share * cols), 0) == 0
        extra = jnp.where(extra, jnp.broadcast_to(observed - centre, extra.shape), 0.0)

        def products(rows):
            return lax.dot_general(
                rows,
                weighted,
                (((1,), (1,)), ((), ())),
                precision=lax.Precision.HIGHEST,
                preferred_element_type=jnp.float32,
            )

        lines = members // 2 // n_ens
        quarters = [spread[n * lines : (n + 1) * lines] for n in range(2 * n_ens)]
        by_core = [
            jnp.concatenate([quarters[e], quarters[n_ens + e]], axis=0) for e in range(n_ens)
        ]
        theirs = jnp.where(ens == 0, by_core[1], by_core[0])
        product = products(jnp.concatenate([theirs, extra], axis=0))
        tail = product[2 * lines :]
        part[...] = packed(1 - ens, product[: 2 * lines], tail)
        trade = send(part, partner_part, send_x.at[t, 1], recv_x.at[t, 1], partner)
        trade.start()
        mine = packed(ens, products(jnp.where(ens == 0, by_core[0], by_core[1])), tail)
        trade.wait()
        half_sum[...] = mine + partner_part[...]

        def half_copy(i):
            return send(
                half_sum,
                halves.at[lon],
                send_x.at[t, 3],
                recv_x.at[t, 3],
                at(lat, east_of(i), ens),
            )

        for i in range(1, n_lon):
            half_copy(i).start()
        halves[lon] = half_sum[...]
        landed(halves.at[0 : n_lon - 1], recv_x.at[t, 3])
        landed(halves.at[0 : n_lon - 1], send_x.at[t, 3])
        total = halves[0]
        for b in range(1, n_lon):
            total = total + halves[b]
        half_sum[...] = total
        finish = send(half_sum, gx.at[ens], send_x.at[t, 2], recv_x.at[t, 2], partner)
        finish.start()
        gx[ens] = total
        swap.wait()
        for k in range(groups_here):
            landed(got.at[k, :, :, 0 : n_lat - 1], send_p.at[k])
            landed(goth.at[k], send_h.at[k])
            landed(arrived.at[:, 0 : column - 1, k * SUB : (k + 1) * SUB], send_y.at[k])
        if t == 0:
            landed(fin.at[0 : n_lat - 1], send_a.at[0])
            landed(outer_fields, send_a.at[2])
            landed(lin.at[0 : blocks - 1], send_a.at[1])
        finish.wait()

    for t in range(ITERS):
        last = t == ITERS - 1
        own = own_out if last and t else owns.at[t]
        other, gx = (other_out, gx_out) if last else (others.at[t], gxs.at[t])
        run_iteration(t, own, other, gx)
        if not last:
            new = own_out if t + 1 == ITERS - 1 else owns.at[t + 1]

            def store(p, r, value, t=t + 1, new=new):
                for g in range(groups):
                    new[g, p, r] = value[g * SUB : (g + 1) * SUB]
                if p == 0 and r == rows - 1:
                    for i in range(1, n_lat):
                        param_copy(t, new, 0, i, pl.ds(0, 1)).start()

            updated_rows(member_weights(gx, ens), own, other, store)


def ensemble_call(sizes, own_shape, *operands):
    n_lat, n_lon, n_ens = sizes
    blocks = n_lat * n_lon
    column = n_lat * n_ens
    groups, _, rows, _, cols = own_shape
    groups_here = groups // n_lat
    members = groups * SUB * n_ens
    share = n_lat // n_ens
    lines = members // 2 // n_ens + SUB
    f32 = jnp.float32
    dma = pltpu.SemaphoreType.DMA
    gx_shape = (n_ens, lines, members)
    outs = [jax.ShapeDtypeStruct(shape, f32) for shape in (gx_shape, own_shape, own_shape)]

    def both(shape):
        return [dma(shape), dma(shape)]

    scratch = [
        VMEM((max(ITERS - 1, 1),) + own_shape, f32),
        VMEM((max(ITERS - 1, 1),) + own_shape, f32),
        VMEM((max(ITERS - 1, 1),) + gx_shape, f32),
        VMEM((5, rows, cols), f32),
        VMEM((blocks, rows, cols), f32),
        VMEM((n_lat, 3, rows, cols), f32),
    ]
    scratch += [VMEM(obs.shape, obs.dtype) for obs in operands[3:]]
    scratch += [VMEM((2 * n_lat, rows, cols), f32)]
    scratch += [
        VMEM((ITERS * n_lat, cols), jnp.int32),
        VMEM((SUB, share * cols), f32),
        VMEM((3, rows, n_lat + 1, SUB, cols), f32),
        VMEM((rows + 2, n_lat + 1, SUB, cols), f32),
        VMEM((rows, n_lat + 1, SUB, cols), f32),
        VMEM((rows + 2, n_lat + 1, SUB, cols), f32),
        VMEM((ITERS, groups_here, 2, rows, n_lat + 1, SUB, cols), f32),
        VMEM((2, groups, 2, SUB, cols), f32),
        VMEM((ITERS, groups_here, n_lat, 2, 2, SUB, cols), f32),
        VMEM((n_lat, groups_here * SUB, cols), f32),
        VMEM((ITERS, share, column, groups_here * SUB, cols), f32),
        VMEM(gx_shape[1:], f32),
        VMEM((ITERS, lines, members), f32),
        VMEM((lines, members), f32),
        VMEM((ITERS, n_lon, lines, members), f32),
        dma((6,)),
    ]
    for shape in ((3,), (groups_here,), (groups_here,), (groups_here,), (ITERS, 4)):
        scratch += both(shape)
    return pl.pallas_call(
        functools.partial(ensemble_kernel, n_lat, n_lon, n_ens),
        out_shape=outs,
        in_specs=[pl.BlockSpec(memory_space=pltpu.HBM)] * len(operands),
        out_specs=[pl.BlockSpec(memory_space=VMEM)] * len(outs),
        scratch_shapes=scratch,
        compiler_params=pltpu.CompilerParams(
            collective_id=0, has_side_effects=True, vmem_limit_bytes=VMEM_LIMIT
        ),
    )(*operands)


def update_kernel(gx, own, other, out, new, sems):
    def store(p, r, value):
        new[p, r] = value
        pltpu.make_async_copy(new.at[p, r], out.at[p, :, r, :], sems.at[p]).start()

    updated_rows(member_weights(gx, lax.axis_index("ens")), own, other, store)
    for p in range(2):
        pltpu.make_async_copy(new.at[p], new.at[p], sems.at[p]).wait()


def update_call(shape, *operands):
    return pl.pallas_call(
        update_kernel,
        out_shape=jax.ShapeDtypeStruct(shape, jnp.float32),
        in_specs=[pl.BlockSpec(memory_space=VMEM)] * len(operands),
        out_specs=pl.BlockSpec(memory_space=pltpu.HBM),
        scratch_shapes=[
            VMEM((shape[0], shape[2], shape[1], shape[3]), jnp.float32),
            pltpu.SemaphoreType.DMA((2,)),
        ],
        compiler_params=pltpu.CompilerParams(vmem_limit_bytes=VMEM_LIMIT),
    )(*operands)


def per_device_columns(sizes, parameters, initial_height, initial_speed, *observations):
    shape = parameters.shape
    own_shape = (shape[1] // SUB, shape[0], shape[2], SUB, shape[3])
    grouped = parameters.reshape(shape[0], shape[1] // SUB, SUB, shape[2], shape[3])
    turned = [jnp.transpose(obs, (0, 1, 3, 2)) for obs in observations]
    operands = [grouped, initial_height, initial_speed] + turned
    operands = [pltpu.with_memory_space_constraint(x, pltpu.HBM) for x in operands]
    gathered = ensemble_call(sizes, own_shape, *operands)
    return update_call(shape, *gathered)


def by_members(sizes, parameters, initial_height, initial_speed, obs_slots, *rest):
    n_lat, n_lon, n_ens = sizes
    members_here, rows, cols = parameters.shape[1:]
    fits = (
        n_ens == 2
        and n_lat % n_ens == 0
        and n_lon >= 3
        and members_here % (SUB * n_lat) == 0
        and rows == SUB
        and members_here * n_ens == cols
        and cols == 128
        and EDGE * rows == cols
        and 2 * EDGE * n_lat == cols
        and 2 * STEPS <= EDGE
        and ITERS * 3 <= rows
        and obs_slots.shape[2] * obs_slots.shape[3] == cols
        and obs_slots.shape[3] == SUB
        and ITERS > 1
    )
    arguments = (parameters, initial_height, initial_speed, obs_slots) + rest
    if fits:
        return per_device_columns(sizes, *arguments)
    return per_device_halo(*arguments)


def solution(mesh):
    placed = (
        P(None, "ens", "lat", "lon"),
        P("lat", "lon"),
        P(None, "lat", "lon"),
        P(None, ("lat", "lon"), None, None),
        P(None, ("lat", "lon"), None, None),
        P(None, ("lat", "lon"), None, None),
    )
    return jax.shard_map(
        functools.partial(by_members, tuple(mesh.shape[a] for a in ("lat", "lon", "ens"))),
        mesh=mesh,
        in_specs=placed,
        out_specs=P(None, "ens", "lat", "lon"),
        check_vma=False,
    )
```

```python
import math

import functools

import jax
import jax.numpy as jnp
from jax import lax
from jax.experimental import pallas as pl
from jax.experimental.pallas import tpu as pltpu
from jax.sharding import PartitionSpec as P

STEPS = 6
ITERS = 2


depth_step = 0.7
gravity_step = 0.7
coriolis = 0.1


def padded_2(value, sides, width, wrap):
    for axis, dim in sides:
        peers, length = (lax.axis_size(axis), value.shape[dim])
        up = [(i, (i + 1) % peers) for i in range(peers if wrap else peers - 1)]
        down = [(j, i) for i, j in up]
        last = lax.slice_in_dim(value, length - width, length, axis=dim)
        leading = lax.slice_in_dim(value, 0, width, axis=dim)
        before = lax.ppermute(last, axis, up)
        after = lax.ppermute(leading, axis, down)
        value = jnp.concatenate([before, value, after], axis=dim)
    return value


def wall_rows(padded):
    row_count = padded.shape[-2]
    position = lax.axis_index("lat")
    last_block = lax.axis_size("lat") - 1
    row_ids = lax.broadcasted_iota(jnp.int32, (row_count, 1), 0)
    lower_wall = jnp.logical_and(row_ids == 0, position == 0)
    upper_wall = jnp.logical_and(row_ids == row_count - 1, position == last_block)
    keep_rows = jnp.logical_not(jnp.logical_or(lower_wall, upper_wall))
    return padded * keep_rows.astype(padded.dtype)


def advance(height, speeds, friction, forcing):
    east_padded = padded_2(speeds[0], (("lon", 2),), 1, True)
    north_padded = padded_2(speeds[1], (("lat", 1),), 1, False)
    east_diff = east_padded[:, :, 2:] - east_padded[:, :, :-2]
    north_diff = north_padded[:, 2:, :] - north_padded[:, :-2, :]
    height = height - depth_step * (east_diff + north_diff) + forcing
    padded_height = padded_2(height, (("lat", 1), ("lon", 2)), 1, True)
    padded_height = wall_rows(padded_height)
    slope_east = padded_height[:, 1:-1, 2:] - padded_height[:, 1:-1, :-2]
    slope_north = padded_height[:, 2:, 1:-1] - padded_height[:, :-2, 1:-1]
    eastward = (1.0 - friction) * speeds[0] - gravity_step * slope_east + coriolis * speeds[1]
    northward = (1.0 - friction) * speeds[1] - gravity_step * slope_north - coriolis * speeds[0]
    return (height, jnp.stack([eastward, northward]))


def forward(parameters, initial_height, initial_speed):
    members = parameters.shape[1]
    height = jnp.broadcast_to(initial_height, (members,) + initial_height.shape)
    speeds = jnp.broadcast_to(initial_speed[:, None], (2, members) + initial_height.shape)
    for substep in range(STEPS):
        height, speeds = advance(height, speeds, parameters[0], parameters[1])
    return height


def predict(height, cells):
    flattened = height.reshape(height.shape[0], -1)
    wanted = cells.reshape(-1)
    picked = jnp.take(flattened, jnp.clip(wanted, 0, flattened.shape[1] - 1), axis=1)
    picked = jnp.where(wanted[None, :] >= 0, picked, jnp.float32(0.0))
    return picked.T.reshape(cells.shape[0], -1)


def gram_terms(predicted, observed, precision):
    members = predicted.shape[1]
    centre = jnp.mean(predicted, axis=1, keepdims=True)
    spread = predicted - centre
    weighted = spread * precision[:, None]
    misfit = observed[:, None] - predicted
    gram_part = jnp.dot(spread.T, weighted, precision=lax.Precision.HIGHEST) / members
    cross_part = jnp.dot(weighted.T, misfit, precision=lax.Precision.HIGHEST) / math.sqrt(members)
    return (gram_part, cross_part)


def solve_weights(gram_part, cross_part):
    members = gram_part.shape[0]
    system = jnp.eye(members, dtype=jnp.float32) + gram_part
    factor = jnp.linalg.cholesky(system)
    weights = jax.scipy.linalg.cho_solve((factor, True), cross_part) / math.sqrt(members)
    return weights - jnp.mean(weights, axis=0, keepdims=True)


def per_device_halo(parameters, initial_height, initial_speed, obs_slots, obs_values, obs_precision):
    owners = obs_slots.shape[2]
    slot_count = obs_slots.shape[3]
    members_here = parameters.shape[1]
    member_block = lax.axis_index("ens")
    owner_values, owner_precision = (
        lax.all_to_all(obs_values[:, 0], ("lat", "lon"), split_axis=1, concat_axis=1, tiled=True),
        lax.all_to_all(
            obs_precision[:, 0], ("lat", "lon"), split_axis=1, concat_axis=1, tiled=True
        ),
    )
    for iteration in range(ITERS):
        height = forward(parameters, initial_height, initial_speed)
        outgoing = predict(height, obs_slots[iteration, 0])
        received = outgoing
        observed = owner_values[iteration]
        precision = owner_precision[iteration]
        received = received.reshape(owners, slot_count, members_here)
        gathered = lax.all_gather(received, "ens", axis=2, tiled=True)
        members = gathered.shape[2]
        gram_part, cross_part = gram_terms(
            gathered.reshape(-1, members), observed.reshape(-1), precision.reshape(-1)
        )
        gram_part, cross_part = lax.psum((gram_part, cross_part), ("lat", "lon"))
        centred = solve_weights(gram_part, cross_part)
        local_weights = lax.dynamic_slice_in_dim(
            centred, member_block * members_here, members_here, 1
        )
        starting = jnp.zeros(
            (2, members_here, parameters.shape[2] * parameters.shape[3]), jnp.float32
        )
        pieces = lax.all_gather(parameters, "ens", axis=1, tiled=True)
        stacked = pieces.reshape(pieces.shape[0], pieces.shape[1], -1)
        increment = starting + jnp.einsum(
            "pjc,jm->pmc", stacked, local_weights, precision=lax.Precision.HIGHEST
        )
        parameters = parameters + increment.reshape(parameters.shape)
    return parameters


MESH = pl.DeviceIdType.MESH
VMEM = pltpu.VMEM
EDGE = 16
SUB = 8
AHEAD = 6
CHUNK = 2
VMEM_LIMIT = 40 * 2**20


def segment_of(shape, tiles):
    lane = lax.broadcasted_iota(jnp.int32, shape, len(shape) - 1)
    width = shape[-1] // tiles
    return lax.rem(lane + width // 2, shape[-1]) // width


def east(field):
    tiles, cols = (field.shape[1] - 1, field.shape[3])
    width = cols // tiles
    lane = lax.broadcasted_iota(jnp.int32, field.shape[2:], 1)

    def moved(shift, seam):
        turned = pltpu.roll(field, shift % cols, 3)
        halo = turned[:, tiles]
        parts = []
        for a in range(tiles):
            here = lane == (a * width + seam) % cols
            parts.append(jnp.where(here, turned[:, tiles], turned[:, a]))
            halo = jnp.where(here, turned[:, a], halo)
        return parts + [halo]

    return jnp.stack(
        [after - before for after, before in zip(moved(-1, -1), moved(1, 0))], axis=1
    )


def set_edges(ref):
    tiles, cols = (ref.shape[1] - 1, ref.shape[3])
    width = cols // tiles
    segment = segment_of(ref.shape[2:], tiles)
    zero = jnp.zeros(ref.shape[2:], jnp.float32)
    first, last = (1, ref.shape[0] - 2)
    for a in range(tiles):
        ref[0, a] = pltpu.roll(ref[last, a - 1], width, 1) if a else zero
        ref[last + 1, a] = (
            pltpu.roll(ref[first, a + 1], cols - width, 1) if a + 1 < tiles else zero
        )
    ref[0, tiles] = jnp.where(segment == 0, 0.0, pltpu.roll(ref[last, tiles], width, 1))
    ref[last + 1, tiles] = jnp.where(
        segment == tiles - 1, 0.0, pltpu.roll(ref[first, tiles], cols - width, 1)
    )


def flat_lines(blocks, width):
    count, groups = blocks[0].shape
    lanes = lax.broadcasted_iota(jnp.int32, (groups, width), 1)
    group_ids = lax.broadcasted_iota(jnp.int32, (groups, width), 0)
    spread_out = jnp.dot(
        jnp.concatenate(blocks, axis=0),
        (lanes // count == group_ids).astype(jnp.float32),
        precision=lax.Precision.HIGHEST,
        preferred_element_type=jnp.float32,
    )
    slots = lax.broadcasted_iota(jnp.int32, (count, width), 0)
    lanes = lax.broadcasted_iota(jnp.int32, (count, width), 1)
    keep = lax.rem(lanes, count) == slots
    lines = []
    for n in range(len(blocks)):
        block = spread_out[n * count : (n + 1) * count]
        lines.append(jnp.sum(jnp.where(keep, block, 0.0), axis=0, keepdims=True))
    return lines


def send(src, dst, send_sem, recv_sem, device):
    return pltpu.make_async_remote_copy(
        src_ref=src,
        dst_ref=dst,
        send_sem=send_sem,
        recv_sem=recv_sem,
        device_id=device,
        device_id_type=MESH,
    )


def run_group(k, got, start, height, speed_e, speed_n):
    rows = start.shape[1]
    chunks = [pl.ds(c, CHUNK) for c in range(0, rows, CHUNK)]
    upper = [pl.ds(c + 2, CHUNK) for c in range(0, rows, CHUNK)]
    inner = [pl.ds(c + 1, CHUNK) for c in range(0, rows, CHUNK)]

    def new_speeds(n, keep, old_e, old_n):
        slope_e = east(height[inner[n]])
        slope_n = height[upper[n]] - height[chunks[n]]
        speed_e[chunks[n]] = keep * old_e - gravity_step * slope_e + coriolis * old_n
        speed_n[inner[n]] = keep * old_n - gravity_step * slope_n - coriolis * old_e

    def new_height():
        for n in range(len(chunks)):
            flow = east(speed_e[chunks[n]]) + (speed_n[upper[n]] - speed_n[chunks[n]])
            height[inner[n]] = height[inner[n]] - depth_step * flow + got[k, 1, chunks[n]]

    for n in range(len(chunks)):
        height[inner[n]] = start[0, chunks[n]] + got[k, 1, chunks[n]]
    set_edges(height)
    for n in range(len(chunks)):
        keep = 1.0 - got[k, 0, chunks[n]]
        got[k, 0, chunks[n]] = keep
        new_speeds(n, keep, start[1, chunks[n]], start[2, chunks[n]])
    set_edges(speed_n)

    def middle(step, carry):
        new_height()
        set_edges(height)
        for n in range(len(chunks)):
            new_speeds(n, got[k, 0, chunks[n]], speed_e[chunks[n]], speed_n[inner[n]])
        set_edges(speed_n)
        return carry

    lax.fori_loop(1, STEPS - 1, middle, 0)
    tiles = start.shape[2] - 1
    for n in range(len(chunks)):
        flow = east(speed_e[chunks[n]])[:, 0:tiles] + (
            speed_n[upper[n], 0:tiles] - speed_n[chunks[n], 0:tiles]
        )
        height[inner[n], 0:tiles] = (
            height[inner[n], 0:tiles] - depth_step * flow + got[k, 1, chunks[n], 0:tiles]
        )


def inverse_rows(matrix):
    size = matrix.shape[1]
    strip = size // 2 // SUB
    row_ids = lax.broadcasted_iota(jnp.int32, (SUB, size), 0)
    lane_ids = lax.broadcasted_iota(jnp.int32, (SUB, size), 1)
    zero = jnp.zeros((SUB, size), jnp.float32)
    tiles = [matrix[n * SUB : (n + 1) * SUB] for n in range(matrix.shape[0] // SUB)]

    def columns_of(tile, start):
        return [
            jnp.broadcast_to(tile[:, start + k : start + k + 1], (SUB, size))
            for k in range(SUB)
        ]

    def less_rows(tile, band, columns, rows):
        tile = jnp.where(band, 0.0, tile)
        for k in range(SUB):
            tile = tile - columns[k] * rows[k : k + 1]
        return tile

    for base in range(0, size // SUB, strip):
        last = base + strip == size // SUB
        inner = tiles[base:] if last else tiles[base : base + strip]
        columns = columns_of(inner[0], base * SUB)
        for n in range(strip):
            start = (base + n) * SUB
            band = jnp.logical_and(lane_ids >= start, lane_ids < start + SUB)
            unit = (lane_ids - start == row_ids).astype(jnp.float32)
            rows = jnp.where(band, unit, inner[n])
            follows = n + 1 < strip
            ahead = []
            if follows:
                ahead = columns_of(inner[n], start + SUB)[:AHEAD]
                below = columns_of(inner[n + 1], start)
                later = columns_of(inner[n + 1], start + SUB)[:AHEAD]
            for k in range(SUB):
                column = columns[k]
                inverse = 1.0 / column[k : k + 1]
                here = row_ids == k

                def reduce(value):
                    pivot_row = value[k : k + 1] * inverse
                    return jnp.where(here, pivot_row, value - column * pivot_row)

                for other in range(k + 1, SUB):
                    columns[other] = reduce(columns[other])
                ahead = [reduce(value) for value in ahead]
                rows = reduce(rows)
            after = list(inner)
            after[n] = rows
            if follows:
                after[n + 1] = less_rows(inner[n + 1], band, below, rows)
                for k in range(SUB):
                    later = [
                        value - below[k] * line[k : k + 1] for value, line in zip(later, ahead)
                    ]
                columns = later + columns_of(after[n + 1], start + SUB)[AHEAD:]
            for m in range(len(inner)):
                if m != n and not (follows and m == n + 1):
                    after[m] = less_rows(inner[m], band, columns_of(inner[m], start), rows)
            inner = after
        if last:
            return inner[:strip], inner[strip]
        outer = [m for m in range(len(tiles)) if not base <= m < base + strip]
        lines = [
            inner[m - base] if base <= m < base + strip else zero for m in range(size // SUB)
        ]
        product = jnp.dot(
            jnp.concatenate([tiles[m] for m in outer], axis=0),
            jnp.concatenate(lines, axis=0),
            precision=lax.Precision.HIGHEST,
            preferred_element_type=jnp.float32,
        )
        band = jnp.logical_and(lane_ids >= base * SUB, lane_ids < (base + strip) * SUB)
        for n, m in enumerate(outer):
            tiles[m] = jnp.where(band, 0.0, tiles[m]) - product[n * SUB : (n + 1) * SUB]
        tiles[base : base + strip] = inner


def packed(e, rows, tail):
    lines, width = (rows.shape[0] // 2, rows.shape[1])
    half = width // 2
    row_ids = lax.broadcasted_iota(jnp.int32, (lines, width), 0) + e * lines
    lane_ids = lax.broadcasted_iota(jnp.int32, (lines, width), 1)
    top, bottom = (rows[:lines], rows[lines:])
    dense = jnp.where(lane_ids <= row_ids + half, bottom, pltpu.roll(top, half, 1))
    diagonal = jnp.sum(jnp.where(lane_ids == row_ids, top, 0.0), axis=0, keepdims=True)
    tail_ids = lax.broadcasted_iota(jnp.int32, tail.shape, 0)
    return jnp.concatenate([dense, jnp.where(tail_ids == 1, diagonal, tail)], axis=0)


def unpacked(parts):
    half = sum(part.shape[0] - SUB for part in parts)
    dense = jnp.concatenate([part[: part.shape[0] - SUB] for part in parts], axis=0)
    tails = [part[part.shape[0] - SUB :] for part in parts]
    diagonal = sum(tail[1:2] for tail in tails)
    row_ids = lax.broadcasted_iota(jnp.int32, (half, 2 * half), 0)
    lane_ids = lax.broadcasted_iota(jnp.int32, (half, 2 * half), 1)
    turned = jnp.concatenate([dense, dense], axis=0).T
    upper = jnp.where(lane_ids > row_ids, pltpu.roll(dense, half, 1), turned[half:])
    upper = jnp.where(lane_ids == row_ids, diagonal, upper)
    top = jnp.where(lane_ids >= half, turned[:half], upper)
    bottom = jnp.where(lane_ids <= row_ids + half, dense, turned[half:])
    return top, bottom, tails[0][0:1]


def member_weights(gx, ens):
    members = gx.shape[2]
    half = members // 2
    top, bottom, line = unpacked([gx[e] for e in range(gx.shape[0])])

    def turned(value):
        return pltpu.roll(value, half, 1)

    swap = ens == 0
    line = jnp.broadcast_to(line, (SUB, members))
    line = jnp.where(swap, turned(line), line)
    upper = jnp.where(swap, turned(bottom), top) / members
    lower = jnp.where(swap, turned(top), bottom) / members
    row_ids = lax.broadcasted_iota(jnp.int32, (half, members), 0)
    lane_ids = lax.broadcasted_iota(jnp.int32, (half, members), 1)
    unit = (lane_ids == row_ids + half).astype(jnp.float32)
    upper = upper + (lane_ids == row_ids).astype(jnp.float32)
    rows, below = inverse_rows(jnp.concatenate([upper, lower + unit, line], axis=0))
    weights = jnp.concatenate(rows, axis=0) - unit - below[0:1] / members
    return weights - jnp.sum(weights, axis=1, keepdims=True) / members


def updated_rows(mine, own, other, store):
    groups, _, rows, _, cols = own.shape
    for p in range(2):
        for r in range(0, rows, 2):
            pair, local = ([], [])
            for q in (r, r + 1):
                local.append(jnp.concatenate([own[g, p, q] for g in range(groups)], axis=0))
                remote = [other[g, p, q] for g in range(groups)]
                pair.append(jnp.concatenate(remote + [local[-1]], axis=0))
            added = jnp.dot(
                mine,
                jnp.concatenate(pair, axis=1),
                precision=lax.Precision.HIGHEST,
                preferred_element_type=jnp.float32,
            )
            for q in range(2):
                store(p, r + q, local[q] + added[:, q * cols : (q + 1) * cols])


def ensemble_kernel(n_lat, n_lon, n_ens, *refs):
    params, start_height, start_speed, slots_in, values_in, precision_in = refs[:6]
    gx_out, own_out, other_out = refs[6:9]
    owns, others, gxs, aux, lin, fin, slots_here, values_here, precision_here = refs[9:18]
    outer_fields, refs = (refs[18], refs[:18] + refs[19:])
    cells, info, start, height, speed_e, speed_n = refs[18:24]
    gots, edges, goths, outgoing, arriveds, part, partner_parts, half_sum, halves_all = refs[24:33]
    load, send_a, recv_a, send_p, recv_p, send_h, recv_h = refs[33:40]
    send_y, recv_y, send_x, recv_x = refs[40:]
    lat, lon, ens = (lax.axis_index("lat"), lax.axis_index("lon"), lax.axis_index("ens"))
    blocks = n_lat * n_lon
    me = lat * n_lon + lon
    column = n_lat * n_ens
    here = ens * n_lat + lat
    groups, _, rows, _, cols = own_out.shape
    groups_here = groups // n_lat
    share = n_lat // n_ens
    lane = lax.broadcasted_iota(jnp.int32, (SUB, cols), 1)

    def at(lat_to, lon_to, ens_to):
        return {"lat": lat_to, "lon": lon_to, "ens": ens_to}

    def same_column(flat):
        return at(lax.rem(flat, n_lat), lon, flat // n_lat)

    def same_core(block):
        return at(block // n_lon, lax.rem(block, n_lon), ens)

    def east_of(d):
        return lax.rem(lon + d + n_lon, n_lon)

    partner = at(lat, lon, 1 - ens)
    barrier = pltpu.get_barrier_semaphore()

    def greet(device):
        pl.semaphore_signal(barrier, inc=1, device_id=device, device_id_type=MESH)

    for i in range(1, blocks):
        greet(same_core(lax.rem(me + i, blocks)))
    for i in range(n_lat):
        greet(at(i, lon, 1 - ens))

    def landed(ref, sem):
        pltpu.make_async_copy(ref, ref, sem).wait()

    small = [
        pltpu.make_async_copy(src, dst, load.at[n])
        for n, (src, dst) in enumerate(
            (
                (slots_in, slots_here),
                (values_in, values_here),
                (precision_in, precision_here),
                (start_height, aux.at[0]),
                (start_speed, aux.at[1:3]),
            )
        )
    ]
    for copy in small:
        copy.start()
    for p in range(2):
        for r in range(rows):
            pltpu.make_async_copy(
                params.at[p, :, :, r, :], owns.at[0, :, p, r], load.at[len(small)]
            ).start()
    info[...] = jnp.zeros(info.shape, jnp.float32)
    for copy in small:
        copy.wait()
    lines = flat_lines(
        [
            ref[t, 0].astype(jnp.float32)
            for ref in (slots_here, values_here, precision_here)
            for t in range(ITERS)
        ],
        cols,
    )
    lines.append(jnp.zeros((rows - len(lines), cols), jnp.float32))
    aux[3] = jnp.concatenate(lines, axis=0)
    slot = lane // EDGE
    packed_fields = jnp.zeros((rows, cols), jnp.float32)
    for i in range(3):
        left = pltpu.roll(aux[i], EDGE * i, 1)
        right = pltpu.roll(aux[i], (EDGE * (i + 5)) % cols, 1)
        packed_fields = jnp.where(slot == i, left, packed_fields)
        packed_fields = jnp.where(slot == i + 4, right, packed_fields)
    aux[4] = packed_fields
    landed(owns.at[0], load.at[len(small)])

    def field_copy(i, d):
        pick = 2 if d else 0
        return send(
            aux.at[4] if d else aux.at[0:3],
            outer_fields.at[(d % 3 - 1) * n_lat + lat] if d else fin.at[lat],
            send_a.at[pick],
            recv_a.at[pick],
            at(lax.rem(lat + i, n_lat), east_of(-d), ens),
        )

    def line_copy(i):
        return send(
            aux.at[3],
            lin.at[me],
            send_a.at[1],
            recv_a.at[1],
            same_core(lax.rem(me + i, blocks)),
        )

    def param_copy(t, own, k, i, which):
        to = lax.rem(lat + i, n_lat)
        return send(
            own.at[to * groups_here + k, which],
            gots.at[t, k, which, :, lat],
            send_p.at[k],
            recv_p.at[k],
            at(to, lon, ens),
        )

    def run_iteration(t, own, other, gx):
        got, goth, arrived = (gots.at[t], goths.at[t], arriveds.at[t])
        partner_part, halves = (partner_parts.at[t], halves_all.at[t])

        def edge_copy(k, i, side):
            to = lax.rem(lat + i, n_lat)
            return send(
                edges.at[side, to * groups_here + k],
                goth.at[k, lat, side],
                send_h.at[k],
                recv_h.at[k],
                at(to, east_of(2 * side - 1), ens),
            )

        swap = send(own, other, send_x.at[t, 0], recv_x.at[t, 0], partner)

        def pack_edges(g):
            slot = lane // EDGE
            for p in range(2):
                left = jnp.zeros((SUB, cols), jnp.float32)
                right = left
                for r in range(rows):
                    tile = pltpu.roll(own[g, p, r], EDGE * r, 1)
                    left = jnp.where(slot == r, tile, left)
                    right = jnp.where(slot == (r + rows - 1) % rows, tile, right)
                edges[0, g, p] = pltpu.roll(left, 2 * EDGE * lat, 1)
                edges[1, g, p] = pltpu.roll(right, 2 * EDGE * lat, 1)

        if t == 0:
            for g in range(groups):
                pack_edges(g)
            pl.semaphore_wait(barrier, blocks - 1 + n_lat)
            for d in (0, 1, -1):
                for i in range(0 if d else 1, n_lat):
                    field_copy(i, d).start()
        for k in range(groups_here):
            for i in range(1, n_lat):
                param_copy(t, own, k, i, pl.ds(1, 1) if t and k == 0 else pl.ds(0, 2)).start()
            if t and k == 0:
                for g in range(groups):
                    pack_edges(g)
            for side in range(2):
                for i in range(n_lat):
                    edge_copy(k, i, side).start()
            if t == 0 and k == 0:
                for i in range(1, blocks):
                    line_copy(i).start()
        for k in range(groups_here):
            got[k, :, :, pl.ds(lat, 1)] = own[pl.ds(lat * groups_here + k, 1)].reshape(
                2, rows, 1, SUB, cols
            )

        if t == 0:
            fin[pl.ds(lat, 1)] = aux[0:3].reshape(1, 3, rows, cols)
            lin[pl.ds(me, 1)] = aux[3:4]
            landed(fin.at[0 : n_lat - 1], recv_a.at[0])
            landed(outer_fields, recv_a.at[2])
            segment = segment_of((rows, cols), n_lat)
            inside = lax.rem(lane + EDGE, 2 * EDGE) < EDGE
            for i in range(3):
                halo = jnp.zeros((rows, cols), jnp.float32)
                tiles = []
                for a in range(n_lat):
                    tiles.append(pltpu.roll(fin[a, i], 2 * EDGE * a, 1))
                    shift = 2 * EDGE * a - EDGE * i
                    after = pltpu.roll(outer_fields[a], shift % cols, 1)
                    before = pltpu.roll(
                        outer_fields[n_lat + a], (shift - 5 * EDGE) % cols, 1
                    )
                    outer = jnp.where(inside, before, after)
                    halo = jnp.where(segment == a, outer, halo)
                for a, tile in enumerate(tiles + [halo]):
                    for r in range(rows):
                        start[i, r, a] = jnp.broadcast_to(tile[r : r + 1], (SUB, cols))
            for r in range(rows):
                speed_n[r + 1] = start[2, r]
            set_edges(speed_n)
            for r in range(0, rows, CHUNK):
                flow = east(start[1, r : r + CHUNK]) + (
                    speed_n[r + 2 : r + 2 + CHUNK] - speed_n[r : r + CHUNK]
                )
                start[0, r : r + CHUNK] = start[0, r : r + CHUNK] - depth_step * flow
            landed(lin.at[0 : blocks - 1], recv_a.at[1])
            for n in range(ITERS):
                for a in range(n_lat):
                    line = lin[a * n_lon + lon][n : n + 1].astype(jnp.int32)
                    cells[n * n_lat + a : n * n_lat + a + 1] = line

        def answer_copy(k, i):
            to = lax.rem(here + i, column)
            part_rows = pl.ds(k * SUB, SUB)
            return send(
                outgoing.at[pl.ds((to // n_lat) * share, share), part_rows],
                arrived.at[:, here, part_rows],
                send_y.at[k],
                recv_y.at[k],
                same_column(to),
            )

        def group(k, carry):
            landed(got.at[k, :, :, 0 : n_lat - 1], recv_p.at[k])
            for p in range(2):
                for r in range(rows):
                    for a in range(1, n_lat):
                        got[k, p, r, a] = pltpu.roll(got[k, p, r, a], 2 * EDGE * a, 1)
            landed(goth.at[k], recv_h.at[k])
            slot = lane // EDGE
            for p in range(2):
                for r in range(rows):
                    halo = jnp.zeros((SUB, cols), jnp.float32)
                    for a in range(n_lat):
                        after, before = (goth[k, a, 0, p], goth[k, a, 1, p])
                        halo = jnp.where(slot == (2 * a + r) % rows, after, halo)
                        halo = jnp.where(slot == (2 * a + r + rows - 1) % rows, before, halo)
                    got[k, p, r, n_lat] = pltpu.roll(halo, (cols - EDGE * r) % cols, 1)
            run_group(k, got, start, height, speed_e, speed_n)
            for a in range(n_lat):
                line = t * n_lat + a
                wanted = jnp.broadcast_to(cells[line : line + 1], (SUB, cols))
                lanes = jnp.bitwise_and(wanted + 2 * EDGE * a, cols - 1)
                where_row = jnp.right_shift(wanted, cols.bit_length() - 1)
                found = jnp.zeros((SUB, cols), jnp.float32)
                for r in range(rows):
                    tile = height[r + 1, a]
                    picked = jnp.take_along_axis(tile, lanes, axis=1)
                    found = jnp.where(where_row == r, picked, found)
                outgoing[a, pl.ds(k * SUB, SUB)] = found
            for i in range(1, column):
                answer_copy(k, i).start()
            return carry

        lax.fori_loop(0, groups_here, group, 0)
        swap.start()
        for j in range(share):
            arrived[j, pl.ds(here, 1)] = outgoing[pl.ds(ens * share + j, 1)]
        if t == 0:
            slots = cols // blocks
            heard = jnp.concatenate([lin[b] for b in range(blocks)], axis=0)
            kinds = lin.shape[1]
            square = (heard.shape[1], cols)
            from_ids = lax.broadcasted_iota(jnp.int32, square, 0)
            to_ids = lax.broadcasted_iota(jnp.int32, square, 1)
            line_ids = lax.broadcasted_iota(jnp.int32, heard.shape, 0)
            lane_ids = lax.broadcasted_iota(jnp.int32, heard.shape, 1)
            for j in range(share):
                owner = (ens * share + j) * n_lon + lon
                chosen = from_ids == owner * slots + lax.rem(to_ids, slots)
                spread_out = jnp.dot(
                    heard,
                    chosen.astype(jnp.float32),
                    precision=lax.Precision.HIGHEST,
                    preferred_element_type=jnp.float32,
                )
                for kind in range(2 * ITERS):
                    wanted = line_ids == (lane_ids // slots) * kinds + ITERS + kind
                    info[kind : kind + 1, j * cols : (j + 1) * cols] = jnp.sum(
                        jnp.where(wanted, spread_out, 0.0), axis=0, keepdims=True
                    )
        for k in range(groups_here):
            landed(arrived.at[:, 0 : column - 1, k * SUB : (k + 1) * SUB], recv_y.at[k])

        members = column * arrived.shape[2]
        predicted = jnp.concatenate(
            [
                jnp.concatenate([arrived[j, s] for s in range(column)], axis=0)
                for j in range(share)
            ],
            axis=1,
        )
        observed = info[t : t + 1]
        precision = info[ITERS + t : ITERS + t + 1]
        centre = jnp.sum(predicted, axis=0, keepdims=True) / members
        spread = predicted - centre
        weighted = spread * precision
        extra = lax.broadcasted_iota(jnp.int32, (SUB, share * cols), 0) == 0
        extra = jnp.where(extra, jnp.broadcast_to(observed - centre, extra.shape), 0.0)

        def products(rows):
            return lax.dot_general(
                rows,
                weighted,
                (((1,), (1,)), ((), ())),
                precision=lax.Precision.HIGHEST,
                preferred_element_type=jnp.float32,
            )

        lines = members // 2 // n_ens
        quarters = [spread[n * lines : (n + 1) * lines] for n in range(2 * n_ens)]
        by_core = [
            jnp.concatenate([quarters[e], quarters[n_ens + e]], axis=0) for e in range(n_ens)
        ]
        theirs = jnp.where(ens == 0, by_core[1], by_core[0])
        product = products(jnp.concatenate([theirs, extra], axis=0))
        tail = product[2 * lines :]
        part[...] = packed(1 - ens, product[: 2 * lines], tail)
        trade = send(part, partner_part, send_x.at[t, 1], recv_x.at[t, 1], partner)
        trade.start()
        mine = packed(ens, products(jnp.where(ens == 0, by_core[0], by_core[1])), tail)
        trade.wait()
        half_sum[...] = mine + partner_part[...]

        def half_copy(i):
            return send(
                half_sum,
                halves.at[lon],
                send_x.at[t, 3],
                recv_x.at[t, 3],
                at(lat, east_of(i), ens),
            )

        for i in range(1, n_lon):
            half_copy(i).start()
        halves[lon] = half_sum[...]
        landed(halves.at[0 : n_lon - 1], recv_x.at[t, 3])
        landed(halves.at[0 : n_lon - 1], send_x.at[t, 3])
        total = halves[0]
        for b in range(1, n_lon):
            total = total + halves[b]
        half_sum[...] = total
        finish = send(half_sum, gx.at[ens], send_x.at[t, 2], recv_x.at[t, 2], partner)
        finish.start()
        gx[ens] = total
        swap.wait()
        for k in range(groups_here):
            landed(got.at[k, :, :, 0 : n_lat - 1], send_p.at[k])
            landed(goth.at[k], send_h.at[k])
            landed(arrived.at[:, 0 : column - 1, k * SUB : (k + 1) * SUB], send_y.at[k])
        if t == 0:
            landed(fin.at[0 : n_lat - 1], send_a.at[0])
            landed(outer_fields, send_a.at[2])
            landed(lin.at[0 : blocks - 1], send_a.at[1])
        finish.wait()

    for t in range(ITERS):
        last = t == ITERS - 1
        own = own_out if last and t else owns.at[t]
        other, gx = (other_out, gx_out) if last else (others.at[t], gxs.at[t])
        run_iteration(t, own, other, gx)
        if not last:
            new = own_out if t + 1 == ITERS - 1 else owns.at[t + 1]

            def store(p, r, value, t=t + 1, new=new):
                for g in range(groups):
                    new[g, p, r] = value[g * SUB : (g + 1) * SUB]
                if p == 0 and r == rows - 1:
                    for i in range(1, n_lat):
                        param_copy(t, new, 0, i, pl.ds(0, 1)).start()

            updated_rows(member_weights(gx, ens), own, other, store)


def ensemble_call(sizes, own_shape, *operands):
    n_lat, n_lon, n_ens = sizes
    blocks = n_lat * n_lon
    column = n_lat * n_ens
    groups, _, rows, _, cols = own_shape
    groups_here = groups // n_lat
    members = groups * SUB * n_ens
    share = n_lat // n_ens
    lines = members // 2 // n_ens + SUB
    f32 = jnp.float32
    dma = pltpu.SemaphoreType.DMA
    gx_shape = (n_ens, lines, members)
    outs = [jax.ShapeDtypeStruct(shape, f32) for shape in (gx_shape, own_shape, own_shape)]

    def both(shape):
        return [dma(shape), dma(shape)]

    scratch = [
        VMEM((max(ITERS - 1, 1),) + own_shape, f32),
        VMEM((max(ITERS - 1, 1),) + own_shape, f32),
        VMEM((max(ITERS - 1, 1),) + gx_shape, f32),
        VMEM((5, rows, cols), f32),
        VMEM((blocks, rows, cols), f32),
        VMEM((n_lat, 3, rows, cols), f32),
    ]
    scratch += [VMEM(obs.shape, obs.dtype) for obs in operands[3:]]
    scratch += [VMEM((2 * n_lat, rows, cols), f32)]
    scratch += [
        VMEM((ITERS * n_lat, cols), jnp.int32),
        VMEM((SUB, share * cols), f32),
        VMEM((3, rows, n_lat + 1, SUB, cols), f32),
        VMEM((rows + 2, n_lat + 1, SUB, cols), f32),
        VMEM((rows, n_lat + 1, SUB, cols), f32),
        VMEM((rows + 2, n_lat + 1, SUB, cols), f32),
        VMEM((ITERS, groups_here, 2, rows, n_lat + 1, SUB, cols), f32),
        VMEM((2, groups, 2, SUB, cols), f32),
        VMEM((ITERS, groups_here, n_lat, 2, 2, SUB, cols), f32),
        VMEM((n_lat, groups_here * SUB, cols), f32),
        VMEM((ITERS, share, column, groups_here * SUB, cols), f32),
        VMEM(gx_shape[1:], f32),
        VMEM((ITERS, lines, members), f32),
        VMEM((lines, members), f32),
        VMEM((ITERS, n_lon, lines, members), f32),
        dma((6,)),
    ]
    for shape in ((3,), (groups_here,), (groups_here,), (groups_here,), (ITERS, 4)):
        scratch += both(shape)
    return pl.pallas_call(
        functools.partial(ensemble_kernel, n_lat, n_lon, n_ens),
        out_shape=outs,
        in_specs=[pl.BlockSpec(memory_space=pltpu.HBM)] * len(operands),
        out_specs=[pl.BlockSpec(memory_space=VMEM)] * len(outs),
        scratch_shapes=scratch,
        compiler_params=pltpu.CompilerParams(
            collective_id=0, has_side_effects=True, vmem_limit_bytes=VMEM_LIMIT
        ),
    )(*operands)


def update_kernel(gx, own, other, out, new, sems):
    def store(p, r, value):
        new[p, r] = value
        pltpu.make_async_copy(new.at[p, r], out.at[p, :, r, :], sems.at[p]).start()

    updated_rows(member_weights(gx, lax.axis_index("ens")), own, other, store)
    for p in range(2):
        pltpu.make_async_copy(new.at[p], new.at[p], sems.at[p]).wait()


def update_call(shape, *operands):
    return pl.pallas_call(
        update_kernel,
        out_shape=jax.ShapeDtypeStruct(shape, jnp.float32),
        in_specs=[pl.BlockSpec(memory_space=VMEM)] * len(operands),
        out_specs=pl.BlockSpec(memory_space=pltpu.HBM),
        scratch_shapes=[
            VMEM((shape[0], shape[2], shape[1], shape[3]), jnp.float32),
            pltpu.SemaphoreType.DMA((2,)),
        ],
        compiler_params=pltpu.CompilerParams(vmem_limit_bytes=VMEM_LIMIT),
    )(*operands)


def per_device_columns(sizes, parameters, initial_height, initial_speed, *observations):
    shape = parameters.shape
    own_shape = (shape[1] // SUB, shape[0], shape[2], SUB, shape[3])
    grouped = parameters.reshape(shape[0], shape[1] // SUB, SUB, shape[2], shape[3])
    turned = [jnp.transpose(obs, (0, 1, 3, 2)) for obs in observations]
    operands = [grouped, initial_height, initial_speed] + turned
    operands = [pltpu.with_memory_space_constraint(x, pltpu.HBM) for x in operands]
    gathered = ensemble_call(sizes, own_shape, *operands)
    return update_call(shape, *gathered)


def by_members(sizes, parameters, initial_height, initial_speed, obs_slots, *rest):
    n_lat, n_lon, n_ens = sizes
    members_here, rows, cols = parameters.shape[1:]
    fits = (
        n_ens == 2
        and n_lat % n_ens == 0
        and n_lon >= 3
        and members_here % (SUB * n_lat) == 0
        and rows == SUB
        and members_here * n_ens == cols
        and cols == 128
        and EDGE * rows == cols
        and 2 * EDGE * n_lat == cols
        and 2 * STEPS <= EDGE
        and ITERS * 3 <= rows
        and obs_slots.shape[2] * obs_slots.shape[3] == cols
        and obs_slots.shape[3] == SUB
        and ITERS > 1
    )
    arguments = (parameters, initial_height, initial_speed, obs_slots) + rest
    if fits:
        return per_device_columns(sizes, *arguments)
    return per_device_halo(*arguments)


def solution(mesh):
    placed = (
        P(None, "ens", "lat", "lon"),
        P("lat", "lon"),
        P(None, "lat", "lon"),
        P(None, ("lat", "lon"), None, None),
        P(None, ("lat", "lon"), None, None),
        P(None, ("lat", "lon"), None, None),
    )
    return jax.shard_map(
        functools.partial(by_members, tuple(mesh.shape[a] for a in ("lat", "lon", "ens"))),
        mesh=mesh,
        in_specs=placed,
        out_specs=P(None, "ens", "lat", "lon"),
        check_vma=False,
    )
```
